64 devices in a mesh: batch: 4 (over x, y), tree: 16 (over z, core).
Axes of the slice: x: 2, y: 2, z: 8, core: 2. Of those that a mesh axis runs over, the one named last changes fastest.
The devices are a block of a 4x4x8 slice.
Arguments:
- x_vecs: float32 [262144, 512], P(('batch', 'tree')), parts along dimension 0
- d_near: bfloat16 [128, 512, 512], P('tree')
- u_leaf: bfloat16 [128, 512, 128], P('tree')
- v_leaf: bfloat16 [128, 512, 128], P('tree')
- w_h0: bfloat16 [128, 128, 256], P('tree')
- r_h0: bfloat16 [128, 128, 256], P('tree')
- b_h0: bfloat16 [128, 128, 128], P('tree')
- w_h1: bfloat16 [64, 256, 256], P('tree')
- r_h1: bfloat16 [64, 256, 256], P('tree')
- b_h1: bfloat16 [64, 256, 256], P('tree')
- w_h2: bfloat16 [32, 256, 512], P('tree')
- r_h2: bfloat16 [32, 256, 512], P('tree')
- b_h2: bfloat16 [32, 256, 256], P('tree')
- w_upper: bfloat16 [16, 512, 512], P('tree')
- r_upper: bfloat16 [16, 512, 512], P('tree')
- b_upper: bfloat16 [16, 512, 512], P('tree')
- w_top: bfloat16 [12, 512, 512], replicated
- r_top: bfloat16 [12, 512, 512], replicated
- b_top: bfloat16 [14, 512, 512], replicated
Outputs:
- output: float32 [262144, 512], P(('batch', 'tree')), parts along dimension 0
There are 4 independent parts. The reference program is written for one: setup_inputs(seed, part) draws one part's arguments, and reference() takes and returns one part's arrays. A program takes and returns all parts, laid end to end along the dimension named above; an argument that names none is the same for every part.
All inputs are finite; a program needn't handle non-finite values.
Results may differ from the reference program's by a relative error of at most 0.0116554.
Values are sent between devices in bfloat16 or wider.
A program may use at most 768 MiB of HBM per device.

```python
import math
import jax
import jax.numpy as jnp
from jax import lax

LEAF_SIZE = 512
LEAF_RANK = 128
NUM_RHS = 512
LEAVES_DEV = 8
TREE_DEVS = 16

LEAF_COUNT = TREE_DEVS * LEAVES_DEV
ROW_COUNT = LEAF_COUNT * LEAF_SIZE
UPPER_DEV = LEAVES_DEV // 4 - 1
TOP_DEPTH = int(math.log2(TREE_DEVS) + 0.5)
UPPER_DEPTH = int(math.log2(UPPER_DEV + 1) + 0.5)


def draw_normal(key, shape, scale):
    return (jax.random.normal(key, shape, jnp.float32) * scale).astype(jnp.bfloat16)


def setup_inputs(seed: int = 0, part: int = 0) -> dict:
    keys = jax.random.split(jax.random.key(seed), 18)
    x_key = jax.random.fold_in(jax.random.key(seed + 1), part)
    rank_one = LEAF_RANK
    rank_two = 2 * LEAF_RANK
    rank_four = 4 * LEAF_RANK
    upper_rows = TREE_DEVS * UPPER_DEV
    return {
        'x_vecs': jax.random.normal(x_key, (ROW_COUNT, NUM_RHS), jnp.float32),
        'd_near': draw_normal(keys[0], (LEAF_COUNT, LEAF_SIZE, LEAF_SIZE), LEAF_SIZE ** -0.5),
        'u_leaf': draw_normal(keys[1], (LEAF_COUNT, LEAF_SIZE, rank_one), rank_one ** -0.5),
        'v_leaf': draw_normal(keys[2], (LEAF_COUNT, LEAF_SIZE, rank_one), LEAF_SIZE ** -0.5),
        'w_h0': draw_normal(keys[3], (LEAF_COUNT, rank_one, rank_two), (2 * rank_one) ** -0.5),
        'r_h0': draw_normal(keys[4], (LEAF_COUNT, rank_one, rank_two), rank_two ** -0.5),
        'b_h0': draw_normal(keys[5], (LEAF_COUNT, rank_one, rank_one), rank_one ** -0.5),
        'w_h1': draw_normal(keys[6], (LEAF_COUNT // 2, rank_two, rank_two), (2 * rank_two) ** -0.5),
        'r_h1': draw_normal(keys[7], (LEAF_COUNT // 2, rank_two, rank_two), rank_two ** -0.5),
        'b_h1': draw_normal(keys[8], (LEAF_COUNT // 2, rank_two, rank_two), rank_two ** -0.5),
        'w_h2': draw_normal(keys[9], (LEAF_COUNT // 4, rank_two, rank_four), (2 * rank_two) ** -0.5),
        'r_h2': draw_normal(keys[10], (LEAF_COUNT // 4, rank_two, rank_four), rank_four ** -0.5),
        'b_h2': draw_normal(keys[11], (LEAF_COUNT // 4, rank_two, rank_two), rank_two ** -0.5),
        'w_upper': draw_normal(keys[12], (upper_rows, rank_four, rank_four), (2 * rank_four) ** -0.5),
        'r_upper': draw_normal(keys[13], (upper_rows, rank_four, rank_four), rank_four ** -0.5),
        'b_upper': draw_normal(keys[14], (upper_rows, rank_four, rank_four), rank_four ** -0.5),
        'w_top': draw_normal(keys[15], (TREE_DEVS - 4, rank_four, rank_four), (2 * rank_four) ** -0.5),
        'r_top': draw_normal(keys[16], (TREE_DEVS - 4, rank_four, rank_four), rank_four ** -0.5),
        'b_top': draw_normal(keys[17], (TREE_DEVS - 2, rank_four, rank_four), rank_four ** -0.5),
    }


def merge_up(w_child, x_child):
    prod = jnp.einsum('nkq,nkc->nqc', w_child.astype(jnp.float32), x_child.astype(jnp.float32))
    pairs = prod.reshape(prod.shape[0] // 2, 2, prod.shape[1], prod.shape[2])
    return (pairs[:, 0] + pairs[:, 1]).astype(jnp.bfloat16)


def couple(b_node, x_level):
    pairs = x_level.reshape(x_level.shape[0] // 2, 2, x_level.shape[1], x_level.shape[2])
    swapped = jnp.flip(pairs, axis=1).reshape(x_level.shape)
    return jnp.einsum('nkj,njc->nkc', b_node.astype(jnp.float32), swapped.astype(jnp.float32))


def push_down(r_child, y_parent, coupled):
    r_pairs = r_child.reshape(r_child.shape[0] // 2, 2, r_child.shape[1], r_child.shape[2])
    prod = jnp.einsum('nekq,nqc->nekc', r_pairs.astype(jnp.float32), y_parent.astype(jnp.float32))
    return (coupled + prod.reshape(coupled.shape)).astype(jnp.bfloat16)


def upper_levels(packed):
    grouped = packed.reshape(TREE_DEVS, UPPER_DEV, packed.shape[1], packed.shape[2])
    return [grouped[:, 2 ** step - 1:2 ** (step + 1) - 1].reshape(TREE_DEVS * 2 ** step, packed.shape[1], packed.shape[2]) for step in range(UPPER_DEPTH)]


def top_levels(packed, first):
    return [packed[2 ** level - 2 ** first:2 ** (level + 1) - 2 ** first] for level in range(first, TOP_DEPTH)]


def reference(x_vecs, d_near, u_leaf, v_leaf, w_h0, r_h0, b_h0, w_h1, r_h1, b_h1, w_h2, r_h2, b_h2, w_upper, r_upper, b_upper, w_top, r_top, b_top):
    x_dev = x_vecs.astype(jnp.bfloat16).reshape(TREE_DEVS, LEAVES_DEV, LEAF_SIZE, NUM_RHS)

    def leaf_up(block):
        v_block, x_block = block
        prod = jnp.einsum('lmk,lmc->lkc', v_block.astype(jnp.float32), x_block.astype(jnp.float32))
        return prod.astype(jnp.bfloat16)

    x_skel = lax.map(leaf_up, (v_leaf.reshape(TREE_DEVS, LEAVES_DEV, LEAF_SIZE, LEAF_RANK), x_dev))
    skel_up = [x_skel.reshape(LEAF_COUNT, LEAF_RANK, NUM_RHS)]
    w_levels = [w_h0, w_h1, w_h2] + list(reversed(upper_levels(w_upper))) + list(reversed(top_levels(w_top, 2)))
    r_levels = [r_h0, r_h1, r_h2] + list(reversed(upper_levels(r_upper))) + list(reversed(top_levels(r_top, 2)))
    b_levels = [b_h0, b_h1, b_h2] + list(reversed(upper_levels(b_upper))) + list(reversed(top_levels(b_top, 1)))
    for w_child in w_levels:
        skel_up.append(merge_up(w_child, skel_up[-1]))
    coupled = [couple(b_node, x_level) for b_node, x_level in zip(b_levels, skel_up)]
    y_skel = coupled[-1].astype(jnp.bfloat16)
    for level in range(len(r_levels) - 1, -1, -1):
        y_skel = push_down(r_levels[level], y_skel, coupled[level])

    def leaf_down(block):
        d_block, u_block, x_block, y_block = block
        near = jnp.einsum('lmj,ljc->lmc', d_block.astype(jnp.float32), x_block.astype(jnp.float32))
        far = jnp.einsum('lmk,lkc->lmc', u_block.astype(jnp.float32), y_block.astype(jnp.float32))
        return near + far

    y_out = lax.map(leaf_down, (d_near.reshape(TREE_DEVS, LEAVES_DEV, LEAF_SIZE, LEAF_SIZE), u_leaf.reshape(TREE_DEVS, LEAVES_DEV, LEAF_SIZE, LEAF_RANK), x_dev, y_skel.reshape(TREE_DEVS, LEAVES_DEV, LEAF_RANK, NUM_RHS)))
    return y_out.reshape(ROW_COUNT, NUM_RHS)
```

```python
import functools
import math

import jax
import jax.numpy as jnp
from jax import lax
from jax.experimental import pallas as pl
from jax.experimental.pallas import tpu as pltpu
from jax.sharding import PartitionSpec as P

MESH = pl.DeviceIdType.MESH
F32 = jnp.float32
BF16 = jnp.bfloat16
VMEM_ALL = pl.BlockSpec(memory_space=pltpu.VMEM)
HBM_ALL = pl.BlockSpec(memory_space=pl.ANY)


def log_two(count):
    return int(math.log2(count) + 0.5)


def mm(lhs, rhs, lhs_dim, rhs_dim):
    return lax.dot_general(lhs, rhs, (((lhs_dim,), (rhs_dim,)), ((), ())), preferred_element_type=F32)


def up_kernel(devs, x_hbm, d_hbm, v_hbm, w0_hbm, b0_hbm, w1_hbm, b1_hbm, w2_hbm, b2_hbm, wu_hbm, bu_hbm, ru_hbm, wt_hbm, rt_hbm, bt_hbm,
              y_dev, near, g0, g1, g2,
              xf, xb, d, v, w0, b0, w1, b1, w2, b2, wu, bu, ru, wt, rt, bt, xh0, xh1, xh2, xt, xsib, xchip, xall, x2, x1, x1_sib, y_out, y_all,
              x_sem, d_sem, v_sem, w_sem, wsib_sem, swap_send, swap_recv, out_send, out_recv, top_send, top_recv, back_send, back_recv, pair_send, pair_recv):
    me = lax.axis_index('tree')
    chips = devs // 2
    half_chips = chips // 2
    core = lax.rem(me, 2)
    chip = me // 2
    other = 1 - core
    partner = chip * 2 + other
    leaves, leaf_size, cols = xf.shape
    part = cols // devs
    half = cols // 2
    my_half = chip // half_chips

    barrier = pltpu.get_barrier_semaphore()
    for step in range(1, devs):
        pl.semaphore_signal(barrier, inc=1, device_id={'tree': lax.rem(me + step, devs)}, device_id_type=MESH)

    def load_x(i):
        return pltpu.make_async_copy(x_hbm.at[pl.ds(i * leaf_size, leaf_size)], xf.at[i], x_sem.at[i])

    def load_d(i):
        return pltpu.make_async_copy(d_hbm.at[i], d.at[i], d_sem.at[i])

    def load_v(i):
        return pltpu.make_async_copy(v_hbm.at[i], v.at[i], v_sem.at[i])

    def top_slices(hbm, vmem, first, base):
        out = []
        at = 0
        for level in range(first, log_two(devs)):
            count = 2 ** (level - 1)
            start = 2 ** level - 2 ** first + core * count
            out.append(pltpu.make_async_copy(hbm.at[pl.ds(start, count)], vmem.at[pl.ds(at, count)], w_sem.at[base + level]))
            at += count
        return out

    copies = {}
    for k, (name, hbm, vmem) in enumerate([('w0', w0_hbm, w0), ('w1', w1_hbm, w1), ('w2', w2_hbm, w2), ('wu', wu_hbm.at[0], wu.at[0]), ('bu', bu_hbm.at[0], bu), ('ru', ru_hbm.at[0], ru), ('b0', b0_hbm, b0), ('b1', b1_hbm, b1), ('b2', b2_hbm, b2)]):
        copies[name] = pltpu.make_async_copy(hbm, vmem, w_sem.at[k])
    depth = log_two(devs)
    wt_copies = top_slices(wt_hbm, wt, 2, 9)
    rt_copies = top_slices(rt_hbm, rt, 2, 9 + depth)
    bt_copies = top_slices(bt_hbm, bt, 1, 9 + 2 * depth)

    ahead = 4
    for i in range(ahead):
        load_v(i).start()
        load_x(i).start()
    copies['w0'].start()
    copies['w1'].start()

    wsib = pltpu.make_async_remote_copy(wu.at[0], wu.at[1], wsib_sem.at[0], wsib_sem.at[1], device_id={'tree': partner}, device_id_type=MESH)

    for i in range(leaves):
        load_v(i).wait()
        load_x(i).wait()
        if i + ahead < leaves:
            load_v(i + ahead).start()
            load_x(i + ahead).start()
        if i == 1:
            copies['wu'].start()
            copies['w2'].start()
        if i == ahead - 1:
            for name in ('bu', 'b0', 'b1', 'b2'):
                copies[name].start()
            for j in range(leaves):
                load_d(j).start()
            for copy in wt_copies + bt_copies + rt_copies:
                copy.start()
            copies['ru'].start()
        xb[i] = xf[i].astype(BF16)
        xh0[i] = mm(v[i], xb[i], 0, 0).astype(BF16)
        if i % 2 == 1:
            n = i // 2
            if n == 0:
                copies['w0'].wait()
            xh1[n] = (mm(w0[2 * n], xh0[2 * n], 0, 0) + mm(w0[2 * n + 1], xh0[2 * n + 1], 0, 0)).astype(BF16)
        if i % 4 == 3:
            n = i // 4
            if n == 0:
                copies['w1'].wait()
                copies['wu'].wait()
                pl.semaphore_wait(barrier, devs - 1)
                wsib.start()
            xh2[n] = (mm(w1[2 * n], xh1[2 * n], 0, 0) + mm(w1[2 * n + 1], xh1[2 * n + 1], 0, 0)).astype(BF16)
    copies['w2'].wait()

    swaps = []
    for k, side in enumerate((other, core)):
        window = pl.ds(pl.multiple_of(side * half, half), half)
        xt[side] = (mm(xh2[0, :, window], w2[0], 0, 0) + mm(xh2[1, :, window], w2[1], 0, 0)).astype(BF16)
        swaps.append(pltpu.make_async_remote_copy(xt.at[side], xsib.at[side], swap_send.at[k], swap_recv.at[k], device_id={'tree': partner}, device_id_type=MESH))
        swaps[-1].start()
    got = [pltpu.make_async_remote_copy(xt.at[core], xsib.at[core], swap_send.at[0], swap_recv.at[0], device_id={'tree': partner}, device_id_type=MESH),
           pltpu.make_async_remote_copy(xt.at[other], xsib.at[other], swap_send.at[1], swap_recv.at[1], device_id={'tree': partner}, device_id_type=MESH)]

    def near_leaf(i):
        load_d(i).wait()
        near[i] = mm(d[i], xb[i], 1, 0)

    near_leaf(0)
    near_leaf(1)
    wsib.wait()
    got[0].wait_recv()
    merged = (mm(xt[core], wu[0], 1, 0) + mm(xsib[core], wu[1], 1, 0)).astype(BF16)
    xchip[...] = merged.reshape(xchip.shape)

    def out_copy(step):
        dest = lax.rem(chip + step, chips)
        slot = lax.rem(chip, half_chips)
        return pltpu.make_async_remote_copy(xchip.at[dest], xall.at[slot, core], out_send.at[step], out_recv.at[slot, core], device_id={'tree': dest * 2 + my_half}, device_id_type=MESH)

    far_first = [half_chips]
    for step in range(half_chips - 1, 0, -1):
        far_first += [step, chips - step]
    for step in far_first:
        out_copy(step).start()

    @pl.when(core != my_half)
    def _():
        out_copy(0).start()

    @pl.when(core == my_half)
    def _():
        xall[lax.rem(chip, half_chips), core] = xchip[chip]

    for i in range(2, leaves):
        near_leaf(i)
    copies['b0'].wait()
    copies['b1'].wait()
    copies['b2'].wait()
    for n in range(leaves):
        g0[n] = mm(b0[n], xh0[n ^ 1], 1, 0)
    for n in range(leaves // 2):
        g1[n] = mm(b1[n], xh1[n ^ 1], 1, 0)
    for n in range(leaves // 4):
        g2[n] = mm(b2[n], xh2[n ^ 1], 1, 0)
    got[1].wait_recv()
    copies['bu'].wait()
    copies['ru'].wait()
    g_dev = mm(bu[...], xsib[...].reshape(cols, -1), 1, 1)
    for copy in wt_copies + bt_copies + rt_copies:
        copy.wait()

    for n in range(half_chips):
        for c in range(2):
            local = jnp.logical_and(core * half_chips + n == chip, core == c)
            landed = pltpu.make_async_remote_copy(xchip.at[0], xall.at[n, c], out_send.at[0], out_recv.at[n, c], device_id={'tree': partner}, device_id_type=MESH)

            @pl.when(jnp.logical_not(local))
            def _():
                landed.wait_recv()

    mine = 2 * part
    levels = [[xall[n].reshape(mine, -1) for n in range(half_chips)]]
    at = [0]
    for level in range(depth - 1, 1, -1):
        at.append(0)
    w_at = {}
    pos = 0
    for level in range(2, depth):
        w_at[level] = pos
        pos += 2 ** (level - 1)
    b_at = {}
    pos = 0
    for level in range(1, depth):
        b_at[level] = pos
        pos += 2 ** (level - 1)
    for level in range(depth - 1, 1, -1):
        below = levels[-1]
        base = w_at[level]
        levels.append([(mm(below[2 * q], wt[base + 2 * q], 1, 0) + mm(below[2 * q + 1], wt[base + 2 * q + 1], 1, 0)).astype(BF16) for q in range(len(below) // 2)])
    x1[...] = levels[-1][0]
    top_swap = pltpu.make_async_remote_copy(x1, x1_sib, top_send.at[0], top_recv.at[0], device_id={'tree': partner}, device_id_type=MESH)
    top_swap.start()
    g_top = {}
    for level in range(depth - 1, 1, -1):
        nodes = levels[depth - 1 - level]
        g_top[level] = [mm(nodes[n ^ 1], bt[b_at[level] + n], 1, 1) for n in range(len(nodes))]
    top_swap.wait()
    y_top = [mm(x1_sib[...], bt[b_at[1]], 1, 1).astype(BF16)]
    for level in range(2, depth):
        y_top = [(g_top[level][n] + mm(y_top[n // 2], rt[w_at[level] + n], 1, 1)).astype(BF16) for n in range(len(g_top[level]))]
    for n in range(half_chips):
        y_out[n] = y_top[n].reshape(y_out.shape[1:])

    def back_copy(n, c):
        dest = core * half_chips + n
        return pltpu.make_async_remote_copy(y_out.at[n, c], y_all.at[c, chip], back_send.at[n, c], back_recv.at[chip], device_id={'tree': dest * 2 + c}, device_id_type=MESH)

    for n in range(half_chips):
        for c in range(2):
            local = jnp.logical_and(core * half_chips + n == chip, core == c)

            @pl.when(jnp.logical_not(local))
            def _():
                back_copy(n, c).start()

            @pl.when(local)
            def _():
                y_all[c, chip] = y_out[n, c]

    for j in range(chips):
        landed = pltpu.make_async_remote_copy(y_out.at[0, 0], y_all.at[core, j], back_send.at[0, 0], back_recv.at[j], device_id={'tree': partner}, device_id_type=MESH)

        @pl.when(jnp.logical_or(j != chip, core != my_half))
        def _():
            landed.wait_recv()

    pair = pltpu.make_async_remote_copy(y_all.at[core], y_all.at[core], pair_send.at[0], pair_recv.at[0], device_id={'tree': partner}, device_id_type=MESH)
    pair.start()
    pltpu.make_async_remote_copy(y_all.at[other], y_all.at[other], pair_send.at[0], pair_recv.at[0], device_id={'tree': partner}, device_id_type=MESH).wait_recv()
    y_dev[...] = (g_dev + mm(ru[...], y_all[...].reshape(cols, -1), 1, 1)).astype(BF16)

    for swap in swaps:
        swap.wait_send()
    for step in far_first:
        out_copy(step).wait_send()

    @pl.when(core != my_half)
    def _():
        out_copy(0).wait_send()

    for n in range(half_chips):
        for c in range(2):
            local = jnp.logical_and(core * half_chips + n == chip, core == c)

            @pl.when(jnp.logical_not(local))
            def _():
                back_copy(n, c).wait_send()

    pair.wait_send()


def down_kernel(y_dev, near, g0, g1, g2, r0, r1, r2, u, out_hbm, y2, y1, stage, out_sem):
    leaves, leaf_size, cols = stage.shape

    def store(i):
        return pltpu.make_async_copy(stage.at[i], out_hbm.at[pl.ds(i * leaf_size, leaf_size)], out_sem.at[i])

    for i in range(leaves):
        if i % 4 == 0:
            y2[i // 4] = (g2[i // 4] + mm(r2[i // 4], y_dev[...], 1, 0)).astype(BF16)
        if i % 2 == 0:
            y1[i // 2] = (g1[i // 2] + mm(r1[i // 2], y2[i // 4], 1, 0)).astype(BF16)
        y_leaf = (g0[i] + mm(r0[i], y1[i // 2], 1, 0)).astype(BF16)
        stage[i] = near[i] + mm(u[i], y_leaf, 1, 0)
        store(i).start()
    for i in range(leaves):
        store(i).wait()


def solution(mesh):
    devs = mesh.shape['tree']
    rows_spec = P(('batch', 'tree'), None)
    tree_spec = P('tree', None, None)
    full_spec = P(None, None, None)

    def body(x_loc, d_near, u_leaf, v_leaf, w_h0, r_h0, b_h0, w_h1, r_h1, b_h1, w_h2, r_h2, b_h2, w_upper, r_upper, b_upper, w_top, r_top, b_top):
        leaves, leaf_size, rank0 = u_leaf.shape
        cols = x_loc.shape[1]
        rank1 = w_h0.shape[2]
        rank2 = w_h1.shape[2]
        rank3 = w_h2.shape[2]
        chips = devs // 2
        part = cols // devs
        half = cols // 2
        depth = log_two(devs)
        sds = jax.ShapeDtypeStruct
        dma = pltpu.SemaphoreType.DMA
        vmem = pltpu.VMEM
        outs = [sds((rank3, cols), BF16), sds((leaves, leaf_size, cols), F32), sds((leaves, rank0, cols), F32), sds((leaves // 2, rank1, cols), F32), sds((leaves // 4, rank2, cols), F32)]
        half_nodes = chips - 2
        scratch = [
            vmem((leaves, leaf_size, cols), F32), vmem((leaves, leaf_size, cols), BF16), vmem(d_near.shape[:0] + (leaves, leaf_size, leaf_size), BF16),
            vmem((leaves, leaf_size, rank0), BF16),
            vmem((leaves, rank0, rank1), BF16), vmem((leaves, rank0, rank0), BF16),
            vmem((leaves // 2, rank1, rank2), BF16), vmem((leaves // 2, rank1, rank1), BF16),
            vmem((leaves // 4, rank2, rank3), BF16), vmem((leaves // 4, rank2, rank2), BF16),
            vmem((2, rank3, rank3), BF16), vmem((rank3, rank3), BF16), vmem((rank3, rank3), BF16),
            vmem((half_nodes, rank3, rank3), BF16), vmem((half_nodes, rank3, rank3), BF16), vmem((half_nodes + 1, rank3, rank3), BF16),
            vmem((leaves, rank0, cols), BF16), vmem((leaves // 2, rank1, cols), BF16), vmem((leaves // 4, rank2, cols), BF16),
            vmem((2, half, rank3), BF16), vmem((2, half, rank3), BF16),
            vmem((chips, part, rank3), BF16), vmem((chips // 2, 2, part, rank3), BF16),
            vmem((2, 2 * part, rank3), BF16), vmem((2 * part, rank3), BF16), vmem((2 * part, rank3), BF16),
            vmem((chips // 2, 2, part, rank3), BF16), vmem((2, chips, part, rank3), BF16),
            dma((leaves,)), dma((leaves,)), dma((leaves,)), dma((9 + 3 * depth,)), dma((2,)),
            dma((2,)), dma((2,)), dma((chips,)), dma((chips // 2, 2)), dma((1,)), dma((1,)), dma((chips // 2, 2)), dma((chips,)), dma((1,)), dma((1,)),
        ]
        y_dev, near, g0, g1, g2 = pl.pallas_call(
            functools.partial(up_kernel, devs),
            out_shape=outs,
            in_specs=[HBM_ALL] * 15,
            out_specs=[VMEM_ALL] * 5,
            scratch_shapes=scratch,
            compiler_params=pltpu.CompilerParams(collective_id=0, has_side_effects=True, vmem_limit_bytes=60 * 2 ** 20),
            name='up_top',
        )(x_loc, d_near, v_leaf, w_h0, b_h0, w_h1, b_h1, w_h2, b_h2, w_upper, b_upper, r_upper, w_top, r_top, b_top)
        return pl.pallas_call(
            down_kernel,
            out_shape=sds(x_loc.shape, F32),
            in_specs=[VMEM_ALL] * 9,
            out_specs=HBM_ALL,
            scratch_shapes=[vmem((leaves // 4, rank2, cols), BF16), vmem((leaves // 2, rank1, cols), BF16), vmem((leaves, leaf_size, cols), F32), dma((leaves,))],
            compiler_params=pltpu.CompilerParams(vmem_limit_bytes=60 * 2 ** 20),
            name='down_out',
        )(y_dev, near, g0, g1, g2, r_h0, r_h1, r_h2, u_leaf)

    return jax.shard_map(body, mesh=mesh, in_specs=(rows_spec,) + (tree_spec,) * 15 + (full_spec,) * 3, out_specs=rows_spec, check_vma=False)
```

```python
import functools
import math

import jax
import jax.numpy as jnp
from jax import lax
from jax.experimental import pallas as pl
from jax.experimental.pallas import tpu as pltpu
from jax.sharding import PartitionSpec as P

MESH = pl.DeviceIdType.MESH
F32 = jnp.float32
BF16 = jnp.bfloat16
VMEM_ALL = pl.BlockSpec(memory_space=pltpu.VMEM)
HBM_ALL = pl.BlockSpec(memory_space=pltpu.HBM)


def log_two(count):
    return int(math.log2(count) + 0.5)


def mm(lhs, rhs, lhs_dim, rhs_dim):
    return lax.dot_general(lhs, rhs, (((lhs_dim,), (rhs_dim,)), ((), ())), preferred_element_type=F32)


def up_kernel(devs, x_hbm, d_hbm, v_hbm, w0_hbm, b0_hbm, w1_hbm, b1_hbm, w2_hbm, b2_hbm, wu_hbm, bu_hbm, ru_hbm, wt_hbm, rt_hbm, bt_hbm,
              y_dev, near, g0, g1, g2,
              xb, d, v, w0, b0, w1, b1, w2, b2, wu, bu, ru, wt, rt, bt, xh0, xh1, xh2, xt, xsib, xchip, xall, x2, x1, x1_sib, y_out, y_all,
              x_sem, d_sem, v_sem, w_sem, wsib_sem, swap_send, swap_recv, out_send, out_recv, top_send, top_recv, back_send, back_recv, pair_send, pair_recv):
    me = lax.axis_index('tree')
    chips = devs // 2
    half_chips = chips // 2
    core = lax.rem(me, 2)
    chip = me // 2
    other = 1 - core
    partner = chip * 2 + other
    leaves, leaf_size, cols = xb.shape
    part = cols // devs
    half = cols // 2
    my_half = chip // half_chips

    barrier = pltpu.get_barrier_semaphore()
    for step in range(1, devs):
        pl.semaphore_signal(barrier, inc=1, device_id={'tree': lax.rem(me + step, devs)}, device_id_type=MESH)

    def load_x(i):
        return pltpu.make_async_copy(x_hbm.at[pl.ds(i * leaf_size, leaf_size)], near.at[i], x_sem.at[i])

    def load_d(i):
        return pltpu.make_async_copy(d_hbm.at[i], d.at[i], d_sem.at[i])

    def load_v(i):
        return pltpu.make_async_copy(v_hbm.at[i], v.at[i], v_sem.at[i])

    def top_slices(hbm, vmem, first, base):
        out = []
        at = 0
        for level in range(first, log_two(devs)):
            count = 2 ** (level - 1)
            start = 2 ** level - 2 ** first + core * count
            out.append(pltpu.make_async_copy(hbm.at[pl.ds(start, count)], vmem.at[pl.ds(at, count)], w_sem.at[base + level]))
            at += count
        return out

    copies = {}
    for k, (name, hbm, vmem) in enumerate([('w0', w0_hbm, w0), ('w1', w1_hbm, w1), ('w2', w2_hbm, w2), ('wu', wu_hbm.at[0], wu.at[0]), ('bu', bu_hbm.at[0], bu), ('ru', ru_hbm.at[0], ru), ('b0', b0_hbm, b0), ('b1', b1_hbm, b1), ('b2', b2_hbm, b2)]):
        copies[name] = pltpu.make_async_copy(hbm, vmem, w_sem.at[k])
    depth = log_two(devs)
    wt_copies = top_slices(wt_hbm, wt, 2, 9)
    rt_copies = top_slices(rt_hbm, rt, 2, 9 + depth)
    bt_copies = top_slices(bt_hbm, bt, 1, 9 + 2 * depth)

    ahead = 4
    for i in range(ahead):
        load_v(i).start()
        load_x(i).start()
    copies['w0'].start()
    copies['w1'].start()

    wsib = pltpu.make_async_remote_copy(wu.at[0], wu.at[1], wsib_sem.at[0], wsib_sem.at[1], device_id={'tree': partner}, device_id_type=MESH)

    for i in range(leaves):
        load_v(i).wait()
        load_x(i).wait()
        if i + ahead < leaves:
            load_v(i + ahead).start()
            load_x(i + ahead).start()
        if i == 1:
            copies['wu'].start()
            copies['w2'].start()
        if i == ahead - 1:
            for name in ('bu', 'b0', 'b1', 'b2'):
                copies[name].start()
            for j in range(leaves):
                load_d(j).start()
            for copy in wt_copies + bt_copies + rt_copies:
                copy.start()
            copies['ru'].start()
        xb[i] = near[i].astype(BF16)
        xh0[i] = mm(v[i], xb[i], 0, 0).astype(BF16)
        if i % 2 == 1:
            n = i // 2
            if n == 0:
                copies['w0'].wait()
            xh1[n] = (mm(w0[2 * n], xh0[2 * n], 0, 0) + mm(w0[2 * n + 1], xh0[2 * n + 1], 0, 0)).astype(BF16)
        if i % 4 == 3:
            n = i // 4
            if n == 0:
                copies['w1'].wait()
                copies['wu'].wait()
                pl.semaphore_wait(barrier, devs - 1)
                wsib.start()
            xh2[n] = (mm(w1[2 * n], xh1[2 * n], 0, 0) + mm(w1[2 * n + 1], xh1[2 * n + 1], 0, 0)).astype(BF16)
    copies['w2'].wait()

    swaps = []
    for k, side in enumerate((other, core)):
        window = pl.ds(pl.multiple_of(side * half, half), half)
        xt[side] = (mm(xh2[0, :, window], w2[0], 0, 0) + mm(xh2[1, :, window], w2[1], 0, 0)).astype(BF16)
        swaps.append(pltpu.make_async_remote_copy(xt.at[side], xsib.at[side], swap_send.at[k], swap_recv.at[k], device_id={'tree': partner}, device_id_type=MESH))
        swaps[-1].start()
    got = [pltpu.make_async_remote_copy(xt.at[core], xsib.at[core], swap_send.at[0], swap_recv.at[0], device_id={'tree': partner}, device_id_type=MESH),
           pltpu.make_async_remote_copy(xt.at[other], xsib.at[other], swap_send.at[1], swap_recv.at[1], device_id={'tree': partner}, device_id_type=MESH)]

    def near_leaf(i):
        load_d(i).wait()
        near[i] = mm(d[i], xb[i], 1, 0)

    near_leaf(0)
    near_leaf(1)
    wsib.wait()
    got[0].wait_recv()
    merged = (mm(xt[core], wu[0], 1, 0) + mm(xsib[core], wu[1], 1, 0)).astype(BF16)
    xchip[...] = merged.reshape(xchip.shape)

    def out_copy(step):
        dest = lax.rem(chip + step, chips)
        slot = lax.rem(chip, half_chips)
        return pltpu.make_async_remote_copy(xchip.at[dest], xall.at[slot, core], out_send.at[step], out_recv.at[slot, core], device_id={'tree': dest * 2 + my_half}, device_id_type=MESH)

    far_first = [half_chips]
    for step in range(half_chips - 1, 0, -1):
        far_first += [step, chips - step]
    for step in far_first:
        out_copy(step).start()

    @pl.when(core != my_half)
    def _():
        out_copy(0).start()

    @pl.when(core == my_half)
    def _():
        xall[lax.rem(chip, half_chips), core] = xchip[chip]

    for i in range(2, leaves):
        near_leaf(i)
    copies['b0'].wait()
    copies['b1'].wait()
    copies['b2'].wait()
    for n in range(leaves):
        g0[n] = mm(b0[n], xh0[n ^ 1], 1, 0)
    for n in range(leaves // 2):
        g1[n] = mm(b1[n], xh1[n ^ 1], 1, 0)
    for n in range(leaves // 4):
        g2[n] = mm(b2[n], xh2[n ^ 1], 1, 0)
    got[1].wait_recv()
    copies['bu'].wait()
    copies['ru'].wait()
    g_dev = mm(bu[...], xsib[...].reshape(cols, -1), 1, 1)
    for copy in wt_copies + bt_copies + rt_copies:
        copy.wait()

    for n in range(half_chips):
        for c in range(2):
            local = jnp.logical_and(core * half_chips + n == chip, core == c)
            landed = pltpu.make_async_remote_copy(xchip.at[0], xall.at[n, c], out_send.at[0], out_recv.at[n, c], device_id={'tree': partner}, device_id_type=MESH)

            @pl.when(jnp.logical_not(local))
            def _():
                landed.wait_recv()

    mine = 2 * part
    levels = [[xall[n].reshape(mine, -1) for n in range(half_chips)]]
    at = [0]
    for level in range(depth - 1, 1, -1):
        at.append(0)
    w_at = {}
    pos = 0
    for level in range(2, depth):
        w_at[level] = pos
        pos += 2 ** (level - 1)
    b_at = {}
    pos = 0
    for level in range(1, depth):
        b_at[level] = pos
        pos += 2 ** (level - 1)
    for level in range(depth - 1, 1, -1):
        below = levels[-1]
        base = w_at[level]
        levels.append([(mm(below[2 * q], wt[base + 2 * q], 1, 0) + mm(below[2 * q + 1], wt[base + 2 * q + 1], 1, 0)).astype(BF16) for q in range(len(below) // 2)])
    x1[...] = levels[-1][0]
    top_swap = pltpu.make_async_remote_copy(x1, x1_sib, top_send.at[0], top_recv.at[0], device_id={'tree': partner}, device_id_type=MESH)
    top_swap.start()
    g_top = {}
    for level in range(depth - 1, 1, -1):
        nodes = levels[depth - 1 - level]
        g_top[level] = [mm(nodes[n ^ 1], bt[b_at[level] + n], 1, 1) for n in range(len(nodes))]
    top_swap.wait()
    y_top = [mm(x1_sib[...], bt[b_at[1]], 1, 1).astype(BF16)]
    for level in range(2, depth):
        y_top = [(g_top[level][n] + mm(y_top[n // 2], rt[w_at[level] + n], 1, 1)).astype(BF16) for n in range(len(g_top[level]))]
    for n in range(half_chips):
        y_out[n] = y_top[n].reshape(y_out.shape[1:])

    def back_copy(n, c):
        dest = core * half_chips + n
        return pltpu.make_async_remote_copy(y_out.at[n, c], y_all.at[c, chip], back_send.at[n, c], back_recv.at[chip], device_id={'tree': dest * 2 + c}, device_id_type=MESH)

    for n in range(half_chips):
        for c in range(2):
            local = jnp.logical_and(core * half_chips + n == chip, core == c)

            @pl.when(jnp.logical_not(local))
            def _():
                back_copy(n, c).start()

            @pl.when(local)
            def _():
                y_all[c, chip] = y_out[n, c]

    for j in range(chips):
        landed = pltpu.make_async_remote_copy(y_out.at[0, 0], y_all.at[core, j], back_send.at[0, 0], back_recv.at[j], device_id={'tree': partner}, device_id_type=MESH)

        @pl.when(jnp.logical_or(j != chip, core != my_half))
        def _():
            landed.wait_recv()

    pair = pltpu.make_async_remote_copy(y_all.at[core], y_all.at[core], pair_send.at[0], pair_recv.at[0], device_id={'tree': partner}, device_id_type=MESH)
    pair.start()
    pltpu.make_async_remote_copy(y_all.at[other], y_all.at[other], pair_send.at[0], pair_recv.at[0], device_id={'tree': partner}, device_id_type=MESH).wait_recv()
    y_dev[...] = (g_dev + mm(ru[...], y_all[...].reshape(cols, -1), 1, 1)).astype(BF16)

    for swap in swaps:
        swap.wait_send()
    for step in far_first:
        out_copy(step).wait_send()

    @pl.when(core != my_half)
    def _():
        out_copy(0).wait_send()

    for n in range(half_chips):
        for c in range(2):
            local = jnp.logical_and(core * half_chips + n == chip, core == c)

            @pl.when(jnp.logical_not(local))
            def _():
                back_copy(n, c).wait_send()

    pair.wait_send()


def down_kernel(y_dev, near, g0, g1, g2, r0, r1, r2, u, out_hbm, y2, y1, stage, out_sem):
    leaves, leaf_size, cols = stage.shape

    def store(i):
        return pltpu.make_async_copy(stage.at[i], out_hbm.at[pl.ds(i * leaf_size, leaf_size)], out_sem.at[i])

    for i in range(leaves):
        if i % 4 == 0:
            y2[i // 4] = (g2[i // 4] + mm(r2[i // 4], y_dev[...], 1, 0)).astype(BF16)
        if i % 2 == 0:
            y1[i // 2] = (g1[i // 2] + mm(r1[i // 2], y2[i // 4], 1, 0)).astype(BF16)
        y_leaf = (g0[i] + mm(r0[i], y1[i // 2], 1, 0)).astype(BF16)
        stage[i] = near[i] + mm(u[i], y_leaf, 1, 0)
        store(i).start()
    for i in range(leaves):
        store(i).wait()


def solution(mesh):
    devs = mesh.shape['tree']
    rows_spec = P(('batch', 'tree'), None)
    tree_spec = P('tree', None, None)
    full_spec = P(None, None, None)

    def body(x_loc, d_near, u_leaf, v_leaf, w_h0, r_h0, b_h0, w_h1, r_h1, b_h1, w_h2, r_h2, b_h2, w_upper, r_upper, b_upper, w_top, r_top, b_top):
        leaves, leaf_size, rank0 = u_leaf.shape
        cols = x_loc.shape[1]
        rank1 = w_h0.shape[2]
        rank2 = w_h1.shape[2]
        rank3 = w_h2.shape[2]
        chips = devs // 2
        part = cols // devs
        half = cols // 2
        depth = log_two(devs)
        sds = jax.ShapeDtypeStruct
        dma = pltpu.SemaphoreType.DMA
        vmem = pltpu.VMEM
        outs = [vmem((rank3, cols), BF16), vmem((leaves, leaf_size, cols), F32), vmem((leaves, rank0, cols), F32), vmem((leaves // 2, rank1, cols), F32), vmem((leaves // 4, rank2, cols), F32)]
        half_nodes = chips - 2
        scratch = [
            vmem((leaves, leaf_size, cols), BF16), vmem((leaves, leaf_size, leaf_size), BF16),
            vmem((leaves, leaf_size, rank0), BF16),
            vmem((leaves, rank0, rank1), BF16), vmem((leaves, rank0, rank0), BF16),
            vmem((leaves // 2, rank1, rank2), BF16), vmem((leaves // 2, rank1, rank1), BF16),
            vmem((leaves // 4, rank2, rank3), BF16), vmem((leaves // 4, rank2, rank2), BF16),
            vmem((2, rank3, rank3), BF16), vmem((rank3, rank3), BF16), vmem((rank3, rank3), BF16),
            vmem((half_nodes, rank3, rank3), BF16), vmem((half_nodes, rank3, rank3), BF16), vmem((half_nodes + 1, rank3, rank3), BF16),
            vmem((leaves, rank0, cols), BF16), vmem((leaves // 2, rank1, cols), BF16), vmem((leaves // 4, rank2, cols), BF16),
            vmem((2, half, rank3), BF16), vmem((2, half, rank3), BF16),
            vmem((chips, part, rank3), BF16), vmem((chips // 2, 2, part, rank3), BF16),
            vmem((2, 2 * part, rank3), BF16), vmem((2 * part, rank3), BF16), vmem((2 * part, rank3), BF16),
            vmem((chips // 2, 2, part, rank3), BF16), vmem((2, chips, part, rank3), BF16),
            dma((leaves,)), dma((leaves,)), dma((leaves,)), dma((9 + 3 * depth,)), dma((2,)),
            dma((2,)), dma((2,)), dma((chips,)), dma((chips // 2, 2)), dma((1,)), dma((1,)), dma((chips // 2, 2)), dma((chips,)), dma((1,)), dma((1,)),
        ]
        y_dev, near, g0, g1, g2 = pl.pallas_call(
            functools.partial(up_kernel, devs),
            out_shape=outs,
            in_specs=[HBM_ALL] * 15,
            out_specs=[VMEM_ALL] * 5,
            scratch_shapes=scratch,
            compiler_params=pltpu.CompilerParams(collective_id=0, has_side_effects=True, vmem_limit_bytes=38 * 2 ** 20),
            name='up_top',
        )(*[pltpu.with_memory_space_constraint(a, pltpu.HBM) for a in (x_loc, d_near, v_leaf, w_h0, b_h0, w_h1, b_h1, w_h2, b_h2, w_upper, b_upper, r_upper, w_top, r_top, b_top)])
        return pl.pallas_call(
            down_kernel,
            out_shape=sds(x_loc.shape, F32),
            in_specs=[VMEM_ALL] * 9,
            out_specs=HBM_ALL,
            scratch_shapes=[vmem((leaves // 4, rank2, cols), BF16), vmem((leaves // 2, rank1, cols), BF16), vmem((leaves, leaf_size, cols), F32), dma((leaves,))],
            compiler_params=pltpu.CompilerParams(vmem_limit_bytes=14 * 2 ** 20),
            name='down_out',
        )(*[pltpu.with_memory_space_constraint(a, pltpu.VMEM) for a in (y_dev, near, g0, g1, g2, r_h0, r_h1, r_h2, u_leaf)])

    return jax.shard_map(body, mesh=mesh, in_specs=(rows_spec,) + (tree_spec,) * 15 + (full_spec,) * 3, out_specs=rows_spec, check_vma=False)
```

```python
import functools
import math

import jax
import jax.numpy as jnp
from jax import lax
from jax.experimental import pallas as pl
from jax.experimental.pallas import tpu as pltpu
from jax.sharding import PartitionSpec as P

MESH = pl.DeviceIdType.MESH
F32 = jnp.float32
BF16 = jnp.bfloat16
VMEM_ALL = pl.BlockSpec(memory_space=pltpu.VMEM)
HBM_ALL = pl.BlockSpec(memory_space=pltpu.HBM)


def log_two(count):
    return int(math.log2(count) + 0.5)


def mm(lhs, rhs, lhs_dim, rhs_dim):
    return lax.dot_general(lhs, rhs, (((lhs_dim,), (rhs_dim,)), ((), ())), preferred_element_type=F32)


def up_kernel(devs, chunks, x_hbm, d_hbm, v_hbm, w0_hbm, b0_hbm, w1_hbm, b1_hbm, w2_hbm, b2_hbm, wu_hbm, bu_hbm, ru_hbm, wt_hbm, rt_hbm, bt_hbm, r0_hbm, r1_hbm, r2_hbm, u_hbm,
              y_dev, near, g0, g1, g2, r0, r1, r2, u,
              xb, d, v, w0, b0, w1, b1, w2, b2, wu, bu, ru, wt, rt, bt, xh0, xh1, xh2, xt, xsib, xchip, xall, x1, x1_sib, g_top, g_dev, y_out, y_all,
              x_sem, d_sem, v_sem, w_sem, wsib_sem, swap_send, swap_recv, out_send, out_recv, top_send, top_recv, back_send, back_recv, pair_send, pair_recv):
    me = lax.axis_index('tree')
    chips = devs // 2
    half_chips = chips // 2
    depth = log_two(devs)
    core = lax.rem(me, 2)
    chip = me // 2
    other = 1 - core
    partner = chip * 2 + other
    leaves, leaf_size, cols = xb.shape
    width = cols // chunks
    side_width = width // 2
    part = side_width // chips
    my_half = chip // half_chips
    my_slot = lax.rem(chip, half_chips)

    barrier = pltpu.get_barrier_semaphore()
    for step in range(1, devs):
        pl.semaphore_signal(barrier, inc=1, device_id={'tree': lax.rem(me + step, devs)}, device_id_type=MESH)

    def remote(src, dst, send, recv, dest):
        return pltpu.make_async_remote_copy(src, dst, send, recv, device_id={'tree': dest}, device_id_type=MESH)

    def window(k):
        return pl.ds(k * width, width)

    def load_x(k, i):
        return pltpu.make_async_copy(x_hbm.at[pl.ds(i * leaf_size, leaf_size), window(k)], near.at[i, :, window(k)], x_sem.at[k, i])

    def load_d(i):
        return pltpu.make_async_copy(d_hbm.at[i], d.at[i], d_sem.at[i])

    def load_v(i):
        return pltpu.make_async_copy(v_hbm.at[i], v.at[i], v_sem.at[i])

    copies = {}
    for k, (name, hbm, vmem) in enumerate([('w0', w0_hbm, w0), ('w1', w1_hbm, w1), ('w2', w2_hbm, w2), ('wu', wu_hbm.at[0], wu.at[0]), ('bu', bu_hbm.at[0], bu), ('ru', ru_hbm.at[0], ru), ('b0', b0_hbm, b0), ('b1', b1_hbm, b1), ('b2', b2_hbm, b2), ('r0', r0_hbm, r0), ('r1', r1_hbm, r1), ('r2', r2_hbm, r2), ('u', u_hbm, u)]):
        copies[name] = pltpu.make_async_copy(hbm, vmem, w_sem.at[k])
    base = len(copies)

    def top_slices(hbm, vmem, first, sem):
        out = []
        at = 0
        for level in range(first, depth):
            count = 2 ** (level - 1)
            start = 2 ** level - 2 ** first + core * count
            out.append(pltpu.make_async_copy(hbm.at[pl.ds(start, count)], vmem.at[pl.ds(at, count)], w_sem.at[sem + level]))
            at += count
        return out

    wt_copies = top_slices(wt_hbm, wt, 2, base)
    rt_copies = top_slices(rt_hbm, rt, 2, base + depth)
    bt_copies = top_slices(bt_hbm, bt, 1, base + 2 * depth)
    wsib = remote(wu.at[0], wu.at[1], wsib_sem.at[0], wsib_sem.at[1], partner)

    for i in range(leaves):
        load_v(i).start()
        load_x(0, i).start()
        if i == 1:
            copies['w0'].start()
        if i == 3:
            copies['w1'].start()
            copies['wu'].start()
            copies['w2'].start()

    def up_leaf(k, i):
        if k == 0:
            load_v(i).wait()
        load_x(k, i).wait()
        xb[i, :, window(k)] = near[i, :, window(k)].astype(BF16)
        xh0[i, :, window(k)] = mm(v[i], xb[i, :, window(k)], 0, 0).astype(BF16)
        if i % 2 == 1:
            n = i // 2
            if k == 0 and n == 0:
                copies['w0'].wait()
            xh1[n, :, window(k)] = (mm(w0[2 * n], xh0[2 * n, :, window(k)], 0, 0) + mm(w0[2 * n + 1], xh0[2 * n + 1, :, window(k)], 0, 0)).astype(BF16)
        if i % 4 == 3:
            n = i // 4
            if k == 0 and n == 0:
                copies['w1'].wait()
            xh2[n, :, window(k)] = (mm(w1[2 * n], xh1[2 * n, :, window(k)], 0, 0) + mm(w1[2 * n + 1], xh1[2 * n + 1, :, window(k)], 0, 0)).astype(BF16)

    def swap_copy(k, side, order):
        return remote(xt.at[k, side], xsib.at[k, side], swap_send.at[k, order], swap_recv.at[k, order], partner)

    def swap_start(k):
        for order, side in enumerate((other, core)):
            cut = pl.ds(pl.multiple_of(k * width + side * side_width, side_width), side_width)
            xt[k, side] = (mm(xh2[0, :, cut], w2[0], 0, 0) + mm(xh2[1, :, cut], w2[1], 0, 0)).astype(BF16)
            swap_copy(k, side, order).start()

    def out_copy(k, step):
        dest = lax.rem(chip + step, chips)
        return remote(xchip.at[k, dest], xall.at[k, my_slot, core], out_send.at[k, step], out_recv.at[k, my_slot, core], dest * 2 + my_half)

    far_first = [half_chips]
    for step in range(half_chips - 1, 0, -1):
        far_first += [step, chips - step]

    def merge_send(k):
        swap_copy(k, core, 0).wait_recv()
        merged = (mm(xt[k, core], wu[0], 1, 0) + mm(xsib[k, core], wu[1], 1, 0)).astype(BF16)
        xchip[k] = merged.reshape(chips, part, merged.shape[1])
        for step in far_first:
            out_copy(k, step).start()

        @pl.when(core != my_half)
        def _():
            out_copy(k, 0).start()

        @pl.when(core == my_half)
        def _():
            xall[k, my_slot, core] = xchip[k, chip]

    def near_leaf(i):
        load_d(i).wait()
        near[i] = mm(d[i], xb[i], 1, 0)

    def is_mine(n, c):
        return jnp.logical_and(core * half_chips + n == chip, core == c)

    w_at = {level: 2 ** (level - 1) - 2 for level in range(2, depth)}
    b_at = {level: 2 ** (level - 1) - 1 for level in range(1, depth)}

    def top_solve(k):
        for n in range(half_chips):
            for c in range(2):
                @pl.when(jnp.logical_not(is_mine(n, c)))
                def _():
                    remote(xchip.at[k, 0], xall.at[k, n, c], out_send.at[k, 0], out_recv.at[k, n, c], partner).wait_recv()

        levels = [[xall[k, n].reshape(2 * part, xall.shape[-1]) for n in range(half_chips)]]
        for level in range(depth - 1, 1, -1):
            below = levels[-1]
            at = w_at[level]
            levels.append([(mm(below[2 * q], wt[at + 2 * q], 1, 0) + mm(below[2 * q + 1], wt[at + 2 * q + 1], 1, 0)).astype(BF16) for q in range(len(below) // 2)])
        x1[k] = levels[-1][0]
        swap = remote(x1.at[k], x1_sib.at[k], top_send.at[k], top_recv.at[k], partner)
        swap.start()
        for level in range(2, depth):
            nodes = levels[depth - 1 - level]
            for n in range(len(nodes)):
                g_top[w_at[level] + n] = mm(nodes[n ^ 1], bt[b_at[level] + n], 1, 1)
        swap.wait()
        y_top = [mm(x1_sib[k], bt[0], 1, 1).astype(BF16)]
        for level in range(2, depth):
            y_top = [(g_top[w_at[level] + n] + mm(y_top[n // 2], rt[w_at[level] + n], 1, 1)).astype(BF16) for n in range(2 ** (level - 1))]
        for n in range(half_chips):
            y_out[k, n] = y_top[n].reshape(2, part, y_out.shape[-1])
        for n in range(half_chips):
            for c in range(2):
                @pl.when(jnp.logical_not(is_mine(n, c)))
                def _():
                    back_copy(k, n, c).start()

                @pl.when(is_mine(n, c))
                def _():
                    y_all[k, c, chip] = y_out[k, n, c]

    def back_copy(k, n, c):
        return remote(y_out.at[k, n, c], y_all.at[k, c, chip], back_send.at[k, n, c], back_recv.at[k, chip], (core * half_chips + n) * 2 + c)

    def pair_copy(k, side):
        return remote(y_all.at[k, side], y_all.at[k, side], pair_send.at[k], pair_recv.at[k], partner)

    def back_wait(k):
        for j in range(chips):
            @pl.when(jnp.logical_or(j != chip, core != my_half))
            def _():
                remote(y_out.at[k, 0, 0], y_all.at[k, core, j], back_send.at[k, 0, 0], back_recv.at[k, j], partner).wait_recv()

        pair_copy(k, core).start()

    def finish(k):
        pair_copy(k, other).wait_recv()
        y_dev[:, window(k)] = (g_dev[:, window(k)] + mm(ru[...], y_all[k].reshape(width, y_all.shape[-1]), 1, 1)).astype(BF16)

    with jax.named_scope('s00_for_i_in_range_leaves'):
        for i in range(leaves):
            up_leaf(0, i)
            if i == 2:
                for j in range(leaves):
                    load_x(1, j).start()
            if i == 5:
                copies['wu'].wait()
                pl.semaphore_wait(barrier, devs - 1)
                wsib.start()
    with jax.named_scope('s01_copies_w2_wait'):
        copies['w2'].wait()
    with jax.named_scope('s02_swap_start_0'):
        swap_start(0)
    with jax.named_scope('s03_for_j_in_range_leaves'):
        for j in range(leaves):
            load_d(j).start()
    with jax.named_scope('s04_for_copy_in_wt_copies_bt_cop'):
        for copy in wt_copies + bt_copies + rt_copies:
            copy.start()
    with jax.named_scope('s05_for_name_in_b0_b1_b2_bu_ru_r'):
        for name in ('b0', 'b1', 'b2', 'bu', 'ru', 'r2', 'r1', 'r0', 'u'):
            copies[name].start()
    with jax.named_scope('s06_for_i_in_range_leaves_2'):
        for i in range(leaves // 2):
            up_leaf(1, i)
    with jax.named_scope('s07_wsib_wait'):
        wsib.wait()
    with jax.named_scope('s08_merge_send_0'):
        merge_send(0)
    with jax.named_scope('s09_for_i_in_range_leaves_2_leav'):
        for i in range(leaves // 2, leaves):
            up_leaf(1, i)
    with jax.named_scope('s10_swap_start_1'):
        swap_start(1)
    with jax.named_scope('s11_for_i_in_range_2'):
        for i in range(2):
            near_leaf(i)
    with jax.named_scope('s12_merge_send_1'):
        merge_send(1)
    with jax.named_scope('s13_for_i_in_range_2_leaves'):
        for i in range(2, leaves):
            near_leaf(i)
    with jax.named_scope('s14_for_copy_in_wt_copies_bt_cop'):
        for copy in wt_copies + bt_copies + rt_copies:
            copy.wait()
    with jax.named_scope('s15_top_solve_0'):
        top_solve(0)
    with jax.named_scope('s16_top_solve_1'):
        top_solve(1)
    with jax.named_scope('s17_for_name_in_b0_b1_b2_bu_ru_r'):
        for name in ('b0', 'b1', 'b2', 'bu', 'ru', 'r2', 'r1', 'r0', 'u'):
            copies[name].wait()
    with jax.named_scope('s18_for_n_in_range_leaves'):
        for n in range(leaves):
            g0[n] = mm(b0[n], xh0[n ^ 1], 1, 0)
    with jax.named_scope('s19_for_n_in_range_leaves_2'):
        for n in range(leaves // 2):
            g1[n] = mm(b1[n], xh1[n ^ 1], 1, 0)
    with jax.named_scope('s20_for_n_in_range_leaves_4'):
        for n in range(leaves // 4):
            g2[n] = mm(b2[n], xh2[n ^ 1], 1, 0)
    with jax.named_scope('s21_for_k_in_range_chunks'):
        for k in range(chunks):
            swap_copy(k, other, 1).wait_recv()
            g_dev[:, window(k)] = mm(bu[...], xsib[k].reshape(width, xsib.shape[-1]), 1, 1)
    with jax.named_scope('s22_back_wait_0'):
        back_wait(0)
    with jax.named_scope('s23_finish_0'):
        finish(0)
    with jax.named_scope('s24_back_wait_1'):
        back_wait(1)
    with jax.named_scope('s25_finish_1'):
        finish(1)

    with jax.named_scope('s26_for_k_in_range_chunks'):
        for k in range(chunks):
            swap_copy(k, other, 0).wait_send()
            swap_copy(k, core, 1).wait_send()
            for step in far_first:
                out_copy(k, step).wait_send()

            @pl.when(core != my_half)
            def _():
                out_copy(k, 0).wait_send()

            for n in range(half_chips):
                for c in range(2):
                    @pl.when(jnp.logical_not(is_mine(n, c)))
                    def _():
                        back_copy(k, n, c).wait_send()

            pair_copy(k, core).wait_send()


def down_kernel(y_dev, near, g0, g1, g2, r0, r1, r2, u, out_hbm, y2, y1, stage, out_sem):
    leaves, leaf_size, cols = stage.shape

    def store(i):
        return pltpu.make_async_copy(stage.at[i], out_hbm.at[pl.ds(i * leaf_size, leaf_size)], out_sem.at[i])

    for i in range(leaves):
        if i % 4 == 0:
            y2[i // 4] = (g2[i // 4] + mm(r2[i // 4], y_dev[...], 1, 0)).astype(BF16)
        if i % 2 == 0:
            y1[i // 2] = (g1[i // 2] + mm(r1[i // 2], y2[i // 4], 1, 0)).astype(BF16)
        y_leaf = (g0[i] + mm(r0[i], y1[i // 2], 1, 0)).astype(BF16)
        stage[i] = near[i] + mm(u[i], y_leaf, 1, 0)
        store(i).start()
    for i in range(leaves):
        store(i).wait()


def solution(mesh):
    devs = mesh.shape['tree']
    rows_spec = P(('batch', 'tree'), None)
    tree_spec = P('tree', None, None)
    full_spec = P(None, None, None)

    def body(x_loc, d_near, u_leaf, v_leaf, w_h0, r_h0, b_h0, w_h1, r_h1, b_h1, w_h2, r_h2, b_h2, w_upper, r_upper, b_upper, w_top, r_top, b_top):
        leaves, leaf_size, rank0 = u_leaf.shape
        cols = x_loc.shape[1]
        rank1 = w_h0.shape[2]
        rank2 = w_h1.shape[2]
        rank3 = w_h2.shape[2]
        chips = devs // 2
        chunks = 2
        width = cols // chunks
        part = cols // (chunks * devs)
        depth = log_two(devs)
        sds = jax.ShapeDtypeStruct
        dma = pltpu.SemaphoreType.DMA
        vmem = pltpu.VMEM
        outs = [vmem((rank3, cols), BF16), vmem((leaves, leaf_size, cols), F32), vmem((leaves, rank0, cols), F32), vmem((leaves // 2, rank1, cols), F32), vmem((leaves // 4, rank2, cols), F32)] + [vmem(a.shape, BF16) for a in (r_h0, r_h1, r_h2, u_leaf)]
        half_nodes = chips - 2
        scratch = [
            vmem((leaves, leaf_size, cols), BF16), vmem((leaves, leaf_size, leaf_size), BF16),
            vmem((leaves, leaf_size, rank0), BF16),
            vmem((leaves, rank0, rank1), BF16), vmem((leaves, rank0, rank0), BF16),
            vmem((leaves // 2, rank1, rank2), BF16), vmem((leaves // 2, rank1, rank1), BF16),
            vmem((leaves // 4, rank2, rank3), BF16), vmem((leaves // 4, rank2, rank2), BF16),
            vmem((2, rank3, rank3), BF16), vmem((rank3, rank3), BF16), vmem((rank3, rank3), BF16),
            vmem((half_nodes, rank3, rank3), BF16), vmem((half_nodes, rank3, rank3), BF16), vmem((half_nodes + 1, rank3, rank3), BF16),
            vmem((leaves, rank0, cols), BF16), vmem((leaves // 2, rank1, cols), BF16), vmem((leaves // 4, rank2, cols), BF16),
            vmem((chunks, 2, width // 2, rank3), BF16), vmem((chunks, 2, width // 2, rank3), BF16),
            vmem((chunks, chips, part, rank3), BF16), vmem((chunks, chips // 2, 2, part, rank3), BF16),
            vmem((chunks, 2 * part, rank3), BF16), vmem((chunks, 2 * part, rank3), BF16), vmem((half_nodes, 2 * part, rank3), F32), vmem((rank3, cols), F32),
            vmem((chunks, chips // 2, 2, part, rank3), BF16), vmem((chunks, 2, chips, part, rank3), BF16),
            dma((chunks, leaves)), dma((leaves,)), dma((leaves,)), dma((13 + 3 * depth,)), dma((2,)),
            dma((chunks, 2)), dma((chunks, 2)), dma((chunks, chips)), dma((chunks, chips // 2, 2)), dma((chunks,)), dma((chunks,)),
            dma((chunks, chips // 2, 2)), dma((chunks, chips)), dma((chunks,)), dma((chunks,)),
        ]
        held = pl.pallas_call(
            functools.partial(up_kernel, devs, chunks),
            out_shape=outs,
            in_specs=[HBM_ALL] * 19,
            out_specs=[VMEM_ALL] * 9,
            scratch_shapes=scratch,
            compiler_params=pltpu.CompilerParams(collective_id=0, has_side_effects=True, vmem_limit_bytes=38 * 2 ** 20),
            name='up_top',
        )(*[pltpu.with_memory_space_constraint(a, pltpu.HBM) for a in (x_loc, d_near, v_leaf, w_h0, b_h0, w_h1, b_h1, w_h2, b_h2, w_upper, b_upper, r_upper, w_top, r_top, b_top, r_h0, r_h1, r_h2, u_leaf)])
        return pl.pallas_call(
            down_kernel,
            out_shape=sds(x_loc.shape, F32),
            in_specs=[VMEM_ALL] * 9,
            out_specs=HBM_ALL,
            scratch_shapes=[vmem((leaves // 4, rank2, cols), BF16), vmem((leaves // 2, rank1, cols), BF16), vmem((leaves, leaf_size, cols), F32), dma((leaves,))],
            compiler_params=pltpu.CompilerParams(vmem_limit_bytes=14 * 2 ** 20),
            name='down_out',
        )(*[pltpu.with_memory_space_constraint(a, pltpu.VMEM) for a in held])

    return jax.shard_map(body, mesh=mesh, in_specs=(rows_spec,) + (tree_spec,) * 15 + (full_spec,) * 3, out_specs=rows_spec, check_vma=False)
```

```python
import functools
import math

import jax
import jax.numpy as jnp
from jax import lax
from jax.experimental import pallas as pl
from jax.experimental.pallas import tpu as pltpu
from jax.sharding import PartitionSpec as P

MESH = pl.DeviceIdType.MESH
F32 = jnp.float32
BF16 = jnp.bfloat16
VMEM_ALL = pl.BlockSpec(memory_space=pltpu.VMEM)
HBM_ALL = pl.BlockSpec(memory_space=pltpu.HBM)


def log_two(count):
    return int(math.log2(count) + 0.5)


def mm(lhs, rhs, lhs_dim, rhs_dim):
    return lax.dot_general(lhs, rhs, (((lhs_dim,), (rhs_dim,)), ((), ())), preferred_element_type=F32)


def down_columns(columns, y_dev, near, g0, g1, g2, r0, r1, r2, u, y2, y1, target, after):
    for i in range(near.shape[0]):
        if i % 4 == 0:
            y2[...] = (g2[i // 4, :, columns] + mm(r2[i // 4], y_dev[:, columns], 1, 0)).astype(BF16)
        if i % 2 == 0:
            y1[...] = (g1[i // 2, :, columns] + mm(r1[i // 2], y2[...], 1, 0)).astype(BF16)
        y_leaf = (g0[i, :, columns] + mm(r0[i], y1[...], 1, 0)).astype(BF16)
        target(i)[...] = near[i, :, columns] + mm(u[i], y_leaf, 1, 0)
        if after is not None:
            after(i)


def up_kernel(devs, chunks, x_hbm, d_hbm, v_hbm, w0_hbm, b0_hbm, w1_hbm, b1_hbm, w2_hbm, b2_hbm, wu_hbm, bu_hbm, ru_hbm, wt_hbm, rt_hbm, bt_hbm, r0_hbm, r1_hbm, r2_hbm, u_hbm,
              y_dev, near, g0, g1, g2, r0, r1, r2, u,
              xb, d, v, w0, b0, w1, b1, w2, b2, wu, bu, ru, wt, rt, bt, xh0, xh1, xh2, xt, xsib, xchip, xall, x1, x1_sib, g_top, g_dev, y_out, y_all, y2, y1,
              x_sem, d_sem, v_sem, w_sem, wsib_sem, swap_send, swap_recv, out_send, out_recv, top_send, top_recv, back_send, back_recv, pair_send, pair_recv):
    me = lax.axis_index('tree')
    chips = devs // 2
    half_chips = chips // 2
    depth = log_two(devs)
    core = lax.rem(me, 2)
    chip = me // 2
    other = 1 - core
    partner = chip * 2 + other
    leaves, leaf_size, cols = xb.shape
    width = cols // chunks
    side_width = width // 2
    part = side_width // chips
    my_half = chip // half_chips
    my_slot = lax.rem(chip, half_chips)

    barrier = pltpu.get_barrier_semaphore()
    for step in range(1, devs):
        pl.semaphore_signal(barrier, inc=1, device_id={'tree': lax.rem(me + step, devs)}, device_id_type=MESH)

    def remote(src, dst, send, recv, dest):
        return pltpu.make_async_remote_copy(src, dst, send, recv, device_id={'tree': dest}, device_id_type=MESH)

    def window(k):
        return pl.ds(k * width, width)

    def load_x(k, i):
        return pltpu.make_async_copy(x_hbm.at[pl.ds(i * leaf_size, leaf_size), window(k)], near.at[i, :, window(k)], x_sem.at[k, i])

    def load_d(i):
        return pltpu.make_async_copy(d_hbm.at[i], d.at[i], d_sem.at[i])

    def load_v(i):
        return pltpu.make_async_copy(v_hbm.at[i], v.at[i], v_sem.at[i])

    copies = {}
    for k, (name, hbm, vmem) in enumerate([('w0', w0_hbm, w0), ('w1', w1_hbm, w1), ('w2', w2_hbm, w2), ('wu', wu_hbm.at[0], wu.at[0]), ('bu', bu_hbm.at[0], bu), ('ru', ru_hbm.at[0], ru), ('b0', b0_hbm, b0), ('b1', b1_hbm, b1), ('b2', b2_hbm, b2), ('r0', r0_hbm, r0), ('r1', r1_hbm, r1), ('r2', r2_hbm, r2), ('u', u_hbm, u)]):
        copies[name] = pltpu.make_async_copy(hbm, vmem, w_sem.at[k])
    base = len(copies)

    def top_slices(hbm, vmem, first, sem):
        out = []
        at = 0
        for level in range(first, depth):
            count = 2 ** (level - 1)
            start = 2 ** level - 2 ** first + core * count
            out.append(pltpu.make_async_copy(hbm.at[pl.ds(start, count)], vmem.at[pl.ds(at, count)], w_sem.at[sem + level]))
            at += count
        return out

    wt_copies = top_slices(wt_hbm, wt, 2, base)
    rt_copies = top_slices(rt_hbm, rt, 2, base + depth)
    bt_copies = top_slices(bt_hbm, bt, 1, base + 2 * depth)
    wsib = remote(wu.at[0], wu.at[1], wsib_sem.at[0], wsib_sem.at[1], partner)

    for i in range(leaves):
        load_v(i).start()
        load_x(0, i).start()
        if i == 1:
            copies['w0'].start()
        if i == 3:
            copies['w1'].start()
            copies['wu'].start()
            copies['w2'].start()

    group = leaves // 2

    def pair_of(ref, n, k):
        both = ref[2 * n:2 * n + 2, :, window(k)]
        return both.reshape(both.shape[0] * both.shape[1], width)

    def stacked(ref, n):
        both = ref[2 * n:2 * n + 2]
        return both.reshape(both.shape[0] * both.shape[1], both.shape[2])

    def up_group(k, part_of):
        first = part_of * group
        for i in range(first, first + group):
            if k == 0:
                load_v(i).wait()
            load_x(k, i).wait()
        if k == 0 and part_of == 0:
            copies['w0'].wait()
            copies['w1'].wait()
        for i in range(first, first + group):
            block = near[i, :, window(k)].astype(BF16)
            xb[i, :, window(k)] = block
            xh0[i, :, window(k)] = mm(v[i], block, 0, 0).astype(BF16)
        for n in range(first // 2, (first + group) // 2):
            xh1[n, :, window(k)] = mm(stacked(w0, n), pair_of(xh0, n, k), 0, 0).astype(BF16)
        for n in range(first // 4, (first + group) // 4):
            xh2[n, :, window(k)] = mm(stacked(w1, n), pair_of(xh1, n, k), 0, 0).astype(BF16)

    def swap_copy(k, side, order):
        return remote(xt.at[k, side], xsib.at[k, side], swap_send.at[k, order], swap_recv.at[k, order], partner)

    def swap_start(k):
        for order, side in enumerate((other, core)):
            cut = pl.ds(pl.multiple_of(k * width + side * side_width, side_width), side_width)
            xt[k, side] = (mm(xh2[0, :, cut], w2[0], 0, 0) + mm(xh2[1, :, cut], w2[1], 0, 0)).astype(BF16)
            swap_copy(k, side, order).start()

    def out_copy(k, step):
        dest = lax.rem(chip + step, chips)
        return remote(xchip.at[k, dest], xall.at[k, my_slot, core], out_send.at[k, step], out_recv.at[k, my_slot, core], dest * 2 + my_half)

    far_first = [half_chips]
    for step in range(half_chips - 1, 0, -1):
        far_first += [step, chips - step]

    def merge_send(k):
        swap_copy(k, core, 0).wait_recv()
        merged = (mm(xt[k, core], wu[0], 1, 0) + mm(xsib[k, core], wu[1], 1, 0)).astype(BF16)
        xchip[k] = merged.reshape(chips, part, merged.shape[1])
        for step in far_first:
            out_copy(k, step).start()

        @pl.when(core != my_half)
        def _():
            out_copy(k, 0).start()

        @pl.when(core == my_half)
        def _():
            xall[k, my_slot, core] = xchip[k, chip]

    def near_leaves(first, last):
        for i in range(first, last):
            load_d(i).wait()
        for i in range(first, last):
            near[i] = mm(d[i], xb[i], 1, 0)

    def is_mine(n, c):
        return jnp.logical_and(core * half_chips + n == chip, core == c)

    w_at = {level: 2 ** (level - 1) - 2 for level in range(2, depth)}
    b_at = {level: 2 ** (level - 1) - 1 for level in range(1, depth)}

    def top_solve(k):
        for n in range(half_chips):
            for c in range(2):
                @pl.when(jnp.logical_not(is_mine(n, c)))
                def _():
                    remote(xchip.at[k, 0], xall.at[k, n, c], out_send.at[k, 0], out_recv.at[k, n, c], partner).wait_recv()

        levels = [[xall[k, n].reshape(2 * part, xall.shape[-1]) for n in range(half_chips)]]
        for level in range(depth - 1, 1, -1):
            below = levels[-1]
            at = w_at[level]
            levels.append([(mm(below[2 * q], wt[at + 2 * q], 1, 0) + mm(below[2 * q + 1], wt[at + 2 * q + 1], 1, 0)).astype(BF16) for q in range(len(below) // 2)])
        x1[k] = levels[-1][0]
        swap = remote(x1.at[k], x1_sib.at[k], top_send.at[k], top_recv.at[k], partner)
        swap.start()
        for level in range(2, depth):
            nodes = levels[depth - 1 - level]
            for n in range(len(nodes)):
                g_top[w_at[level] + n] = mm(nodes[n ^ 1], bt[b_at[level] + n], 1, 1)
        swap.wait()
        y_top = [mm(x1_sib[k], bt[0], 1, 1).astype(BF16)]
        for level in range(2, depth):
            y_top = [(g_top[w_at[level] + n] + mm(y_top[n // 2], rt[w_at[level] + n], 1, 1)).astype(BF16) for n in range(2 ** (level - 1))]
        for n in range(half_chips):
            y_out[k, n] = y_top[n].reshape(2, part, y_out.shape[-1])
        for n in range(half_chips):
            for c in range(2):
                @pl.when(jnp.logical_not(is_mine(n, c)))
                def _():
                    back_copy(k, n, c).start()

                @pl.when(is_mine(n, c))
                def _():
                    y_all[k, c, chip] = y_out[k, n, c]

    def back_copy(k, n, c):
        return remote(y_out.at[k, n, c], y_all.at[k, c, chip], back_send.at[k, n, c], back_recv.at[k, chip], (core * half_chips + n) * 2 + c)

    def pair_copy(k, side):
        return remote(y_all.at[k, side], y_all.at[k, side], pair_send.at[k], pair_recv.at[k], partner)

    def back_wait(k):
        for j in range(chips):
            @pl.when(jnp.logical_or(j != chip, core != my_half))
            def _():
                remote(y_out.at[k, 0, 0], y_all.at[k, core, j], back_send.at[k, 0, 0], back_recv.at[k, j], partner).wait_recv()

        pair_copy(k, core).start()

    def finish(k):
        pair_copy(k, other).wait_recv()
        y_dev[:, window(k)] = (g_dev[:, window(k)] + mm(ru[...], y_all[k].reshape(width, y_all.shape[-1]), 1, 1)).astype(BF16)

    with jax.named_scope('s00_up_group_0_0'):
        up_group(0, 0)
    with jax.named_scope('s01_for_j_in_range_leaves'):
        for j in range(leaves):
            load_x(1, j).start()
    with jax.named_scope('s02_copies_wu_wait'):
        copies['wu'].wait()
    with jax.named_scope('s03_pl_semaphore_wait_barrier_de'):
        pl.semaphore_wait(barrier, devs - 1)
    with jax.named_scope('s04_wsib_start'):
        wsib.start()
    with jax.named_scope('s05_up_group_0_1'):
        up_group(0, 1)
    with jax.named_scope('s06_copies_w2_wait'):
        copies['w2'].wait()
    with jax.named_scope('s07_swap_start_0'):
        swap_start(0)
    with jax.named_scope('s08_for_j_in_range_leaves'):
        for j in range(leaves):
            load_d(j).start()
    with jax.named_scope('s09_for_copy_in_wt_copies_bt_cop'):
        for copy in wt_copies + bt_copies + rt_copies:
            copy.start()
    with jax.named_scope('s10_for_name_in_b0_b1_b2_bu_ru_r'):
        for name in ('b0', 'b1', 'b2', 'bu', 'ru', 'r2', 'r1', 'r0', 'u'):
            copies[name].start()
    with jax.named_scope('s11_up_group_1_0'):
        up_group(1, 0)
    with jax.named_scope('s12_wsib_wait'):
        wsib.wait()
    with jax.named_scope('s13_merge_send_0'):
        merge_send(0)
    with jax.named_scope('s14_up_group_1_1'):
        up_group(1, 1)
    with jax.named_scope('s15_swap_start_1'):
        swap_start(1)
    with jax.named_scope('s16_near_leaves_0_3'):
        near_leaves(0, 3)
    with jax.named_scope('s17_merge_send_1'):
        merge_send(1)
    with jax.named_scope('s18_near_leaves_3_leaves'):
        near_leaves(3, leaves)
    with jax.named_scope('s19_for_copy_in_wt_copies_bt_cop'):
        for copy in wt_copies + bt_copies + rt_copies:
            copy.wait()
    with jax.named_scope('s20_top_solve_0'):
        top_solve(0)
    with jax.named_scope('s21_top_solve_1'):
        top_solve(1)
    with jax.named_scope('s22_for_name_in_b0_b1_b2_bu_ru_r'):
        for name in ('b0', 'b1', 'b2', 'bu', 'ru', 'r2', 'r1', 'r0', 'u'):
            copies[name].wait()
    with jax.named_scope('s23_for_k_in_range_chunks'):
        for k in range(chunks):
            swap_copy(k, other, 1).wait_recv()
            g_dev[:, window(k)] = mm(bu[...], xsib[k].reshape(width, xsib.shape[-1]), 1, 1)
    with jax.named_scope('s24_for_n_in_range_leaves_4'):
        for n in range(leaves // 4):
            g2[n] = mm(b2[n], xh2[n ^ 1], 1, 0)
    with jax.named_scope('s25_for_n_in_range_leaves_2'):
        for n in range(leaves // 2):
            g1[n] = mm(b1[n], xh1[n ^ 1], 1, 0)
    with jax.named_scope('s26_back_wait_0'):
        back_wait(0)
    with jax.named_scope('s27_for_n_in_range_leaves'):
        for n in range(leaves):
            g0[n] = mm(b0[n], xh0[n ^ 1], 1, 0)
    with jax.named_scope('s28_finish_0'):
        finish(0)
    with jax.named_scope('s29_down_columns_window_0_y_dev_'):
        down_columns(window(0), y_dev, near, g0, g1, g2, r0, r1, r2, u, y2, y1, lambda i: near.at[i, :, window(0)], None)
    with jax.named_scope('s30_back_wait_1'):
        back_wait(1)
    with jax.named_scope('s31_finish_1'):
        finish(1)

    with jax.named_scope('s32_for_k_in_range_chunks'):
        for k in range(chunks):
            swap_copy(k, other, 0).wait_send()
            swap_copy(k, core, 1).wait_send()
            for step in far_first:
                out_copy(k, step).wait_send()

            @pl.when(core != my_half)
            def _():
                out_copy(k, 0).wait_send()

            for n in range(half_chips):
                for c in range(2):
                    @pl.when(jnp.logical_not(is_mine(n, c)))
                    def _():
                        back_copy(k, n, c).wait_send()

            pair_copy(k, core).wait_send()


def down_kernel(chunks, y_dev, near, g0, g1, g2, r0, r1, r2, u, out_hbm, y2, y1, stage, out_sem):
    leaves, leaf_size, width = stage.shape
    last = pl.ds((chunks - 1) * width, width)
    done = pl.ds(0, (chunks - 1) * width)

    def store(i, src, columns, sem):
        return pltpu.make_async_copy(src, out_hbm.at[pl.ds(i * leaf_size, leaf_size), columns], sem)

    early = [store(i, near.at[i, :, done], done, out_sem.at[0, i]) for i in range(leaves)]
    late = [store(i, stage.at[i], last, out_sem.at[1, i]) for i in range(leaves)]
    for copy in early:
        copy.start()
    down_columns(last, y_dev, near, g0, g1, g2, r0, r1, r2, u, y2, y1, lambda i: stage.at[i], lambda i: late[i].start())
    for copy in early + late:
        copy.wait()


def solution(mesh):
    devs = mesh.shape['tree']
    rows_spec = P(('batch', 'tree'), None)
    tree_spec = P('tree', None, None)
    full_spec = P(None, None, None)

    def body(x_loc, d_near, u_leaf, v_leaf, w_h0, r_h0, b_h0, w_h1, r_h1, b_h1, w_h2, r_h2, b_h2, w_upper, r_upper, b_upper, w_top, r_top, b_top):
        leaves, leaf_size, rank0 = u_leaf.shape
        cols = x_loc.shape[1]
        rank1 = w_h0.shape[2]
        rank2 = w_h1.shape[2]
        rank3 = w_h2.shape[2]
        chips = devs // 2
        chunks = 2
        width = cols // chunks
        part = cols // (chunks * devs)
        depth = log_two(devs)
        sds = jax.ShapeDtypeStruct
        dma = pltpu.SemaphoreType.DMA
        vmem = pltpu.VMEM
        outs = [vmem((rank3, cols), BF16), vmem((leaves, leaf_size, cols), F32), vmem((leaves, rank0, cols), F32), vmem((leaves // 2, rank1, cols), F32), vmem((leaves // 4, rank2, cols), F32)] + [vmem(a.shape, BF16) for a in (r_h0, r_h1, r_h2, u_leaf)]
        half_nodes = chips - 2
        scratch = [
            vmem((leaves, leaf_size, cols), BF16), vmem((leaves, leaf_size, leaf_size), BF16),
            vmem((leaves, leaf_size, rank0), BF16),
            vmem((leaves, rank0, rank1), BF16), vmem((leaves, rank0, rank0), BF16),
            vmem((leaves // 2, rank1, rank2), BF16), vmem((leaves // 2, rank1, rank1), BF16),
            vmem((leaves // 4, rank2, rank3), BF16), vmem((leaves // 4, rank2, rank2), BF16),
            vmem((2, rank3, rank3), BF16), vmem((rank3, rank3), BF16), vmem((rank3, rank3), BF16),
            vmem((half_nodes, rank3, rank3), BF16), vmem((half_nodes, rank3, rank3), BF16), vmem((half_nodes + 1, rank3, rank3), BF16),
            vmem((leaves, rank0, cols), BF16), vmem((leaves // 2, rank1, cols), BF16), vmem((leaves // 4, rank2, cols), BF16),
            vmem((chunks, 2, width // 2, rank3), BF16), vmem((chunks, 2, width // 2, rank3), BF16),
            vmem((chunks, chips, part, rank3), BF16), vmem((chunks, chips // 2, 2, part, rank3), BF16),
            vmem((chunks, 2 * part, rank3), BF16), vmem((chunks, 2 * part, rank3), BF16), vmem((half_nodes, 2 * part, rank3), F32), vmem((rank3, cols), F32),
            vmem((chunks, chips // 2, 2, part, rank3), BF16), vmem((chunks, 2, chips, part, rank3), BF16), vmem((rank2, width), BF16), vmem((rank1, width), BF16),
            dma((chunks, leaves)), dma((leaves,)), dma((leaves,)), dma((13 + 3 * depth,)), dma((2,)),
            dma((chunks, 2)), dma((chunks, 2)), dma((chunks, chips)), dma((chunks, chips // 2, 2)), dma((chunks,)), dma((chunks,)),
            dma((chunks, chips // 2, 2)), dma((chunks, chips)), dma((chunks,)), dma((chunks,)),
        ]
        held = pl.pallas_call(
            functools.partial(up_kernel, devs, chunks),
            out_shape=outs,
            in_specs=[HBM_ALL] * 19,
            out_specs=[VMEM_ALL] * 9,
            scratch_shapes=scratch,
            compiler_params=pltpu.CompilerParams(collective_id=0, has_side_effects=True, vmem_limit_bytes=38 * 2 ** 20),
            name='up_top',
        )(*[pltpu.with_memory_space_constraint(a, pltpu.HBM) for a in (x_loc, d_near, v_leaf, w_h0, b_h0, w_h1, b_h1, w_h2, b_h2, w_upper, b_upper, r_upper, w_top, r_top, b_top, r_h0, r_h1, r_h2, u_leaf)])
        return pl.pallas_call(
            functools.partial(down_kernel, chunks),
            out_shape=sds(x_loc.shape, F32),
            in_specs=[VMEM_ALL] * 9,
            out_specs=HBM_ALL,
            scratch_shapes=[vmem((rank2, width), BF16), vmem((rank1, width), BF16), vmem((leaves, leaf_size, width), F32), dma((2, leaves))],
            compiler_params=pltpu.CompilerParams(vmem_limit_bytes=14 * 2 ** 20),
            name='down_out',
        )(*[pltpu.with_memory_space_constraint(a, pltpu.VMEM) for a in held])

    return jax.shard_map(body, mesh=mesh, in_specs=(rows_spec,) + (tree_spec,) * 15 + (full_spec,) * 3, out_specs=rows_spec, check_vma=False)
```

```python
import functools
import math

import jax
import jax.numpy as jnp
from jax import lax
from jax.experimental import pallas as pl
from jax.experimental.pallas import tpu as pltpu
from jax.sharding import PartitionSpec as P

MESH = pl.DeviceIdType.MESH
F32 = jnp.float32
BF16 = jnp.bfloat16
VMEM_ALL = pl.BlockSpec(memory_space=pltpu.VMEM)
HBM_ALL = pl.BlockSpec(memory_space=pltpu.HBM)


def log_two(count):
    return int(math.log2(count) + 0.5)


def mm(lhs, rhs, lhs_dim, rhs_dim):
    return lax.dot_general(lhs, rhs, (((lhs_dim,), (rhs_dim,)), ((), ())), preferred_element_type=F32)


def down_columns(columns, first, last, y_dev, near, g0, g1, g2, r0, r1, r2, u, y2, y1, target, after):
    for n in range(first // 4, last // 4):
        y2[n] = (g2[n, :, columns] + mm(r2[n], y_dev[:, columns], 1, 0)).astype(BF16)
    for n in range(first // 2, last // 2):
        y1[n] = (g1[n, :, columns] + mm(r1[n], y2[n // 2], 1, 0)).astype(BF16)
    for i in range(first, last):
        y_leaf = (g0[i, :, columns] + mm(r0[i], y1[i // 2], 1, 0)).astype(BF16)
        target(i)[...] = near[i, :, columns] + mm(u[i], y_leaf, 1, 0)
        if after is not None:
            after(i)


def up_kernel(devs, chunks, x_hbm, d_hbm, v_hbm, w0_hbm, b0_hbm, w1_hbm, b1_hbm, w2_hbm, b2_hbm, wu_hbm, bu_hbm, ru_hbm, wt_hbm, rt_hbm, bt_hbm, r0_hbm, r1_hbm, r2_hbm, u_hbm,
              y_dev, near, g0, g1, g2, r0, r1, r2, u,
              xb, d, v, w0, b0, w1, b1, w2, b2, wu, bu, ru, wt, rt, bt, xh0, xh1, xh2, xt, xsib, xchip, xall, x1, x1_sib, g_top, g_dev, y_out, y_all, y2, y1,
              x_sem, d_sem, v_sem, w_sem, wsib_sem, swap_send, swap_recv, out_send, out_recv, top_send, top_recv, back_send, back_recv, pair_send, pair_recv):
    me = lax.axis_index('tree')
    chips = devs // 2
    half_chips = chips // 2
    depth = log_two(devs)
    core = lax.rem(me, 2)
    chip = me // 2
    other = 1 - core
    partner = chip * 2 + other
    leaves, leaf_size, cols = xb.shape
    width = cols // chunks
    side_width = width // 2
    part = side_width // chips
    my_half = chip // half_chips
    my_slot = lax.rem(chip, half_chips)

    barrier = pltpu.get_barrier_semaphore()
    for step in range(1, devs):
        pl.semaphore_signal(barrier, inc=1, device_id={'tree': lax.rem(me + step, devs)}, device_id_type=MESH)

    def remote(src, dst, send, recv, dest):
        return pltpu.make_async_remote_copy(src, dst, send, recv, device_id={'tree': dest}, device_id_type=MESH)

    def window(k):
        return pl.ds(k * width, width)

    def load_x(k, i):
        return pltpu.make_async_copy(x_hbm.at[pl.ds(i * leaf_size, leaf_size), window(k)], near.at[i, :, window(k)], x_sem.at[k, i])

    def load_d(i):
        return pltpu.make_async_copy(d_hbm.at[i], d.at[i], d_sem.at[i])

    def load_v(i):
        return pltpu.make_async_copy(v_hbm.at[i], v.at[i], v_sem.at[i])

    copies = {}
    for k, (name, hbm, vmem) in enumerate([('w0', w0_hbm, w0), ('w1', w1_hbm, w1), ('w2', w2_hbm, w2), ('wu', wu_hbm.at[0], wu.at[0]), ('bu', bu_hbm.at[0], bu), ('ru', ru_hbm.at[0], ru), ('b0', b0_hbm, b0), ('b1', b1_hbm, b1), ('b2', b2_hbm, b2), ('r0', r0_hbm, r0), ('r1', r1_hbm, r1), ('r2', r2_hbm, r2), ('u', u_hbm, u)]):
        copies[name] = pltpu.make_async_copy(hbm, vmem, w_sem.at[k])
    base = len(copies)

    def top_slices(hbm, vmem, first, sem):
        out = []
        at = 0
        for level in range(first, depth):
            count = 2 ** (level - 1)
            start = 2 ** level - 2 ** first + core * count
            out.append(pltpu.make_async_copy(hbm.at[pl.ds(start, count)], vmem.at[pl.ds(at, count)], w_sem.at[sem + level]))
            at += count
        return out

    wt_copies = top_slices(wt_hbm, wt, 2, base)
    rt_copies = top_slices(rt_hbm, rt, 2, base + depth)
    bt_copies = top_slices(bt_hbm, bt, 1, base + 2 * depth)
    wsib = remote(wu.at[0], wu.at[1], wsib_sem.at[0], wsib_sem.at[1], partner)

    for i in range(leaves):
        load_v(i).start()
        load_x(0, i).start()
        if i == 3:
            copies['wu'].start()
            copies['w0'].start()
    copies['w1'].start()
    copies['w2'].start()
    for i in range(leaves):
        load_x(1, i).start()

    group = leaves // 2

    def pair_of(ref, n, k):
        both = ref[2 * n:2 * n + 2, :, window(k)]
        return both.reshape(both.shape[0] * both.shape[1], width)

    def stacked(ref, n):
        both = ref[2 * n:2 * n + 2]
        return both.reshape(both.shape[0] * both.shape[1], both.shape[2])

    def up_leaves(k, first, last):
        for i in range(first, last):
            if k == 0:
                load_v(i).wait()
            load_x(k, i).wait()
        for i in range(first, last):
            block = near[i, :, window(k)].astype(BF16)
            xb[i, :, window(k)] = block
            xh0[i, :, window(k)] = mm(v[i], block, 0, 0).astype(BF16)

    def up_merges(k):
        for n in range(leaves // 2):
            xh1[n, :, window(k)] = mm(stacked(w0, n), pair_of(xh0, n, k), 0, 0).astype(BF16)
        for n in range(leaves // 4):
            xh2[n, :, window(k)] = mm(stacked(w1, n), pair_of(xh1, n, k), 0, 0).astype(BF16)

    def swap_copy(k, side, order):
        return remote(xt.at[k, side], xsib.at[k, side], swap_send.at[k, order], swap_recv.at[k, order], partner)

    def swap_start(k):
        for order, side in enumerate((other, core)):
            cut = pl.ds(pl.multiple_of(k * width + side * side_width, side_width), side_width)
            both = xh2[:, :, cut]
            xt[k, side] = mm(both.reshape(both.shape[0] * both.shape[1], side_width), w2[...].reshape(both.shape[0] * both.shape[1], w2.shape[2]), 0, 0).astype(BF16)
            swap_copy(k, side, order).start()

    def out_copy(k, step):
        dest = lax.rem(chip + step, chips)
        return remote(xchip.at[k, dest], xall.at[k, my_slot, core], out_send.at[k, step], out_recv.at[k, my_slot, core], dest * 2 + my_half)

    far_first = [half_chips]
    for step in range(half_chips - 1, 0, -1):
        far_first += [step, chips - step]

    def merge_send(k):
        swap_copy(k, core, 0).wait_recv()
        merged = (mm(xt[k, core], wu[0], 1, 0) + mm(xsib[k, core], wu[1], 1, 0)).astype(BF16)
        xchip[k] = merged.reshape(chips, part, merged.shape[1])
        for step in far_first:
            out_copy(k, step).start()

        @pl.when(core != my_half)
        def _():
            out_copy(k, 0).start()

        @pl.when(core == my_half)
        def _():
            xall[k, my_slot, core] = xchip[k, chip]

    def near_leaves(first, last):
        for i in range(first, last):
            load_d(i).wait()
        for i in range(first, last):
            near[i] = mm(d[i], xb[i], 1, 0)

    def is_mine(n, c):
        return jnp.logical_and(core * half_chips + n == chip, core == c)

    w_at = {level: 2 ** (level - 1) - 2 for level in range(2, depth)}
    b_at = {level: 2 ** (level - 1) - 1 for level in range(1, depth)}

    def top_solve(k):
        for n in range(half_chips):
            for c in range(2):
                @pl.when(jnp.logical_not(is_mine(n, c)))
                def _():
                    remote(xchip.at[k, 0], xall.at[k, n, c], out_send.at[k, 0], out_recv.at[k, n, c], partner).wait_recv()

        levels = [[xall[k, n].reshape(2 * part, xall.shape[-1]) for n in range(half_chips)]]
        for level in range(depth - 1, 1, -1):
            below = levels[-1]
            at = w_at[level]
            levels.append([(mm(below[2 * q], wt[at + 2 * q], 1, 0) + mm(below[2 * q + 1], wt[at + 2 * q + 1], 1, 0)).astype(BF16) for q in range(len(below) // 2)])
        x1[k] = levels[-1][0]
        swap = remote(x1.at[k], x1_sib.at[k], top_send.at[k], top_recv.at[k], partner)
        swap.start()
        for level in range(2, depth):
            nodes = levels[depth - 1 - level]
            for n in range(len(nodes)):
                g_top[w_at[level] + n] = mm(nodes[n ^ 1], bt[b_at[level] + n], 1, 1)
        swap.wait()
        y_top = [mm(x1_sib[k], bt[0], 1, 1).astype(BF16)]
        for level in range(2, depth):
            y_top = [(g_top[w_at[level] + n] + mm(y_top[n // 2], rt[w_at[level] + n], 1, 1)).astype(BF16) for n in range(2 ** (level - 1))]
        for n in range(half_chips):
            y_out[k, n] = y_top[n].reshape(2, part, y_out.shape[-1])
        for n in range(half_chips):
            for c in range(2):
                @pl.when(jnp.logical_not(is_mine(n, c)))
                def _():
                    back_copy(k, n, c).start()

                @pl.when(is_mine(n, c))
                def _():
                    y_all[k, c, chip] = y_out[k, n, c]

    def back_copy(k, n, c):
        return remote(y_out.at[k, n, c], y_all.at[k, c, chip], back_send.at[k, n, c], back_recv.at[k, chip], (core * half_chips + n) * 2 + c)

    def pair_copy(k, side):
        return remote(y_all.at[k, side], y_all.at[k, side], pair_send.at[k], pair_recv.at[k], partner)

    def back_wait(k):
        for j in range(chips):
            @pl.when(jnp.logical_or(j != chip, core != my_half))
            def _():
                remote(y_out.at[k, 0, 0], y_all.at[k, core, j], back_send.at[k, 0, 0], back_recv.at[k, j], partner).wait_recv()

        pair_copy(k, core).start()

    def finish(k):
        pair_copy(k, other).wait_recv()
        y_dev[:, window(k)] = (g_dev[:, window(k)] + mm(ru[...], y_all[k].reshape(width, y_all.shape[-1]), 1, 1)).astype(BF16)

    with jax.named_scope('s00_up_leaves_0_0_group'):
        up_leaves(0, 0, group)
    with jax.named_scope('s01_copies_wu_wait'):
        copies['wu'].wait()
    with jax.named_scope('s02_pl_semaphore_wait_barrier_de'):
        pl.semaphore_wait(barrier, devs - 1)
    with jax.named_scope('s03_wsib_start'):
        wsib.start()
    with jax.named_scope('s04_copies_w0_wait'):
        copies['w0'].wait()
    with jax.named_scope('s05_copies_w1_wait'):
        copies['w1'].wait()
    with jax.named_scope('s06_copies_w2_wait'):
        copies['w2'].wait()
    with jax.named_scope('s07_up_leaves_0_group_leaves'):
        up_leaves(0, group, leaves)
    with jax.named_scope('s08_up_merges_0'):
        up_merges(0)
    with jax.named_scope('s09_swap_start_0'):
        swap_start(0)
    with jax.named_scope('s10_for_j_in_range_leaves'):
        for j in range(leaves):
            load_d(j).start()
    with jax.named_scope('s11_for_name_in_b2_b1'):
        for name in ('b2', 'b1'):
            copies[name].start()
    with jax.named_scope('s12_for_copy_in_wt_copies_bt_cop'):
        for copy in wt_copies + bt_copies + rt_copies:
            copy.start()
    with jax.named_scope('s13_for_name_in_bu_b0_ru_r2_r1_r'):
        for name in ('bu', 'b0', 'ru', 'r2', 'r1', 'r0', 'u'):
            copies[name].start()
    with jax.named_scope('s14_up_leaves_1_0_group'):
        up_leaves(1, 0, group)
    with jax.named_scope('s15_wsib_wait'):
        wsib.wait()
    with jax.named_scope('s16_merge_send_0'):
        merge_send(0)
    with jax.named_scope('s17_up_leaves_1_group_leaves'):
        up_leaves(1, group, leaves)
    with jax.named_scope('s18_up_merges_1'):
        up_merges(1)
    with jax.named_scope('s19_swap_start_1'):
        swap_start(1)
    with jax.named_scope('s20_near_leaves_0_3'):
        near_leaves(0, 3)
    with jax.named_scope('s21_merge_send_1'):
        merge_send(1)
    with jax.named_scope('s22_copies_b2_wait'):
        copies['b2'].wait()
    with jax.named_scope('s23_copies_b1_wait'):
        copies['b1'].wait()
    with jax.named_scope('s24_near_leaves_3_leaves'):
        near_leaves(3, leaves)
    with jax.named_scope('s25_for_n_in_range_leaves_4'):
        for n in range(leaves // 4):
            g2[n] = mm(b2[n], xh2[n ^ 1], 1, 0)
    with jax.named_scope('s26_for_n_in_range_leaves_2'):
        for n in range(leaves // 2):
            g1[n] = mm(b1[n], xh1[n ^ 1], 1, 0)
    with jax.named_scope('s27_for_copy_in_wt_copies_bt_cop'):
        for copy in wt_copies + bt_copies + rt_copies:
            copy.wait()
    with jax.named_scope('s28_top_solve_0'):
        top_solve(0)
    with jax.named_scope('s29_top_solve_1'):
        top_solve(1)
    with jax.named_scope('s30_for_name_in_b0_bu_ru_r2_r1_r'):
        for name in ('b0', 'bu', 'ru', 'r2', 'r1', 'r0', 'u'):
            copies[name].wait()
    with jax.named_scope('s31_for_k_in_range_chunks'):
        for k in range(chunks):
            swap_copy(k, other, 1).wait_recv()
    with jax.named_scope('s32_for_k_in_range_chunks'):
        for k in range(chunks):
            g_dev[:, window(k)] = mm(bu[...], xsib[k].reshape(width, xsib.shape[-1]), 1, 1)
    with jax.named_scope('s33_back_wait_0'):
        back_wait(0)
    with jax.named_scope('s34_for_n_in_range_leaves'):
        for n in range(leaves):
            g0[n] = mm(b0[n], xh0[n ^ 1], 1, 0)
    with jax.named_scope('s35_finish_0'):
        finish(0)
    with jax.named_scope('s36_down_columns_window_0_0_grou'):
        down_columns(window(0), 0, group, y_dev, near, g0, g1, g2, r0, r1, r2, u, y2, y1, lambda i: near.at[i, :, window(0)], None)
    with jax.named_scope('s37_back_wait_1'):
        back_wait(1)
    with jax.named_scope('s38_down_columns_window_0_group_'):
        down_columns(window(0), group, leaves, y_dev, near, g0, g1, g2, r0, r1, r2, u, y2, y1, lambda i: near.at[i, :, window(0)], None)
    with jax.named_scope('s39_finish_1'):
        finish(1)

    with jax.named_scope('s40_for_k_in_range_chunks'):
        for k in range(chunks):
            swap_copy(k, other, 0).wait_send()
            swap_copy(k, core, 1).wait_send()
            for step in far_first:
                out_copy(k, step).wait_send()

            @pl.when(core != my_half)
            def _():
                out_copy(k, 0).wait_send()

            for n in range(half_chips):
                for c in range(2):
                    @pl.when(jnp.logical_not(is_mine(n, c)))
                    def _():
                        back_copy(k, n, c).wait_send()

            pair_copy(k, core).wait_send()


def down_kernel(chunks, y_dev, near, g0, g1, g2, r0, r1, r2, u, out_hbm, y2, y1, stage, out_sem):
    leaves, leaf_size, width = stage.shape
    last = pl.ds((chunks - 1) * width, width)
    done = pl.ds(0, (chunks - 1) * width)

    def store(i, src, columns, sem):
        return pltpu.make_async_copy(src, out_hbm.at[pl.ds(i * leaf_size, leaf_size), columns], sem)

    early = [store(i, near.at[i, :, done], done, out_sem.at[0, i]) for i in range(leaves)]
    late = [store(i, stage.at[i], last, out_sem.at[1, i]) for i in range(leaves)]
    for copy in early:
        copy.start()
    down_columns(last, 0, leaves, y_dev, near, g0, g1, g2, r0, r1, r2, u, y2, y1, lambda i: stage.at[i], lambda i: late[i].start())
    for copy in early + late:
        copy.wait()


def solution(mesh):
    devs = mesh.shape['tree']
    rows_spec = P(('batch', 'tree'), None)
    tree_spec = P('tree', None, None)
    full_spec = P(None, None, None)

    def body(x_loc, d_near, u_leaf, v_leaf, w_h0, r_h0, b_h0, w_h1, r_h1, b_h1, w_h2, r_h2, b_h2, w_upper, r_upper, b_upper, w_top, r_top, b_top):
        leaves, leaf_size, rank0 = u_leaf.shape
        cols = x_loc.shape[1]
        rank1 = w_h0.shape[2]
        rank2 = w_h1.shape[2]
        rank3 = w_h2.shape[2]
        chips = devs // 2
        chunks = 2
        width = cols // chunks
        part = cols // (chunks * devs)
        depth = log_two(devs)
        sds = jax.ShapeDtypeStruct
        dma = pltpu.SemaphoreType.DMA
        vmem = pltpu.VMEM
        outs = [vmem((rank3, cols), BF16), vmem((leaves, leaf_size, cols), F32), vmem((leaves, rank0, cols), F32), vmem((leaves // 2, rank1, cols), F32), vmem((leaves // 4, rank2, cols), F32)] + [vmem(a.shape, BF16) for a in (r_h0, r_h1, r_h2, u_leaf)]
        half_nodes = chips - 2
        scratch = [
            vmem((leaves, leaf_size, cols), BF16), vmem((leaves, leaf_size, leaf_size), BF16),
            vmem((leaves, leaf_size, rank0), BF16),
            vmem((leaves, rank0, rank1), BF16), vmem((leaves, rank0, rank0), BF16),
            vmem((leaves // 2, rank1, rank2), BF16), vmem((leaves // 2, rank1, rank1), BF16),
            vmem((leaves // 4, rank2, rank3), BF16), vmem((leaves // 4, rank2, rank2), BF16),
            vmem((2, rank3, rank3), BF16), vmem((rank3, rank3), BF16), vmem((rank3, rank3), BF16),
            vmem((half_nodes, rank3, rank3), BF16), vmem((half_nodes, rank3, rank3), BF16), vmem((half_nodes + 1, rank3, rank3), BF16),
            vmem((leaves, rank0, cols), BF16), vmem((leaves // 2, rank1, cols), BF16), vmem((leaves // 4, rank2, cols), BF16),
            vmem((chunks, 2, width // 2, rank3), BF16), vmem((chunks, 2, width // 2, rank3), BF16),
            vmem((chunks, chips, part, rank3), BF16), vmem((chunks, chips // 2, 2, part, rank3), BF16),
            vmem((chunks, 2 * part, rank3), BF16), vmem((chunks, 2 * part, rank3), BF16), vmem((half_nodes, 2 * part, rank3), F32), vmem((rank3, cols), F32),
            vmem((chunks, chips // 2, 2, part, rank3), BF16), vmem((chunks, 2, chips, part, rank3), BF16), vmem((leaves // 4, rank2, width), BF16), vmem((leaves // 2, rank1, width), BF16),
            dma((chunks, leaves)), dma((leaves,)), dma((leaves,)), dma((13 + 3 * depth,)), dma((2,)),
            dma((chunks, 2)), dma((chunks, 2)), dma((chunks, chips)), dma((chunks, chips // 2, 2)), dma((chunks,)), dma((chunks,)),
            dma((chunks, chips // 2, 2)), dma((chunks, chips)), dma((chunks,)), dma((chunks,)),
        ]
        held = pl.pallas_call(
            functools.partial(up_kernel, devs, chunks),
            out_shape=outs,
            in_specs=[HBM_ALL] * 19,
            out_specs=[VMEM_ALL] * 9,
            scratch_shapes=scratch,
            compiler_params=pltpu.CompilerParams(collective_id=0, has_side_effects=True, vmem_limit_bytes=38 * 2 ** 20),
            name='up_top',
        )(*[pltpu.with_memory_space_constraint(a, pltpu.HBM) for a in (x_loc, d_near, v_leaf, w_h0, b_h0, w_h1, b_h1, w_h2, b_h2, w_upper, b_upper, r_upper, w_top, r_top, b_top, r_h0, r_h1, r_h2, u_leaf)])
        return pl.pallas_call(
            functools.partial(down_kernel, chunks),
            out_shape=sds(x_loc.shape, F32),
            in_specs=[VMEM_ALL] * 9,
            out_specs=HBM_ALL,
            scratch_shapes=[vmem((leaves // 4, rank2, width), BF16), vmem((leaves // 2, rank1, width), BF16), vmem((leaves, leaf_size, width), F32), dma((2, leaves))],
            compiler_params=pltpu.CompilerParams(vmem_limit_bytes=14 * 2 ** 20),
            name='down_out',
        )(*[pltpu.with_memory_space_constraint(a, pltpu.VMEM) for a in held])

    return jax.shard_map(body, mesh=mesh, in_specs=(rows_spec,) + (tree_spec,) * 15 + (full_spec,) * 3, out_specs=rows_spec, check_vma=False)
```

```python
import functools
import math

import jax
import jax.numpy as jnp
from jax import lax
from jax.experimental import pallas as pl
from jax.experimental.pallas import tpu as pltpu
from jax.sharding import PartitionSpec as P

MESH = pl.DeviceIdType.MESH
F32 = jnp.float32
BF16 = jnp.bfloat16
VMEM_ALL = pl.BlockSpec(memory_space=pltpu.VMEM)
HBM_ALL = pl.BlockSpec(memory_space=pltpu.HBM)


def log_two(count):
    return int(math.log2(count) + 0.5)


def mm(lhs, rhs, lhs_dim, rhs_dim):
    return lax.dot_general(lhs, rhs, (((lhs_dim,), (rhs_dim,)), ((), ())), preferred_element_type=F32)


def down_columns(columns, first, last, y_dev, near, g0, g1, g2, r0, r1, r2, u, y2, y1, y0, target, after):
    for n in range(first // 4, last // 4):
        y2[n] = (g2[n, :, columns] + mm(r2[n], y_dev[:, columns], 1, 0)).astype(BF16)
    for n in range(first // 2, last // 2):
        y1[n] = (g1[n, :, columns] + mm(r1[n], y2[n // 2], 1, 0)).astype(BF16)
    for i in range(first, last):
        y0[i] = (g0[i, :, columns] + mm(r0[i], y1[i // 2], 1, 0)).astype(BF16)
    for i in range(first, last):
        target(i)[...] = near[i, :, columns] + mm(u[i], y0[i], 1, 0)
        if after is not None:
            after(i)


def up_kernel(devs, chunks, x_hbm, d_hbm, v_hbm, w0_hbm, b0_hbm, w1_hbm, b1_hbm, w2_hbm, b2_hbm, wu_hbm, bu_hbm, ru_hbm, wt_hbm, rt_hbm, bt_hbm, r0_hbm, r1_hbm, r2_hbm, u_hbm,
              y_dev, near, g0, g1, g2, r0, r1, r2, u,
              xb, d, v, w0, b0, w1, b1, w2, b2, wu, bu, ru, wt, rt, bt, xh0, xh1, xh2, xt, xsib, xchip, xall, x1, x1_sib, g_top, g_dev, y_out, y_all, y2, y1, y0, rt_t, bt_t,
              x_sem, d_sem, v_sem, w_sem, wsib_sem, swap_send, swap_recv, out_send, out_recv, top_send, top_recv, back_send, back_recv, pair_send, pair_recv):
    me = lax.axis_index('tree')
    chips = devs // 2
    half_chips = chips // 2
    depth = log_two(devs)
    core = lax.rem(me, 2)
    chip = me // 2
    other = 1 - core
    partner = chip * 2 + other
    leaves, leaf_size, cols = xb.shape
    width = cols // chunks
    side_width = width // 2
    part = side_width // chips
    my_half = chip // half_chips
    my_slot = lax.rem(chip, half_chips)

    barrier = pltpu.get_barrier_semaphore()
    for step in range(1, devs):
        pl.semaphore_signal(barrier, inc=1, device_id={'tree': lax.rem(me + step, devs)}, device_id_type=MESH)

    def remote(src, dst, send, recv, dest):
        return pltpu.make_async_remote_copy(src, dst, send, recv, device_id={'tree': dest}, device_id_type=MESH)

    def window(k):
        return pl.ds(k * width, width)

    def load_x(k, i):
        return pltpu.make_async_copy(x_hbm.at[pl.ds(i * leaf_size, leaf_size), window(k)], near.at[i, :, window(k)], x_sem.at[k, i])

    def load_d(i):
        return pltpu.make_async_copy(d_hbm.at[i], d.at[i], d_sem.at[i])

    def load_v(i):
        return pltpu.make_async_copy(v_hbm.at[i], v.at[i], v_sem.at[i])

    copies = {}
    for k, (name, hbm, vmem) in enumerate([('w0', w0_hbm, w0), ('w1', w1_hbm, w1), ('w2', w2_hbm, w2), ('wu', wu_hbm.at[0], wu.at[0]), ('bu', bu_hbm.at[0], bu), ('ru', ru_hbm.at[0], ru), ('b0', b0_hbm, b0), ('b1', b1_hbm, b1), ('b2', b2_hbm, b2), ('r0', r0_hbm, r0), ('r1', r1_hbm, r1), ('r2', r2_hbm, r2), ('u', u_hbm, u)]):
        copies[name] = pltpu.make_async_copy(hbm, vmem, w_sem.at[k])
    base = len(copies)

    def top_slices(hbm, vmem, first, sem):
        out = []
        at = 0
        for level in range(first, depth):
            count = 2 ** (level - 1)
            start = 2 ** level - 2 ** first + core * count
            out.append(pltpu.make_async_copy(hbm.at[pl.ds(start, count)], vmem.at[pl.ds(at, count)], w_sem.at[sem + level]))
            at += count
        return out

    wt_copies = top_slices(wt_hbm, wt, 2, base)
    rt_copies = top_slices(rt_hbm, rt, 2, base + depth)
    bt_copies = top_slices(bt_hbm, bt, 1, base + 2 * depth)
    wsib = remote(wu.at[0], wu.at[1], wsib_sem.at[0], wsib_sem.at[1], partner)

    group = leaves // 2
    for i in range(group):
        load_v(i).start()
        load_x(0, i).start()
    copies['wu'].start()
    copies['w0'].start()
    for i in range(group, leaves):
        load_v(i).start()
        load_x(0, i).start()
    copies['w1'].start()
    copies['w2'].start()

    def pair_of(ref, n, k):
        both = ref[2 * n:2 * n + 2, :, window(k)]
        return both.reshape(both.shape[0] * both.shape[1], width)

    def stacked(ref, n):
        both = ref[2 * n:2 * n + 2]
        return both.reshape(both.shape[0] * both.shape[1], both.shape[2])

    def up_leaves(k, first, last):
        for i in range(first, last):
            if k == 0:
                load_v(i).wait()
            load_x(k, i).wait()
        if k == 0 and first == 0:
            for i in range(leaves):
                load_x(1, i).start()
        for i in range(first, last):
            block = near[i, :, window(k)].astype(BF16)
            xb[i, :, window(k)] = block
            xh0[i, :, window(k)] = mm(v[i], block, 0, 0).astype(BF16)

    def up_merges(k):
        for n in range(leaves // 2):
            xh1[n, :, window(k)] = mm(stacked(w0, n), pair_of(xh0, n, k), 0, 0).astype(BF16)
        for n in range(leaves // 4):
            xh2[n, :, window(k)] = mm(stacked(w1, n), pair_of(xh1, n, k), 0, 0).astype(BF16)

    def swap_copy(k, side, order):
        return remote(xt.at[k, side], xsib.at[k, side], swap_send.at[k, order], swap_recv.at[k, order], partner)

    def swap_start(k):
        for order, side in enumerate((other, core)):
            cut = pl.ds(pl.multiple_of(k * width + side * side_width, side_width), side_width)
            both = xh2[:, :, cut]
            xt[k, side] = mm(both.reshape(both.shape[0] * both.shape[1], side_width), w2[...].reshape(both.shape[0] * both.shape[1], w2.shape[2]), 0, 0).astype(BF16)
            swap_copy(k, side, order).start()

    def out_copy(k, step):
        dest = lax.rem(chip + step, chips)
        return remote(xchip.at[k, dest], xall.at[k, my_slot, core], out_send.at[k, step], out_recv.at[k, my_slot, core], dest * 2 + my_half)

    far_first = [half_chips]
    for step in range(half_chips - 1, 0, -1):
        far_first += [step, chips - step]

    def merge_send(k):
        swap_copy(k, core, 0).wait_recv()
        merged = (mm(xt[k, core], wu[0], 1, 0) + mm(xsib[k, core], wu[1], 1, 0)).astype(BF16)
        xchip[k] = merged.reshape(chips, part, merged.shape[1])
        for step in far_first:
            out_copy(k, step).start()

        @pl.when(core != my_half)
        def _():
            out_copy(k, 0).start()

        @pl.when(core == my_half)
        def _():
            xall[k, my_slot, core] = xchip[k, chip]

    def near_leaves(first, last):
        for i in range(first, last):
            load_d(i).wait()
        for i in range(first, last):
            near[i] = mm(d[i], xb[i], 1, 0)

    def is_mine(n, c):
        return jnp.logical_and(core * half_chips + n == chip, core == c)

    w_at = {level: 2 ** (level - 1) - 2 for level in range(2, depth)}
    b_at = {level: 2 ** (level - 1) - 1 for level in range(1, depth)}

    def top_solve(k):
        for n in range(half_chips):
            for c in range(2):
                @pl.when(jnp.logical_not(is_mine(n, c)))
                def _():
                    remote(xchip.at[k, 0], xall.at[k, n, c], out_send.at[k, 0], out_recv.at[k, n, c], partner).wait_recv()

        levels = [[xall[k, n].reshape(2 * part, xall.shape[-1]) for n in range(half_chips)]]
        for level in range(depth - 1, 1, -1):
            below = levels[-1]
            at = w_at[level]
            levels.append([(mm(below[2 * q], wt[at + 2 * q], 1, 0) + mm(below[2 * q + 1], wt[at + 2 * q + 1], 1, 0)).astype(BF16) for q in range(len(below) // 2)])
        x1[k] = levels[-1][0]
        swap = remote(x1.at[k], x1_sib.at[k], top_send.at[k], top_recv.at[k], partner)
        swap.start()
        for level in range(2, depth):
            nodes = levels[depth - 1 - level]
            for n in range(len(nodes)):
                g_top[w_at[level] + n] = mm(nodes[n ^ 1], bt[b_at[level] + n], 1, 1)
        swap.wait()
        y_top = [mm(x1_sib[k], bt_t[...], 1, 0).astype(BF16)]
        for level in range(2, depth):
            y_top = [(g_top[w_at[level] + n] + mm(y_top[n // 2], rt_t[w_at[level] + n], 1, 0)).astype(BF16) for n in range(2 ** (level - 1))]
        for n in range(half_chips):
            y_out[k, n] = y_top[n].reshape(2, part, y_out.shape[-1])
        for n in range(half_chips):
            for c in range(2):
                @pl.when(jnp.logical_not(is_mine(n, c)))
                def _():
                    back_copy(k, n, c).start()

                @pl.when(is_mine(n, c))
                def _():
                    y_all[k, c, chip] = y_out[k, n, c]

    def back_copy(k, n, c):
        return remote(y_out.at[k, n, c], y_all.at[k, c, chip], back_send.at[k, n, c], back_recv.at[k, chip], (core * half_chips + n) * 2 + c)

    def pair_copy(k, side):
        return remote(y_all.at[k, side], y_all.at[k, side], pair_send.at[k], pair_recv.at[k], partner)

    def back_wait(k):
        for j in range(chips):
            @pl.when(jnp.logical_or(j != chip, core != my_half))
            def _():
                remote(y_out.at[k, 0, 0], y_all.at[k, core, j], back_send.at[k, 0, 0], back_recv.at[k, j], partner).wait_recv()

        pair_copy(k, core).start()

    def finish(k):
        pair_copy(k, other).wait_recv()
        y_dev[:, window(k)] = (g_dev[:, window(k)] + mm(ru[...], y_all[k].reshape(width, y_all.shape[-1]), 1, 1)).astype(BF16)

    with jax.named_scope('s00_up_leaves_0_0_group'):
        up_leaves(0, 0, group)
    with jax.named_scope('s01_copies_wu_wait'):
        copies['wu'].wait()
    with jax.named_scope('s02_pl_semaphore_wait_barrier_de'):
        pl.semaphore_wait(barrier, devs - 1)
    with jax.named_scope('s03_wsib_start'):
        wsib.start()
    with jax.named_scope('s04_copies_w0_wait'):
        copies['w0'].wait()
    with jax.named_scope('s05_copies_w1_wait'):
        copies['w1'].wait()
    with jax.named_scope('s06_copies_w2_wait'):
        copies['w2'].wait()
    with jax.named_scope('s07_up_leaves_0_group_leaves'):
        up_leaves(0, group, leaves)
    with jax.named_scope('s08_up_merges_0'):
        up_merges(0)
    with jax.named_scope('s09_swap_start_0'):
        swap_start(0)
    with jax.named_scope('s10_for_j_in_range_leaves'):
        for j in range(leaves):
            load_d(j).start()
    with jax.named_scope('s11_for_copy_in_rt_copies_bt_cop'):
        for copy in rt_copies + bt_copies + wt_copies:
            copy.start()
    with jax.named_scope('s12_for_name_in_b2_b1_bu_b0_ru_r'):
        for name in ('b2', 'b1', 'bu', 'b0', 'ru', 'r2', 'r1', 'r0', 'u'):
            copies[name].start()
    with jax.named_scope('s13_up_leaves_1_0_group'):
        up_leaves(1, 0, group)
    with jax.named_scope('s14_wsib_wait'):
        wsib.wait()
    with jax.named_scope('s15_merge_send_0'):
        merge_send(0)
    with jax.named_scope('s16_up_leaves_1_group_leaves'):
        up_leaves(1, group, leaves)
    with jax.named_scope('s17_up_merges_1'):
        up_merges(1)
    with jax.named_scope('s18_swap_start_1'):
        swap_start(1)
    with jax.named_scope('s19_near_leaves_0_3'):
        near_leaves(0, 3)
    with jax.named_scope('s20_merge_send_1'):
        merge_send(1)
    with jax.named_scope('s21_for_copy_in_bt_copies_rt_cop'):
        for copy in bt_copies + rt_copies:
            copy.wait()
    with jax.named_scope('s22_near_leaves_3_leaves'):
        near_leaves(3, leaves)
    with jax.named_scope('s23_for_n_in_range_rt_shape_0'):
        for n in range(rt.shape[0]):
            rt_t[n] = rt[n].T
    with jax.named_scope('s24_bt_t_bt_0_t'):
        bt_t[...] = bt[0].T
    with jax.named_scope('s25_copies_b2_wait'):
        copies['b2'].wait()
    with jax.named_scope('s26_copies_b1_wait'):
        copies['b1'].wait()
    with jax.named_scope('s27_for_n_in_range_leaves_4'):
        for n in range(leaves // 4):
            g2[n] = mm(b2[n], xh2[n ^ 1], 1, 0)
    with jax.named_scope('s28_for_n_in_range_leaves_2'):
        for n in range(leaves // 2):
            g1[n] = mm(b1[n], xh1[n ^ 1], 1, 0)
    with jax.named_scope('s29_for_copy_in_wt_copies'):
        for copy in wt_copies:
            copy.wait()
    with jax.named_scope('s30_top_solve_0'):
        top_solve(0)
    with jax.named_scope('s31_top_solve_1'):
        top_solve(1)
    with jax.named_scope('s32_for_name_in_b0_bu_ru_r2_r1_r'):
        for name in ('b0', 'bu', 'ru', 'r2', 'r1', 'r0', 'u'):
            copies[name].wait()
    with jax.named_scope('s33_for_k_in_range_chunks'):
        for k in range(chunks):
            swap_copy(k, other, 1).wait_recv()
    with jax.named_scope('s34_for_k_in_range_chunks'):
        for k in range(chunks):
            g_dev[:, window(k)] = mm(bu[...], xsib[k].reshape(width, xsib.shape[-1]), 1, 1)
    with jax.named_scope('s35_back_wait_0'):
        back_wait(0)
    with jax.named_scope('s36_for_n_in_range_leaves'):
        for n in range(leaves):
            g0[n] = mm(b0[n], xh0[n ^ 1], 1, 0)
    with jax.named_scope('s37_finish_0'):
        finish(0)
    with jax.named_scope('s38_down_columns_window_0_0_grou'):
        down_columns(window(0), 0, group, y_dev, near, g0, g1, g2, r0, r1, r2, u, y2, y1, y0, lambda i: near.at[i, :, window(0)], None)
    with jax.named_scope('s39_back_wait_1'):
        back_wait(1)
    with jax.named_scope('s40_down_columns_window_0_group_'):
        down_columns(window(0), group, leaves, y_dev, near, g0, g1, g2, r0, r1, r2, u, y2, y1, y0, lambda i: near.at[i, :, window(0)], None)
    with jax.named_scope('s41_finish_1'):
        finish(1)

    with jax.named_scope('s42_for_k_in_range_chunks'):
        for k in range(chunks):
            swap_copy(k, other, 0).wait_send()
            swap_copy(k, core, 1).wait_send()
            for step in far_first:
                out_copy(k, step).wait_send()

            @pl.when(core != my_half)
            def _():
                out_copy(k, 0).wait_send()

            for n in range(half_chips):
                for c in range(2):
                    @pl.when(jnp.logical_not(is_mine(n, c)))
                    def _():
                        back_copy(k, n, c).wait_send()

            pair_copy(k, core).wait_send()


def down_kernel(chunks, y_dev, near, g0, g1, g2, r0, r1, r2, u, out_hbm, y2, y1, y0, stage, out_sem):
    leaves, leaf_size, width = stage.shape
    last = pl.ds((chunks - 1) * width, width)
    done = pl.ds(0, (chunks - 1) * width)

    def store(i, src, columns, sem):
        return pltpu.make_async_copy(src, out_hbm.at[pl.ds(i * leaf_size, leaf_size), columns], sem)

    early = [store(i, near.at[i, :, done], done, out_sem.at[0, i]) for i in range(leaves)]
    late = [store(i, stage.at[i], last, out_sem.at[1, i]) for i in range(leaves)]
    for copy in early:
        copy.start()
    down_columns(last, 0, leaves, y_dev, near, g0, g1, g2, r0, r1, r2, u, y2, y1, y0, lambda i: stage.at[i], lambda i: late[i].start())
    for copy in early + late:
        copy.wait()


def solution(mesh):
    devs = mesh.shape['tree']
    rows_spec = P(('batch', 'tree'), None)
    tree_spec = P('tree', None, None)
    full_spec = P(None, None, None)

    def body(x_loc, d_near, u_leaf, v_leaf, w_h0, r_h0, b_h0, w_h1, r_h1, b_h1, w_h2, r_h2, b_h2, w_upper, r_upper, b_upper, w_top, r_top, b_top):
        leaves, leaf_size, rank0 = u_leaf.shape
        cols = x_loc.shape[1]
        rank1 = w_h0.shape[2]
        rank2 = w_h1.shape[2]
        rank3 = w_h2.shape[2]
        chips = devs // 2
        chunks = 2
        width = cols // chunks
        part = cols // (chunks * devs)
        depth = log_two(devs)
        sds = jax.ShapeDtypeStruct
        dma = pltpu.SemaphoreType.DMA
        vmem = pltpu.VMEM
        outs = [vmem((rank3, cols), BF16), vmem((leaves, leaf_size, cols), F32), vmem((leaves, rank0, cols), F32), vmem((leaves // 2, rank1, cols), F32), vmem((leaves // 4, rank2, cols), F32)] + [vmem(a.shape, BF16) for a in (r_h0, r_h1, r_h2, u_leaf)]
        half_nodes = chips - 2
        scratch = [
            vmem((leaves, leaf_size, cols), BF16), vmem((leaves, leaf_size, leaf_size), BF16),
            vmem((leaves, leaf_size, rank0), BF16),
            vmem((leaves, rank0, rank1), BF16), vmem((leaves, rank0, rank0), BF16),
            vmem((leaves // 2, rank1, rank2), BF16), vmem((leaves // 2, rank1, rank1), BF16),
            vmem((leaves // 4, rank2, rank3), BF16), vmem((leaves // 4, rank2, rank2), BF16),
            vmem((2, rank3, rank3), BF16), vmem((rank3, rank3), BF16), vmem((rank3, rank3), BF16),
            vmem((half_nodes, rank3, rank3), BF16), vmem((half_nodes, rank3, rank3), BF16), vmem((half_nodes + 1, rank3, rank3), BF16),
            vmem((leaves, rank0, cols), BF16), vmem((leaves // 2, rank1, cols), BF16), vmem((leaves // 4, rank2, cols), BF16),
            vmem((chunks, 2, width // 2, rank3), BF16), vmem((chunks, 2, width // 2, rank3), BF16),
            vmem((chunks, chips, part, rank3), BF16), vmem((chunks, chips // 2, 2, part, rank3), BF16),
            vmem((chunks, 2 * part, rank3), BF16), vmem((chunks, 2 * part, rank3), BF16), vmem((half_nodes, 2 * part, rank3), F32), vmem((rank3, cols), F32),
            vmem((chunks, chips // 2, 2, part, rank3), BF16), vmem((chunks, 2, chips, part, rank3), BF16), vmem((leaves // 4, rank2, width), BF16), vmem((leaves // 2, rank1, width), BF16), vmem((leaves, rank0, width), BF16), vmem((half_nodes, rank3, rank3), BF16), vmem((rank3, rank3), BF16),
            dma((chunks, leaves)), dma((leaves,)), dma((leaves,)), dma((13 + 3 * depth,)), dma((2,)),
            dma((chunks, 2)), dma((chunks, 2)), dma((chunks, chips)), dma((chunks, chips // 2, 2)), dma((chunks,)), dma((chunks,)),
            dma((chunks, chips // 2, 2)), dma((chunks, chips)), dma((chunks,)), dma((chunks,)),
        ]
        held = pl.pallas_call(
            functools.partial(up_kernel, devs, chunks),
            out_shape=outs,
            in_specs=[HBM_ALL] * 19,
            out_specs=[VMEM_ALL] * 9,
            scratch_shapes=scratch,
            compiler_params=pltpu.CompilerParams(collective_id=0, has_side_effects=True, vmem_limit_bytes=40 * 2 ** 20),
            name='up_top',
        )(*[pltpu.with_memory_space_constraint(a, pltpu.HBM) for a in (x_loc, d_near, v_leaf, w_h0, b_h0, w_h1, b_h1, w_h2, b_h2, w_upper, b_upper, r_upper, w_top, r_top, b_top, r_h0, r_h1, r_h2, u_leaf)])
        return pl.pallas_call(
            functools.partial(down_kernel, chunks),
            out_shape=sds(x_loc.shape, F32),
            in_specs=[VMEM_ALL] * 9,
            out_specs=HBM_ALL,
            scratch_shapes=[vmem((leaves // 4, rank2, width), BF16), vmem((leaves // 2, rank1, width), BF16), vmem((leaves, rank0, width), BF16), vmem((leaves, leaf_size, width), F32), dma((2, leaves))],
            compiler_params=pltpu.CompilerParams(vmem_limit_bytes=14 * 2 ** 20),
            name='down_out',
        )(*[pltpu.with_memory_space_constraint(a, pltpu.VMEM) for a in held])

    return jax.shard_map(body, mesh=mesh, in_specs=(rows_spec,) + (tree_spec,) * 15 + (full_spec,) * 3, out_specs=rows_spec, check_vma=False)
```

```python
import functools
import math

import jax
import jax.numpy as jnp
from jax import lax
from jax.experimental import pallas as pl
from jax.experimental.pallas import tpu as pltpu
from jax.sharding import PartitionSpec as P

MESH = pl.DeviceIdType.MESH
F32 = jnp.float32
BF16 = jnp.bfloat16
VMEM_ALL = pl.BlockSpec(memory_space=pltpu.VMEM)
HBM_ALL = pl.BlockSpec(memory_space=pltpu.HBM)


def log_two(count):
    return int(math.log2(count) + 0.5)


def mm(lhs, rhs, lhs_dim, rhs_dim):
    return lax.dot_general(lhs, rhs, (((lhs_dim,), (rhs_dim,)), ((), ())), preferred_element_type=F32)


def down_skeletons(columns, y_dev, g0, g1, g2, r0, r1, r2, y2, y1, y0):
    for n in range(r2.shape[0]):
        y2[n] = (g2[n, :, columns] + mm(r2[n], y_dev[:, columns], 1, 0)).astype(BF16)
    for n in range(r1.shape[0]):
        y1[n] = (g1[n, :, columns] + mm(r1[n], y2[n // 2], 1, 0)).astype(BF16)
    for n in range(r0.shape[0]):
        y0[n] = (g0[n, :, columns] + mm(r0[n], y1[n // 2], 1, 0)).astype(BF16)


def up_kernel(devs, chunks, x_hbm, d_hbm, v_hbm, w0_hbm, b0_hbm, w1_hbm, b1_hbm, w2_hbm, b2_hbm, wu_hbm, bu_hbm, ru_hbm, wt_hbm, rt_hbm, bt_hbm, r0_hbm, r1_hbm, r2_hbm, u_hbm,
              y_dev, near, g0, g1, g2, r0, r1, r2, u,
              xb, d, v, w0, b0, w1, b1, w2, b2, wu, bu, ru, wt, rt, bt, xh0, xh1, xh2, xt, xsib, xchip, xall, x1, x1_sib, g_top, g_dev, y_out, y_all, y2, y1, y0, rt_t, bt_t,
              x_sem, d_sem, v_sem, w_sem, wsib_sem, swap_send, swap_recv, out_send, out_recv, top_send, top_recv, back_send, back_recv, pair_send, pair_recv):
    me = lax.axis_index('tree')
    chips = devs // 2
    half_chips = chips // 2
    depth = log_two(devs)
    core = lax.rem(me, 2)
    chip = me // 2
    other = 1 - core
    partner = chip * 2 + other
    leaves, leaf_size, cols = xb.shape
    width = cols // chunks
    side_width = width // 2
    part = side_width // chips
    my_half = chip // half_chips
    my_slot = lax.rem(chip, half_chips)

    barrier = pltpu.get_barrier_semaphore()
    for step in range(1, devs):
        pl.semaphore_signal(barrier, inc=1, device_id={'tree': lax.rem(me + step, devs)}, device_id_type=MESH)

    def remote(src, dst, send, recv, dest):
        return pltpu.make_async_remote_copy(src, dst, send, recv, device_id={'tree': dest}, device_id_type=MESH)

    def window(k):
        return pl.ds(k * width, width)

    def load_x(k, i):
        return pltpu.make_async_copy(x_hbm.at[pl.ds(i * leaf_size, leaf_size), window(k)], near.at[i, :, window(k)], x_sem.at[k, i])

    def load_d(i):
        return pltpu.make_async_copy(d_hbm.at[i], d.at[i], d_sem.at[i])

    def load_v(i):
        return pltpu.make_async_copy(v_hbm.at[i], v.at[i], v_sem.at[i])

    copies = {}
    for k, (name, hbm, vmem) in enumerate([('w0', w0_hbm, w0), ('w1', w1_hbm, w1), ('w2', w2_hbm, w2), ('wu', wu_hbm.at[0], wu.at[0]), ('bu', bu_hbm.at[0], bu), ('ru', ru_hbm.at[0], ru), ('b0', b0_hbm, b0), ('b1', b1_hbm, b1), ('b2', b2_hbm, b2), ('r0', r0_hbm, r0), ('r1', r1_hbm, r1), ('r2', r2_hbm, r2), ('u', u_hbm, u)]):
        copies[name] = pltpu.make_async_copy(hbm, vmem, w_sem.at[k])
    base = len(copies)

    def top_slices(hbm, vmem, first, sem):
        out = []
        at = 0
        for level in range(first, depth):
            count = 2 ** (level - 1)
            start = 2 ** level - 2 ** first + core * count
            out.append(pltpu.make_async_copy(hbm.at[pl.ds(start, count)], vmem.at[pl.ds(at, count)], w_sem.at[sem + level]))
            at += count
        return out

    wt_copies = top_slices(wt_hbm, wt, 2, base)
    rt_copies = top_slices(rt_hbm, rt, 2, base + depth)
    bt_copies = top_slices(bt_hbm, bt, 1, base + 2 * depth)
    wsib = remote(wu.at[0], wu.at[1], wsib_sem.at[0], wsib_sem.at[1], partner)

    group = leaves // 2
    for i in range(group):
        load_v(i).start()
        load_x(0, i).start()
    copies['wu'].start()
    copies['w0'].start()
    for i in range(group, leaves):
        load_v(i).start()
        load_x(0, i).start()
    copies['w1'].start()
    copies['w2'].start()

    def pair_of(ref, n, k):
        both = ref[2 * n:2 * n + 2, :, window(k)]
        return both.reshape(both.shape[0] * both.shape[1], width)

    def stacked(ref, n):
        both = ref[2 * n:2 * n + 2]
        return both.reshape(both.shape[0] * both.shape[1], both.shape[2])

    def up_leaves(k, first, last):
        for i in range(first, last):
            if k == 0:
                load_v(i).wait()
            load_x(k, i).wait()
        if k == 0 and first == 0:
            for i in range(leaves):
                load_x(1, i).start()
        for i in range(first, last):
            block = near[i, :, window(k)].astype(BF16)
            xb[i, :, window(k)] = block
            xh0[i, :, window(k)] = mm(v[i], block, 0, 0).astype(BF16)

    def up_merges(k):
        for n in range(leaves // 2):
            xh1[n, :, window(k)] = mm(stacked(w0, n), pair_of(xh0, n, k), 0, 0).astype(BF16)
        for n in range(leaves // 4):
            xh2[n, :, window(k)] = mm(stacked(w1, n), pair_of(xh1, n, k), 0, 0).astype(BF16)

    def swap_copy(k, side, order):
        return remote(xt.at[k, side], xsib.at[k, side], swap_send.at[k, order], swap_recv.at[k, order], partner)

    def swap_start(k):
        for order, side in enumerate((other, core)):
            cut = pl.ds(pl.multiple_of(k * width + side * side_width, side_width), side_width)
            both = xh2[:, :, cut]
            xt[k, side] = mm(both.reshape(both.shape[0] * both.shape[1], side_width), w2[...].reshape(both.shape[0] * both.shape[1], w2.shape[2]), 0, 0).astype(BF16)
            swap_copy(k, side, order).start()

    def out_copy(k, step):
        dest = lax.rem(chip + step, chips)
        return remote(xchip.at[k, dest], xall.at[k, my_slot, core], out_send.at[k, step], out_recv.at[k, my_slot, core], dest * 2 + my_half)

    far_first = [half_chips]
    for step in range(half_chips - 1, 0, -1):
        far_first += [step, chips - step]

    def merge_send(k):
        swap_copy(k, core, 0).wait_recv()
        merged = (mm(xt[k, core], wu[0], 1, 0) + mm(xsib[k, core], wu[1], 1, 0)).astype(BF16)
        xchip[k] = merged.reshape(chips, part, merged.shape[1])
        for step in far_first:
            out_copy(k, step).start()

        @pl.when(core != my_half)
        def _():
            out_copy(k, 0).start()

        @pl.when(core == my_half)
        def _():
            xall[k, my_slot, core] = xchip[k, chip]

    def near_leaves(first, last):
        for i in range(first, last):
            load_d(i).wait()
        for i in range(first, last):
            near[i] = mm(d[i], xb[i], 1, 0)

    def is_mine(n, c):
        return jnp.logical_and(core * half_chips + n == chip, core == c)

    w_at = {level: 2 ** (level - 1) - 2 for level in range(2, depth)}
    b_at = {level: 2 ** (level - 1) - 1 for level in range(1, depth)}

    def top_solve(k):
        for n in range(half_chips):
            for c in range(2):
                @pl.when(jnp.logical_not(is_mine(n, c)))
                def _():
                    remote(xchip.at[k, 0], xall.at[k, n, c], out_send.at[k, 0], out_recv.at[k, n, c], partner).wait_recv()

        levels = [[xall[k, n].reshape(2 * part, xall.shape[-1]) for n in range(half_chips)]]
        for level in range(depth - 1, 1, -1):
            below = levels[-1]
            at = w_at[level]
            levels.append([(mm(below[2 * q], wt[at + 2 * q], 1, 0) + mm(below[2 * q + 1], wt[at + 2 * q + 1], 1, 0)).astype(BF16) for q in range(len(below) // 2)])
        x1[k] = levels[-1][0]
        swap = remote(x1.at[k], x1_sib.at[k], top_send.at[k], top_recv.at[k], partner)
        swap.start()
        for level in range(2, depth):
            nodes = levels[depth - 1 - level]
            for n in range(len(nodes)):
                g_top[w_at[level] + n] = mm(nodes[n ^ 1], bt[b_at[level] + n], 1, 1)
        swap.wait()
        y_top = [mm(x1_sib[k], bt_t[...], 1, 0).astype(BF16)]
        for level in range(2, depth):
            y_top = [(g_top[w_at[level] + n] + mm(y_top[n // 2], rt_t[w_at[level] + n], 1, 0)).astype(BF16) for n in range(2 ** (level - 1))]
        for n in range(half_chips):
            y_out[k, n] = y_top[n].reshape(2, part, y_out.shape[-1])
        for n in range(half_chips):
            for c in range(2):
                @pl.when(jnp.logical_not(is_mine(n, c)))
                def _():
                    back_copy(k, n, c).start()

                @pl.when(is_mine(n, c))
                def _():
                    y_all[k, c, chip] = y_out[k, n, c]

    def back_copy(k, n, c):
        return remote(y_out.at[k, n, c], y_all.at[k, c, chip], back_send.at[k, n, c], back_recv.at[k, chip], (core * half_chips + n) * 2 + c)

    def pair_copy(k, side):
        return remote(y_all.at[k, side], y_all.at[k, side], pair_send.at[k], pair_recv.at[k], partner)

    def back_wait(k):
        for j in range(chips):
            @pl.when(jnp.logical_or(j != chip, core != my_half))
            def _():
                remote(y_out.at[k, 0, 0], y_all.at[k, core, j], back_send.at[k, 0, 0], back_recv.at[k, j], partner).wait_recv()

        pair_copy(k, core).start()

    def finish(k):
        pair_copy(k, other).wait_recv()
        y_dev[:, window(k)] = (g_dev[:, window(k)] + mm(ru[...], y_all[k].reshape(width, y_all.shape[-1]), 1, 1)).astype(BF16)

    up_leaves(0, 0, group)
    copies['wu'].wait()
    pl.semaphore_wait(barrier, devs - 1)
    wsib.start()
    copies['w0'].wait()
    copies['w1'].wait()
    copies['w2'].wait()
    up_leaves(0, group, leaves)
    up_merges(0)
    swap_start(0)
    for j in range(leaves):
        load_d(j).start()
    for copy in rt_copies + bt_copies + wt_copies:
        copy.start()
    for name in ('b2', 'b1', 'bu', 'b0', 'ru', 'r2', 'r1', 'r0', 'u'):
        copies[name].start()
    up_leaves(1, 0, group)
    wsib.wait()
    merge_send(0)
    up_leaves(1, group, leaves)
    up_merges(1)
    swap_start(1)
    near_leaves(0, 3)
    merge_send(1)
    for copy in bt_copies + rt_copies:
        copy.wait()
    near_leaves(3, leaves)
    for n in range(rt.shape[0]):
        rt_t[n] = rt[n].T
    bt_t[...] = bt[0].T
    for copy in wt_copies:
        copy.wait()
    top_solve(0)
    top_solve(1)
    for name in ('b2', 'b1', 'b0', 'bu', 'ru', 'r2', 'r1', 'r0', 'u'):
        copies[name].wait()
    for k in range(chunks):
        swap_copy(k, other, 1).wait_recv()
    for k in range(chunks):
        g_dev[:, window(k)] = mm(bu[...], xsib[k].reshape(width, xsib.shape[-1]), 1, 1)
    for n in range(leaves // 4):
        g2[n] = mm(b2[n], xh2[n ^ 1], 1, 0)
    for n in range(leaves // 2):
        g1[n] = mm(b1[n], xh1[n ^ 1], 1, 0)
    back_wait(0)
    for n in range(leaves):
        g0[n] = mm(b0[n], xh0[n ^ 1], 1, 0)
    finish(0)
    down_skeletons(window(0), y_dev, g0, g1, g2, r0, r1, r2, y2, y1, y0)
    back_wait(1)
    for i in range(leaves):
        near[i, :, window(0)] = near[i, :, window(0)] + mm(u[i], y0[i], 1, 0)
    finish(1)

    for k in range(chunks):
        swap_copy(k, other, 0).wait_send()
        swap_copy(k, core, 1).wait_send()
        for step in far_first:
            out_copy(k, step).wait_send()

        @pl.when(core != my_half)
        def _():
            out_copy(k, 0).wait_send()

        for n in range(half_chips):
            for c in range(2):
                @pl.when(jnp.logical_not(is_mine(n, c)))
                def _():
                    back_copy(k, n, c).wait_send()

        pair_copy(k, core).wait_send()


def down_kernel(chunks, y_dev, near, g0, g1, g2, r0, r1, r2, u, out_hbm, y2, y1, y0, stage, out_sem):
    leaves, leaf_size, width = stage.shape
    last = pl.ds((chunks - 1) * width, width)
    done = pl.ds(0, (chunks - 1) * width)

    def store(i, src, columns, sem):
        return pltpu.make_async_copy(src, out_hbm.at[pl.ds(i * leaf_size, leaf_size), columns], sem)

    def early(i):
        return store(i, near.at[i, :, done], done, out_sem.at[0, i])

    def late(i):
        return store(i, stage.at[i], last, out_sem.at[1, i])

    def start_early(i, carry):
        early(i).start()
        return carry

    lax.fori_loop(0, leaves, start_early, 0)
    down_skeletons(last, y_dev, g0, g1, g2, r0, r1, r2, y2, y1, y0)
    for i in range(leaves):
        stage[i] = near[i, :, last] + mm(u[i], y0[i], 1, 0)
        late(i).start()
    for i in range(leaves):
        early(i).wait()
        late(i).wait()


def solution(mesh):
    devs = mesh.shape['tree']
    rows_spec = P(('batch', 'tree'), None)
    tree_spec = P('tree', None, None)
    full_spec = P(None, None, None)

    def body(x_loc, d_near, u_leaf, v_leaf, w_h0, r_h0, b_h0, w_h1, r_h1, b_h1, w_h2, r_h2, b_h2, w_upper, r_upper, b_upper, w_top, r_top, b_top):
        leaves, leaf_size, rank0 = u_leaf.shape
        cols = x_loc.shape[1]
        rank1 = w_h0.shape[2]
        rank2 = w_h1.shape[2]
        rank3 = w_h2.shape[2]
        chips = devs // 2
        chunks = 2
        width = cols // chunks
        part = cols // (chunks * devs)
        depth = log_two(devs)
        sds = jax.ShapeDtypeStruct
        dma = pltpu.SemaphoreType.DMA
        vmem = pltpu.VMEM
        outs = [vmem((rank3, cols), BF16), vmem((leaves, leaf_size, cols), F32), vmem((leaves, rank0, cols), F32), vmem((leaves // 2, rank1, cols), F32), vmem((leaves // 4, rank2, cols), F32)] + [vmem(a.shape, BF16) for a in (r_h0, r_h1, r_h2, u_leaf)]
        half_nodes = chips - 2
        scratch = [
            vmem((leaves, leaf_size, cols), BF16), vmem((leaves, leaf_size, leaf_size), BF16),
            vmem((leaves, leaf_size, rank0), BF16),
            vmem((leaves, rank0, rank1), BF16), vmem((leaves, rank0, rank0), BF16),
            vmem((leaves // 2, rank1, rank2), BF16), vmem((leaves // 2, rank1, rank1), BF16),
            vmem((leaves // 4, rank2, rank3), BF16), vmem((leaves // 4, rank2, rank2), BF16),
            vmem((2, rank3, rank3), BF16), vmem((rank3, rank3), BF16), vmem((rank3, rank3), BF16),
            vmem((half_nodes, rank3, rank3), BF16), vmem((half_nodes, rank3, rank3), BF16), vmem((half_nodes + 1, rank3, rank3), BF16),
            vmem((leaves, rank0, cols), BF16), vmem((leaves // 2, rank1, cols), BF16), vmem((leaves // 4, rank2, cols), BF16),
            vmem((chunks, 2, width // 2, rank3), BF16), vmem((chunks, 2, width // 2, rank3), BF16),
            vmem((chunks, chips, part, rank3), BF16), vmem((chunks, chips // 2, 2, part, rank3), BF16),
            vmem((chunks, 2 * part, rank3), BF16), vmem((chunks, 2 * part, rank3), BF16), vmem((half_nodes, 2 * part, rank3), F32), vmem((rank3, cols), F32),
            vmem((chunks, chips // 2, 2, part, rank3), BF16), vmem((chunks, 2, chips, part, rank3), BF16), vmem((leaves // 4, rank2, width), BF16), vmem((leaves // 2, rank1, width), BF16), vmem((leaves, rank0, width), BF16), vmem((half_nodes, rank3, rank3), BF16), vmem((rank3, rank3), BF16),
            dma((chunks, leaves)), dma((leaves,)), dma((leaves,)), dma((13 + 3 * depth,)), dma((2,)),
            dma((chunks, 2)), dma((chunks, 2)), dma((chunks, chips)), dma((chunks, chips // 2, 2)), dma((chunks,)), dma((chunks,)),
            dma((chunks, chips // 2, 2)), dma((chunks, chips)), dma((chunks,)), dma((chunks,)),
        ]
        held = pl.pallas_call(
            functools.partial(up_kernel, devs, chunks),
            out_shape=outs,
            in_specs=[HBM_ALL] * 19,
            out_specs=[VMEM_ALL] * 9,
            scratch_shapes=scratch,
            compiler_params=pltpu.CompilerParams(collective_id=0, has_side_effects=True, vmem_limit_bytes=40 * 2 ** 20),
            name='up_top',
        )(*[pltpu.with_memory_space_constraint(a, pltpu.HBM) for a in (x_loc, d_near, v_leaf, w_h0, b_h0, w_h1, b_h1, w_h2, b_h2, w_upper, b_upper, r_upper, w_top, r_top, b_top, r_h0, r_h1, r_h2, u_leaf)])
        return pl.pallas_call(
            functools.partial(down_kernel, chunks),
            out_shape=sds(x_loc.shape, F32),
            in_specs=[VMEM_ALL] * 9,
            out_specs=HBM_ALL,
            scratch_shapes=[vmem((leaves // 4, rank2, width), BF16), vmem((leaves // 2, rank1, width), BF16), vmem((leaves, rank0, width), BF16), vmem((leaves, leaf_size, width), F32), dma((2, leaves))],
            compiler_params=pltpu.CompilerParams(vmem_limit_bytes=14 * 2 ** 20),
            name='down_out',
        )(*[pltpu.with_memory_space_constraint(a, pltpu.VMEM) for a in held])

    return jax.shard_map(body, mesh=mesh, in_specs=(rows_spec,) + (tree_spec,) * 15 + (full_spec,) * 3, out_specs=rows_spec, check_vma=False)
```

```python
import functools
import math

import jax
import jax.numpy as jnp
from jax import lax
from jax.experimental import pallas as pl
from jax.experimental.pallas import tpu as pltpu
from jax.sharding import PartitionSpec as P

MESH = pl.DeviceIdType.MESH
F32 = jnp.float32
BF16 = jnp.bfloat16
VMEM_ALL = pl.BlockSpec(memory_space=pltpu.VMEM)
HBM_ALL = pl.BlockSpec(memory_space=pltpu.HBM)


def log_two(count):
    return int(math.log2(count) + 0.5)


def mm(lhs, rhs, lhs_dim, rhs_dim):
    return lax.dot_general(lhs, rhs, (((lhs_dim,), (rhs_dim,)), ((), ())), preferred_element_type=F32)


def down_skeletons(columns, y_dev, g0, g1, g2, r0, r1, r2, y2, y1, y0):
    for n in range(r2.shape[0]):
        y2[n] = (g2[n, :, columns] + mm(r2[n], y_dev[:, columns], 1, 0)).astype(BF16)
    for n in range(r1.shape[0]):
        y1[n] = (g1[n, :, columns] + mm(r1[n], y2[n // 2], 1, 0)).astype(BF16)
    for n in range(r0.shape[0]):
        y0[n] = (g0[n, :, columns] + mm(r0[n], y1[n // 2], 1, 0)).astype(BF16)


def up_kernel(devs, chunks, x_hbm, d_hbm, v_hbm, w0_hbm, b0_hbm, w1_hbm, b1_hbm, w2_hbm, b2_hbm, wu_hbm, bu_hbm, ru_hbm, wt_hbm, rt_hbm, bt_hbm, r0_hbm, r1_hbm, r2_hbm, u_hbm,
              y_dev, near, g0, g1, g2, r0, r1, r2, u,
              xb, d, v, w0, b0, w1, b1, w2, b2, wu, bu, ru, wt, rt, bt, xh0, xh1, xh2, xt, xsib, xchip, xall, x1, x1_sib, g_top, g_dev, y_out, y_all, y2, y1, y0, rt_t, bt_t,
              x_sem, d_sem, v_sem, w_sem, wsib_sem, swap_send, swap_recv, out_send, out_recv, top_send, top_recv, back_send, back_recv, pair_send, pair_recv):
    me = lax.axis_index('tree')
    chips = devs // 2
    half_chips = chips // 2
    depth = log_two(devs)
    core = lax.rem(me, 2)
    chip = me // 2
    other = 1 - core
    partner = chip * 2 + other
    leaves, leaf_size, cols = xb.shape
    width = cols // chunks
    side_width = width // 2
    part = side_width // chips
    my_half = chip // half_chips
    my_slot = lax.rem(chip, half_chips)

    barrier = pltpu.get_barrier_semaphore()
    for step in range(1, devs):
        pl.semaphore_signal(barrier, inc=1, device_id={'tree': lax.rem(me + step, devs)}, device_id_type=MESH)

    def remote(src, dst, send, recv, dest):
        return pltpu.make_async_remote_copy(src, dst, send, recv, device_id={'tree': dest}, device_id_type=MESH)

    def window(k):
        return pl.ds(k * width, width)

    def load_x(k, i):
        return pltpu.make_async_copy(x_hbm.at[pl.ds(i * leaf_size, leaf_size), window(k)], near.at[i, :, window(k)], x_sem.at[k, i])

    def load_d(i):
        return pltpu.make_async_copy(d_hbm.at[i], d.at[i], d_sem.at[i])

    def load_v(i):
        return pltpu.make_async_copy(v_hbm.at[i], v.at[i], v_sem.at[i])

    copies = {}
    for k, (name, hbm, vmem) in enumerate([('w0', w0_hbm, w0), ('w1', w1_hbm, w1), ('w2', w2_hbm, w2), ('wu', wu_hbm.at[0], wu.at[0]), ('bu', bu_hbm.at[0], bu), ('ru', ru_hbm.at[0], ru), ('b0', b0_hbm, b0), ('b1', b1_hbm, b1), ('b2', b2_hbm, b2), ('r0', r0_hbm, r0), ('r1', r1_hbm, r1), ('r2', r2_hbm, r2), ('u', u_hbm, u)]):
        copies[name] = pltpu.make_async_copy(hbm, vmem, w_sem.at[k])
    base = len(copies)

    def top_slices(hbm, vmem, first, sem):
        out = []
        at = 0
        for level in range(first, depth):
            count = 2 ** (level - 1)
            start = 2 ** level - 2 ** first + core * count
            out.append(pltpu.make_async_copy(hbm.at[pl.ds(start, count)], vmem.at[pl.ds(at, count)], w_sem.at[sem + level]))
            at += count
        return out

    wt_copies = top_slices(wt_hbm, wt, 2, base)
    rt_copies = top_slices(rt_hbm, rt, 2, base + depth)
    bt_copies = top_slices(bt_hbm, bt, 1, base + 2 * depth)
    wsib = remote(wu.at[0], wu.at[1], wsib_sem.at[0], wsib_sem.at[1], partner)

    group = leaves // 2
    for i in range(group):
        load_v(i).start()
        load_x(0, i).start()
    copies['wu'].start()
    copies['w0'].start()
    for i in range(group, leaves):
        load_v(i).start()
        load_x(0, i).start()
    copies['w1'].start()
    copies['w2'].start()

    def pair_of(ref, n, k):
        both = ref[2 * n:2 * n + 2, :, window(k)]
        return both.reshape(both.shape[0] * both.shape[1], width)

    def stacked(ref, n):
        both = ref[2 * n:2 * n + 2]
        return both.reshape(both.shape[0] * both.shape[1], both.shape[2])

    def up_leaves(k, first, last):
        for i in range(first, last):
            if k == 0:
                load_v(i).wait()
            load_x(k, i).wait()
        if k == 0 and first == 0:
            for i in range(leaves):
                load_x(1, i).start()
        for i in range(first, last):
            block = near[i, :, window(k)].astype(BF16)
            xb[i, :, window(k)] = block
            xh0[i, :, window(k)] = mm(v[i], block, 0, 0).astype(BF16)

    def up_merges(k):
        for n in range(leaves // 2):
            xh1[n, :, window(k)] = mm(stacked(w0, n), pair_of(xh0, n, k), 0, 0).astype(BF16)
        for n in range(leaves // 4):
            xh2[n, :, window(k)] = mm(stacked(w1, n), pair_of(xh1, n, k), 0, 0).astype(BF16)

    def swap_copy(k, side, order):
        return remote(xt.at[k, side], xsib.at[k, side], swap_send.at[k, order], swap_recv.at[k, order], partner)

    def swap_start(k, order):
        side = (other, core)[order]
        cut = pl.ds(pl.multiple_of(k * width + side * side_width, side_width), side_width)
        both = xh2[:, :, cut]
        xt[k, side] = mm(both.reshape(both.shape[0] * both.shape[1], side_width), w2[...].reshape(both.shape[0] * both.shape[1], w2.shape[2]), 0, 0).astype(BF16)
        swap_copy(k, side, order).start()

    def out_copy(k, step):
        dest = lax.rem(chip + step, chips)
        return remote(xchip.at[k, dest], xall.at[k, my_slot, core], out_send.at[k, step], out_recv.at[k, my_slot, core], dest * 2 + my_half)

    far_first = [half_chips]
    for step in range(half_chips - 1, 0, -1):
        far_first += [step, chips - step]

    def merge_send(k):
        swap_copy(k, core, 0).wait_recv()
        merged = (mm(xt[k, core], wu[0], 1, 0) + mm(xsib[k, core], wu[1], 1, 0)).astype(BF16)
        xchip[k] = merged.reshape(chips, part, merged.shape[1])
        for step in far_first:
            out_copy(k, step).start()

        @pl.when(core != my_half)
        def _():
            out_copy(k, 0).start()

        @pl.when(core == my_half)
        def _():
            xall[k, my_slot, core] = xchip[k, chip]

    def near_leaves(first, last):
        for i in range(first, last):
            load_d(i).wait()
        for i in range(first, last):
            near[i] = mm(d[i], xb[i], 1, 0)

    def is_mine(n, c):
        return jnp.logical_and(core * half_chips + n == chip, core == c)

    w_at = {level: 2 ** (level - 1) - 2 for level in range(2, depth)}
    b_at = {level: 2 ** (level - 1) - 1 for level in range(1, depth)}

    def top_solve(k):
        for n in range(half_chips):
            for c in range(2):
                @pl.when(jnp.logical_not(is_mine(n, c)))
                def _():
                    remote(xchip.at[k, 0], xall.at[k, n, c], out_send.at[k, 0], out_recv.at[k, n, c], partner).wait_recv()

        levels = [[xall[k, n].reshape(2 * part, xall.shape[-1]) for n in range(half_chips)]]
        for level in range(depth - 1, 1, -1):
            below = levels[-1]
            at = w_at[level]
            levels.append([(mm(below[2 * q], wt[at + 2 * q], 1, 0) + mm(below[2 * q + 1], wt[at + 2 * q + 1], 1, 0)).astype(BF16) for q in range(len(below) // 2)])
        x1[k] = levels[-1][0]
        swap = remote(x1.at[k], x1_sib.at[k], top_send.at[k], top_recv.at[k], partner)
        swap.start()
        for level in range(2, depth):
            nodes = levels[depth - 1 - level]
            for n in range(len(nodes)):
                g_top[w_at[level] + n] = mm(nodes[n ^ 1], bt[b_at[level] + n], 1, 1)
        swap.wait()
        y_top = [mm(x1_sib[k], bt_t[...], 1, 0).astype(BF16)]
        for level in range(2, depth):
            y_top = [(g_top[w_at[level] + n] + mm(y_top[n // 2], rt_t[w_at[level] + n], 1, 0)).astype(BF16) for n in range(2 ** (level - 1))]
        for n in range(half_chips):
            y_out[k, n] = y_top[n].reshape(2, part, y_out.shape[-1])
        for n in range(half_chips):
            for c in range(2):
                @pl.when(jnp.logical_not(is_mine(n, c)))
                def _():
                    back_copy(k, n, c).start()

                @pl.when(is_mine(n, c))
                def _():
                    y_all[k, c, chip] = y_out[k, n, c]

    def back_copy(k, n, c):
        return remote(y_out.at[k, n, c], y_all.at[k, c, chip], back_send.at[k, n, c], back_recv.at[k, chip], (core * half_chips + n) * 2 + c)

    def pair_copy(k, side):
        return remote(y_all.at[k, side], y_all.at[k, side], pair_send.at[k], pair_recv.at[k], partner)

    def back_wait(k):
        for j in range(chips):
            @pl.when(jnp.logical_or(j != chip, core != my_half))
            def _():
                remote(y_out.at[k, 0, 0], y_all.at[k, core, j], back_send.at[k, 0, 0], back_recv.at[k, j], partner).wait_recv()

        pair_copy(k, core).start()

    def finish(k):
        pair_copy(k, other).wait_recv()
        y_dev[:, window(k)] = (g_dev[:, window(k)] + mm(ru[...], y_all[k].reshape(width, y_all.shape[-1]), 1, 1)).astype(BF16)

    with jax.named_scope('p0'):
        up_leaves(0, 0, group)
        copies['wu'].wait()
        pl.semaphore_wait(barrier, devs - 1)
        wsib.start()
        copies['w0'].wait()
        copies['w1'].wait()
        copies['w2'].wait()
    with jax.named_scope('p1'):
        up_leaves(0, group, leaves)
        up_merges(0)
        swap_start(0, 0)
    with jax.named_scope('p2'):
        swap_start(0, 1)
    with jax.named_scope('p3'):
        for j in range(leaves):
            load_d(j).start()
        for copy in rt_copies + bt_copies + wt_copies:
            copy.start()
        for name in ('b2', 'b1', 'bu', 'b0', 'ru', 'r2', 'r1', 'r0', 'u'):
            copies[name].start()
    with jax.named_scope('p4'):
        up_leaves(1, 0, group)
        wsib.wait()
    with jax.named_scope('p5'):
        merge_send(0)
    with jax.named_scope('p6'):
        up_leaves(1, group, leaves)
        up_merges(1)
        swap_start(1, 0)
    with jax.named_scope('p7'):
        swap_start(1, 1)
    with jax.named_scope('p8'):
        near_leaves(0, 3)
    with jax.named_scope('p9'):
        merge_send(1)
        for copy in bt_copies + rt_copies:
            copy.wait()
    with jax.named_scope('p10'):
        near_leaves(3, leaves)
        for n in range(rt.shape[0]):
            rt_t[n] = rt[n].T
        bt_t[...] = bt[0].T
        for copy in wt_copies:
            copy.wait()
    with jax.named_scope('p11'):
        top_solve(0)
    with jax.named_scope('p12'):
        top_solve(1)
    with jax.named_scope('p13'):
        for name in ('b2', 'b1', 'b0', 'bu', 'ru', 'r2', 'r1', 'r0', 'u'):
            copies[name].wait()
        for k in range(chunks):
            swap_copy(k, other, 1).wait_recv()
        for k in range(chunks):
            g_dev[:, window(k)] = mm(bu[...], xsib[k].reshape(width, xsib.shape[-1]), 1, 1)
        for n in range(leaves // 4):
            g2[n] = mm(b2[n], xh2[n ^ 1], 1, 0)
        for n in range(leaves // 2):
            g1[n] = mm(b1[n], xh1[n ^ 1], 1, 0)
    with jax.named_scope('p14'):
        back_wait(0)
    with jax.named_scope('p15'):
        for n in range(leaves):
            g0[n] = mm(b0[n], xh0[n ^ 1], 1, 0)
    with jax.named_scope('p16'):
        finish(0)
        down_skeletons(window(0), y_dev, g0, g1, g2, r0, r1, r2, y2, y1, y0)
    with jax.named_scope('p17'):
        back_wait(1)
    with jax.named_scope('p18'):
        for i in range(leaves):
            near[i, :, window(0)] = near[i, :, window(0)] + mm(u[i], y0[i], 1, 0)
    with jax.named_scope('p19'):
        finish(1)

    for k in range(chunks):
        swap_copy(k, other, 0).wait_send()
        swap_copy(k, core, 1).wait_send()
        for step in far_first:
            out_copy(k, step).wait_send()

        @pl.when(core != my_half)
        def _():
            out_copy(k, 0).wait_send()

        for n in range(half_chips):
            for c in range(2):
                @pl.when(jnp.logical_not(is_mine(n, c)))
                def _():
                    back_copy(k, n, c).wait_send()

        pair_copy(k, core).wait_send()


def down_kernel(chunks, y_dev, near, g0, g1, g2, r0, r1, r2, u, out_hbm, y2, y1, y0, stage, out_sem):
    leaves, leaf_size, width = stage.shape
    last = pl.ds((chunks - 1) * width, width)
    done = pl.ds(0, (chunks - 1) * width)

    def store(i, src, columns, sem):
        return pltpu.make_async_copy(src, out_hbm.at[pl.ds(i * leaf_size, leaf_size), columns], sem)

    def early(i):
        return store(i, near.at[i, :, done], done, out_sem.at[0, i])

    def late(i):
        return store(i, stage.at[i], last, out_sem.at[1, i])

    def start_early(i, carry):
        early(i).start()
        return carry

    lax.fori_loop(0, leaves, start_early, 0)
    down_skeletons(last, y_dev, g0, g1, g2, r0, r1, r2, y2, y1, y0)
    for i in range(leaves):
        stage[i] = near[i, :, last] + mm(u[i], y0[i], 1, 0)
        late(i).start()
    for i in range(leaves):
        early(i).wait()
        late(i).wait()


def solution(mesh):
    devs = mesh.shape['tree']
    rows_spec = P(('batch', 'tree'), None)
    tree_spec = P('tree', None, None)
    full_spec = P(None, None, None)

    def body(x_loc, d_near, u_leaf, v_leaf, w_h0, r_h0, b_h0, w_h1, r_h1, b_h1, w_h2, r_h2, b_h2, w_upper, r_upper, b_upper, w_top, r_top, b_top):
        leaves, leaf_size, rank0 = u_leaf.shape
        cols = x_loc.shape[1]
        rank1 = w_h0.shape[2]
        rank2 = w_h1.shape[2]
        rank3 = w_h2.shape[2]
        chips = devs // 2
        chunks = 2
        width = cols // chunks
        part = cols // (chunks * devs)
        depth = log_two(devs)
        sds = jax.ShapeDtypeStruct
        dma = pltpu.SemaphoreType.DMA
        vmem = pltpu.VMEM
        outs = [vmem((rank3, cols), BF16), vmem((leaves, leaf_size, cols), F32), vmem((leaves, rank0, cols), F32), vmem((leaves // 2, rank1, cols), F32), vmem((leaves // 4, rank2, cols), F32)] + [vmem(a.shape, BF16) for a in (r_h0, r_h1, r_h2, u_leaf)]
        half_nodes = chips - 2
        scratch = [
            vmem((leaves, leaf_size, cols), BF16), vmem((leaves, leaf_size, leaf_size), BF16),
            vmem((leaves, leaf_size, rank0), BF16),
            vmem((leaves, rank0, rank1), BF16), vmem((leaves, rank0, rank0), BF16),
            vmem((leaves // 2, rank1, rank2), BF16), vmem((leaves // 2, rank1, rank1), BF16),
            vmem((leaves // 4, rank2, rank3), BF16), vmem((leaves // 4, rank2, rank2), BF16),
            vmem((2, rank3, rank3), BF16), vmem((rank3, rank3), BF16), vmem((rank3, rank3), BF16),
            vmem((half_nodes, rank3, rank3), BF16), vmem((half_nodes, rank3, rank3), BF16), vmem((half_nodes + 1, rank3, rank3), BF16),
            vmem((leaves, rank0, cols), BF16), vmem((leaves // 2, rank1, cols), BF16), vmem((leaves // 4, rank2, cols), BF16),
            vmem((chunks, 2, width // 2, rank3), BF16), vmem((chunks, 2, width // 2, rank3), BF16),
            vmem((chunks, chips, part, rank3), BF16), vmem((chunks, chips // 2, 2, part, rank3), BF16),
            vmem((chunks, 2 * part, rank3), BF16), vmem((chunks, 2 * part, rank3), BF16), vmem((half_nodes, 2 * part, rank3), F32), vmem((rank3, cols), F32),
            vmem((chunks, chips // 2, 2, part, rank3), BF16), vmem((chunks, 2, chips, part, rank3), BF16), vmem((leaves // 4, rank2, width), BF16), vmem((leaves // 2, rank1, width), BF16), vmem((leaves, rank0, width), BF16), vmem((half_nodes, rank3, rank3), BF16), vmem((rank3, rank3), BF16),
            dma((chunks, leaves)), dma((leaves,)), dma((leaves,)), dma((13 + 3 * depth,)), dma((2,)),
            dma((chunks, 2)), dma((chunks, 2)), dma((chunks, chips)), dma((chunks, chips // 2, 2)), dma((chunks,)), dma((chunks,)),
            dma((chunks, chips // 2, 2)), dma((chunks, chips)), dma((chunks,)), dma((chunks,)),
        ]
        held = pl.pallas_call(
            functools.partial(up_kernel, devs, chunks),
            out_shape=outs,
            in_specs=[HBM_ALL] * 19,
            out_specs=[VMEM_ALL] * 9,
            scratch_shapes=scratch,
            compiler_params=pltpu.CompilerParams(collective_id=0, has_side_effects=True, vmem_limit_bytes=40 * 2 ** 20),
            name='up_top',
        )(*[pltpu.with_memory_space_constraint(a, pltpu.HBM) for a in (x_loc, d_near, v_leaf, w_h0, b_h0, w_h1, b_h1, w_h2, b_h2, w_upper, b_upper, r_upper, w_top, r_top, b_top, r_h0, r_h1, r_h2, u_leaf)])
        return pl.pallas_call(
            functools.partial(down_kernel, chunks),
            out_shape=sds(x_loc.shape, F32),
            in_specs=[VMEM_ALL] * 9,
            out_specs=HBM_ALL,
            scratch_shapes=[vmem((leaves // 4, rank2, width), BF16), vmem((leaves // 2, rank1, width), BF16), vmem((leaves, rank0, width), BF16), vmem((leaves, leaf_size, width), F32), dma((2, leaves))],
            compiler_params=pltpu.CompilerParams(vmem_limit_bytes=14 * 2 ** 20),
            name='down_out',
        )(*[pltpu.with_memory_space_constraint(a, pltpu.VMEM) for a in held])

    return jax.shard_map(body, mesh=mesh, in_specs=(rows_spec,) + (tree_spec,) * 15 + (full_spec,) * 3, out_specs=rows_spec, check_vma=False)
```

```python
import functools
import math

import jax
import jax.numpy as jnp
from jax import lax
from jax.experimental import pallas as pl
from jax.experimental.pallas import tpu as pltpu
from jax.sharding import PartitionSpec as P

MESH = pl.DeviceIdType.MESH
F32 = jnp.float32
BF16 = jnp.bfloat16
VMEM_ALL = pl.BlockSpec(memory_space=pltpu.VMEM)
HBM_ALL = pl.BlockSpec(memory_space=pltpu.HBM)


def log_two(count):
    return int(math.log2(count) + 0.5)


def mm(lhs, rhs, lhs_dim, rhs_dim):
    return lax.dot_general(lhs, rhs, (((lhs_dim,), (rhs_dim,)), ((), ())), preferred_element_type=F32)


def down_skeletons(columns, y_dev, g0, g1, g2, r0, r1, r2, y2, y1, y0):
    for n in range(r2.shape[0]):
        y2[n] = (g2[n, :, columns] + mm(r2[n], y_dev[:, columns], 1, 0)).astype(BF16)
    for n in range(r1.shape[0]):
        y1[n] = (g1[n, :, columns] + mm(r1[n], y2[n // 2], 1, 0)).astype(BF16)
    for n in range(r0.shape[0]):
        y0[n] = (g0[n, :, columns] + mm(r0[n], y1[n // 2], 1, 0)).astype(BF16)


def up_kernel(devs, chunks, x_hbm, d_hbm, v_hbm, w0_hbm, b0_hbm, w1_hbm, b1_hbm, w2_hbm, b2_hbm, wu_hbm, bu_hbm, ru_hbm, wt_hbm, rt_hbm, bt_hbm, r0_hbm, r1_hbm, r2_hbm, u_hbm,
              y_dev, near, g0, g1, g2, r0, r1, r2, u,
              xb, d, v, w0, b0, w1, b1, w2, b2, wu, bu, ru, wt, rt, bt, xh0, xh1, xh2, xt, xsib, xchip, xall, x1, x1_sib, g_top, g_dev, y_out, y_all, y2, y1, y0, rt_t, bt_t,
              x_sem, d_sem, v_sem, w_sem, wsib_sem, swap_send, swap_recv, out_send, out_recv, top_send, top_recv, back_send, back_recv, pair_send, pair_recv):
    me = lax.axis_index('tree')
    chips = devs // 2
    half_chips = chips // 2
    depth = log_two(devs)
    core = lax.rem(me, 2)
    chip = me // 2
    other = 1 - core
    partner = chip * 2 + other
    leaves, leaf_size, cols = xb.shape
    width = cols // chunks
    side_width = width // 2
    part = side_width // chips
    my_half = chip // half_chips
    my_slot = lax.rem(chip, half_chips)

    barrier = pltpu.get_barrier_semaphore()
    for step in range(1, devs):
        pl.semaphore_signal(barrier, inc=1, device_id={'tree': lax.rem(me + step, devs)}, device_id_type=MESH)

    def remote(src, dst, send, recv, dest):
        return pltpu.make_async_remote_copy(src, dst, send, recv, device_id={'tree': dest}, device_id_type=MESH)

    def window(k):
        return pl.ds(k * width, width)

    def load_x(k, i):
        return pltpu.make_async_copy(x_hbm.at[pl.ds(i * leaf_size, leaf_size), window(k)], near.at[i, :, window(k)], x_sem.at[k, i])

    def load_d(i):
        return pltpu.make_async_copy(d_hbm.at[i], d.at[i], d_sem.at[i])

    def load_v(i):
        return pltpu.make_async_copy(v_hbm.at[i], v.at[i], v_sem.at[i])

    copies = {}
    for k, (name, hbm, vmem) in enumerate([('w0', w0_hbm, w0), ('w1', w1_hbm, w1), ('w2', w2_hbm, w2), ('wu', wu_hbm.at[0], wu.at[0]), ('bu', bu_hbm.at[0], bu), ('ru', ru_hbm.at[0], ru), ('b0', b0_hbm, b0), ('b1', b1_hbm, b1), ('b2', b2_hbm, b2), ('r0', r0_hbm, r0), ('r1', r1_hbm, r1), ('r2', r2_hbm, r2), ('u', u_hbm, u)]):
        copies[name] = pltpu.make_async_copy(hbm, vmem, w_sem.at[k])
    base = len(copies)

    def top_slices(hbm, vmem, first, sem):
        out = []
        at = 0
        for level in range(first, depth):
            count = 2 ** (level - 1)
            start = 2 ** level - 2 ** first + core * count
            out.append(pltpu.make_async_copy(hbm.at[pl.ds(start, count)], vmem.at[pl.ds(at, count)], w_sem.at[sem + level]))
            at += count
        return out

    wt_copies = top_slices(wt_hbm, wt, 2, base)
    rt_copies = top_slices(rt_hbm, rt, 2, base + depth)
    bt_copies = top_slices(bt_hbm, bt, 1, base + 2 * depth)
    wsib = remote(wu.at[0], wu.at[1], wsib_sem.at[0], wsib_sem.at[1], partner)

    group = leaves // 2

    def load_many(some):
        with jax.named_scope('l'):
            for copy in some:
                copy.start()

    first_half, second_half = range(group), range(group, leaves)
    load_many([load(i) for i in first_half for load in (load_v, lambda i: load_x(0, i))])
    load_many([copies['wu'], copies['w0']])
    load_many([load(i) for i in second_half for load in (load_v, lambda i: load_x(0, i))])
    load_many([copies['w1'], copies['w2']])
    load_many([load_x(1, i) for i in first_half])
    load_many([load_x(1, i) for i in second_half])
    load_many([load_d(i) for i in range(3)])
    load_many([load_d(i) for i in range(3, leaves)])
    load_many(rt_copies + bt_copies)
    load_many(wt_copies)
    load_many([copies[name] for name in ('b2', 'b1', 'bu', 'b0', 'ru', 'r2', 'r1', 'r0', 'u')])

    def pair_of(ref, n, k):
        both = ref[2 * n:2 * n + 2, :, window(k)]
        return both.reshape(both.shape[0] * both.shape[1], width)

    def stacked(ref, n):
        both = ref[2 * n:2 * n + 2]
        return both.reshape(both.shape[0] * both.shape[1], both.shape[2])

    def up_leaves(k, first, last):
        for i in range(first, last):
            if k == 0:
                load_v(i).wait()
            load_x(k, i).wait()
        for i in range(first, last):
            block = near[i, :, window(k)].astype(BF16)
            xb[i, :, window(k)] = block
            xh0[i, :, window(k)] = mm(v[i], block, 0, 0).astype(BF16)

    def up_merges(k):
        for n in range(leaves // 2):
            xh1[n, :, window(k)] = mm(stacked(w0, n), pair_of(xh0, n, k), 0, 0).astype(BF16)
        for n in range(leaves // 4):
            xh2[n, :, window(k)] = mm(stacked(w1, n), pair_of(xh1, n, k), 0, 0).astype(BF16)

    def swap_copy(k, side, order):
        return remote(xt.at[k, side], xsib.at[k, side], swap_send.at[k, order], swap_recv.at[k, order], partner)

    def swap_start(k, order):
        side = (other, core)[order]
        cut = pl.ds(pl.multiple_of(k * width + side * side_width, side_width), side_width)
        both = xh2[:, :, cut]
        xt[k, side] = mm(both.reshape(both.shape[0] * both.shape[1], side_width), w2[...].reshape(both.shape[0] * both.shape[1], w2.shape[2]), 0, 0).astype(BF16)
        swap_copy(k, side, order).start()

    def out_copy(k, step):
        dest = lax.rem(chip + step, chips)
        return remote(xchip.at[k, dest], xall.at[k, my_slot, core], out_send.at[k, step], out_recv.at[k, my_slot, core], dest * 2 + my_half)

    far_first = [half_chips]
    for step in range(half_chips - 1, 0, -1):
        far_first += [step, chips - step]

    def merge_send(k):
        swap_copy(k, core, 0).wait_recv()
        merged = (mm(xt[k, core], wu[0], 1, 0) + mm(xsib[k, core], wu[1], 1, 0)).astype(BF16)
        xchip[k] = merged.reshape(chips, part, merged.shape[1])
        for step in far_first:
            out_copy(k, step).start()

        @pl.when(core != my_half)
        def _():
            out_copy(k, 0).start()

        @pl.when(core == my_half)
        def _():
            xall[k, my_slot, core] = xchip[k, chip]

    def near_leaves(first, last):
        for i in range(first, last):
            load_d(i).wait()
        for i in range(first, last):
            near[i] = mm(d[i], xb[i], 1, 0)

    def is_mine(n, c):
        return jnp.logical_and(core * half_chips + n == chip, core == c)

    w_at = {level: 2 ** (level - 1) - 2 for level in range(2, depth)}
    b_at = {level: 2 ** (level - 1) - 1 for level in range(1, depth)}

    def top_solve(k):
        for n in range(half_chips):
            for c in range(2):
                @pl.when(jnp.logical_not(is_mine(n, c)))
                def _():
                    remote(xchip.at[k, 0], xall.at[k, n, c], out_send.at[k, 0], out_recv.at[k, n, c], partner).wait_recv()

        levels = [[xall[k, n].reshape(2 * part, xall.shape[-1]) for n in range(half_chips)]]
        for level in range(depth - 1, 1, -1):
            below = levels[-1]
            at = w_at[level]
            levels.append([(mm(below[2 * q], wt[at + 2 * q], 1, 0) + mm(below[2 * q + 1], wt[at + 2 * q + 1], 1, 0)).astype(BF16) for q in range(len(below) // 2)])
        x1[k] = levels[-1][0]
        swap = remote(x1.at[k], x1_sib.at[k], top_send.at[k], top_recv.at[k], partner)
        swap.start()
        for level in range(2, depth):
            nodes = levels[depth - 1 - level]
            for n in range(len(nodes)):
                g_top[w_at[level] + n] = mm(nodes[n ^ 1], bt[b_at[level] + n], 1, 1)
        swap.wait()
        y_top = [mm(x1_sib[k], bt_t[...], 1, 0).astype(BF16)]
        for level in range(2, depth):
            y_top = [(g_top[w_at[level] + n] + mm(y_top[n // 2], rt_t[w_at[level] + n], 1, 0)).astype(BF16) for n in range(2 ** (level - 1))]
        for n in range(half_chips):
            y_out[k, n] = y_top[n].reshape(2, part, y_out.shape[-1])
        for n in range(half_chips):
            for c in range(2):
                @pl.when(jnp.logical_not(is_mine(n, c)))
                def _():
                    back_copy(k, n, c).start()

                @pl.when(is_mine(n, c))
                def _():
                    y_all[k, c, chip] = y_out[k, n, c]

    def back_copy(k, n, c):
        return remote(y_out.at[k, n, c], y_all.at[k, c, chip], back_send.at[k, n, c], back_recv.at[k, chip], (core * half_chips + n) * 2 + c)

    def pair_copy(k, side):
        return remote(y_all.at[k, side], y_all.at[k, side], pair_send.at[k], pair_recv.at[k], partner)

    def back_wait(k):
        for j in range(chips):
            @pl.when(jnp.logical_or(j != chip, core != my_half))
            def _():
                remote(y_out.at[k, 0, 0], y_all.at[k, core, j], back_send.at[k, 0, 0], back_recv.at[k, j], partner).wait_recv()

        pair_copy(k, core).start()

    def finish(k):
        pair_copy(k, other).wait_recv()
        y_dev[:, window(k)] = (g_dev[:, window(k)] + mm(ru[...], y_all[k].reshape(width, y_all.shape[-1]), 1, 1)).astype(BF16)

    with jax.named_scope('p0'):
        up_leaves(0, 0, group)
        copies['wu'].wait()
        pl.semaphore_wait(barrier, devs - 1)
        wsib.start()
        copies['w0'].wait()
        copies['w1'].wait()
        copies['w2'].wait()
    with jax.named_scope('p1'):
        up_leaves(0, group, leaves)
        up_merges(0)
        swap_start(0, 0)
    with jax.named_scope('p2'):
        swap_start(0, 1)
    with jax.named_scope('p4'):
        up_leaves(1, 0, group)
        wsib.wait()
    with jax.named_scope('p5'):
        merge_send(0)
    with jax.named_scope('p6'):
        up_leaves(1, group, leaves)
        up_merges(1)
        swap_start(1, 0)
    with jax.named_scope('p7'):
        swap_start(1, 1)
    with jax.named_scope('p8'):
        near_leaves(0, 3)
    with jax.named_scope('p9'):
        merge_send(1)
        for copy in bt_copies + rt_copies:
            copy.wait()
    with jax.named_scope('p10'):
        near_leaves(3, leaves)
        for n in range(rt.shape[0]):
            rt_t[n] = rt[n].T
        bt_t[...] = bt[0].T
        for copy in wt_copies:
            copy.wait()
    with jax.named_scope('p11'):
        top_solve(0)
    with jax.named_scope('p12'):
        top_solve(1)
    with jax.named_scope('p13'):
        for name in ('b2', 'b1', 'b0', 'bu', 'ru', 'r2', 'r1', 'r0', 'u'):
            copies[name].wait()
        for k in range(chunks):
            swap_copy(k, other, 1).wait_recv()
        for k in range(chunks):
            g_dev[:, window(k)] = mm(bu[...], xsib[k].reshape(width, xsib.shape[-1]), 1, 1)
        for n in range(leaves // 4):
            g2[n] = mm(b2[n], xh2[n ^ 1], 1, 0)
        for n in range(leaves // 2):
            g1[n] = mm(b1[n], xh1[n ^ 1], 1, 0)
    with jax.named_scope('p14'):
        back_wait(0)
    with jax.named_scope('p15'):
        for n in range(leaves):
            g0[n] = mm(b0[n], xh0[n ^ 1], 1, 0)
    with jax.named_scope('p16'):
        finish(0)
        down_skeletons(window(0), y_dev, g0, g1, g2, r0, r1, r2, y2, y1, y0)
    with jax.named_scope('p17'):
        back_wait(1)
    with jax.named_scope('p18'):
        for i in range(leaves):
            near[i, :, window(0)] = near[i, :, window(0)] + mm(u[i], y0[i], 1, 0)
    with jax.named_scope('p19'):
        finish(1)

    for k in range(chunks):
        swap_copy(k, other, 0).wait_send()
        swap_copy(k, core, 1).wait_send()
        for step in far_first:
            out_copy(k, step).wait_send()

        @pl.when(core != my_half)
        def _():
            out_copy(k, 0).wait_send()

        for n in range(half_chips):
            for c in range(2):
                @pl.when(jnp.logical_not(is_mine(n, c)))
                def _():
                    back_copy(k, n, c).wait_send()

        pair_copy(k, core).wait_send()


def down_kernel(chunks, y_dev, near, g0, g1, g2, r0, r1, r2, u, out_hbm, y2, y1, y0, stage, out_sem):
    leaves, leaf_size, width = stage.shape
    last = pl.ds((chunks - 1) * width, width)
    done = pl.ds(0, (chunks - 1) * width)

    def store(i, src, columns, sem):
        return pltpu.make_async_copy(src, out_hbm.at[pl.ds(i * leaf_size, leaf_size), columns], sem)

    def early(i):
        return store(i, near.at[i, :, done], done, out_sem.at[0, i])

    def late(i):
        return store(i, stage.at[i], last, out_sem.at[1, i])

    def start_early(i, carry):
        early(i).start()
        return carry

    lax.fori_loop(0, leaves, start_early, 0)
    down_skeletons(last, y_dev, g0, g1, g2, r0, r1, r2, y2, y1, y0)
    for i in range(leaves):
        stage[i] = near[i, :, last] + mm(u[i], y0[i], 1, 0)
        late(i).start()
    for i in range(leaves):
        early(i).wait()
        late(i).wait()


def solution(mesh):
    devs = mesh.shape['tree']
    rows_spec = P(('batch', 'tree'), None)
    tree_spec = P('tree', None, None)
    full_spec = P(None, None, None)

    def body(x_loc, d_near, u_leaf, v_leaf, w_h0, r_h0, b_h0, w_h1, r_h1, b_h1, w_h2, r_h2, b_h2, w_upper, r_upper, b_upper, w_top, r_top, b_top):
        leaves, leaf_size, rank0 = u_leaf.shape
        cols = x_loc.shape[1]
        rank1 = w_h0.shape[2]
        rank2 = w_h1.shape[2]
        rank3 = w_h2.shape[2]
        chips = devs // 2
        chunks = 2
        width = cols // chunks
        part = cols // (chunks * devs)
        depth = log_two(devs)
        sds = jax.ShapeDtypeStruct
        dma = pltpu.SemaphoreType.DMA
        vmem = pltpu.VMEM
        outs = [vmem((rank3, cols), BF16), vmem((leaves, leaf_size, cols), F32), vmem((leaves, rank0, cols), F32), vmem((leaves // 2, rank1, cols), F32), vmem((leaves // 4, rank2, cols), F32)] + [vmem(a.shape, BF16) for a in (r_h0, r_h1, r_h2, u_leaf)]
        half_nodes = chips - 2
        scratch = [
            vmem((leaves, leaf_size, cols), BF16), vmem((leaves, leaf_size, leaf_size), BF16),
            vmem((leaves, leaf_size, rank0), BF16),
            vmem((leaves, rank0, rank1), BF16), vmem((leaves, rank0, rank0), BF16),
            vmem((leaves // 2, rank1, rank2), BF16), vmem((leaves // 2, rank1, rank1), BF16),
            vmem((leaves // 4, rank2, rank3), BF16), vmem((leaves // 4, rank2, rank2), BF16),
            vmem((2, rank3, rank3), BF16), vmem((rank3, rank3), BF16), vmem((rank3, rank3), BF16),
            vmem((half_nodes, rank3, rank3), BF16), vmem((half_nodes, rank3, rank3), BF16), vmem((half_nodes + 1, rank3, rank3), BF16),
            vmem((leaves, rank0, cols), BF16), vmem((leaves // 2, rank1, cols), BF16), vmem((leaves // 4, rank2, cols), BF16),
            vmem((chunks, 2, width // 2, rank3), BF16), vmem((chunks, 2, width // 2, rank3), BF16),
            vmem((chunks, chips, part, rank3), BF16), vmem((chunks, chips // 2, 2, part, rank3), BF16),
            vmem((chunks, 2 * part, rank3), BF16), vmem((chunks, 2 * part, rank3), BF16), vmem((half_nodes, 2 * part, rank3), F32), vmem((rank3, cols), F32),
            vmem((chunks, chips // 2, 2, part, rank3), BF16), vmem((chunks, 2, chips, part, rank3), BF16), vmem((leaves // 4, rank2, width), BF16), vmem((leaves // 2, rank1, width), BF16), vmem((leaves, rank0, width), BF16), vmem((half_nodes, rank3, rank3), BF16), vmem((rank3, rank3), BF16),
            dma((chunks, leaves)), dma((leaves,)), dma((leaves,)), dma((13 + 3 * depth,)), dma((2,)),
            dma((chunks, 2)), dma((chunks, 2)), dma((chunks, chips)), dma((chunks, chips // 2, 2)), dma((chunks,)), dma((chunks,)),
            dma((chunks, chips // 2, 2)), dma((chunks, chips)), dma((chunks,)), dma((chunks,)),
        ]
        held = pl.pallas_call(
            functools.partial(up_kernel, devs, chunks),
            out_shape=outs,
            in_specs=[HBM_ALL] * 19,
            out_specs=[VMEM_ALL] * 9,
            scratch_shapes=scratch,
            compiler_params=pltpu.CompilerParams(collective_id=0, has_side_effects=True, vmem_limit_bytes=40 * 2 ** 20),
            name='up_top',
        )(*[pltpu.with_memory_space_constraint(a, pltpu.HBM) for a in (x_loc, d_near, v_leaf, w_h0, b_h0, w_h1, b_h1, w_h2, b_h2, w_upper, b_upper, r_upper, w_top, r_top, b_top, r_h0, r_h1, r_h2, u_leaf)])
        return pl.pallas_call(
            functools.partial(down_kernel, chunks),
            out_shape=sds(x_loc.shape, F32),
            in_specs=[VMEM_ALL] * 9,
            out_specs=HBM_ALL,
            scratch_shapes=[vmem((leaves // 4, rank2, width), BF16), vmem((leaves // 2, rank1, width), BF16), vmem((leaves, rank0, width), BF16), vmem((leaves, leaf_size, width), F32), dma((2, leaves))],
            compiler_params=pltpu.CompilerParams(vmem_limit_bytes=14 * 2 ** 20),
            name='down_out',
        )(*[pltpu.with_memory_space_constraint(a, pltpu.VMEM) for a in held])

    return jax.shard_map(body, mesh=mesh, in_specs=(rows_spec,) + (tree_spec,) * 15 + (full_spec,) * 3, out_specs=rows_spec, check_vma=False)
```

```python
import functools
import math

import jax
import jax.numpy as jnp
from jax import lax
from jax.experimental import pallas as pl
from jax.experimental.pallas import tpu as pltpu
from jax.sharding import PartitionSpec as P

MESH = pl.DeviceIdType.MESH
F32 = jnp.float32
BF16 = jnp.bfloat16
VMEM_ALL = pl.BlockSpec(memory_space=pltpu.VMEM)
HBM_ALL = pl.BlockSpec(memory_space=pltpu.HBM)


def log_two(count):
    return int(math.log2(count) + 0.5)


def mm(lhs, rhs, lhs_dim, rhs_dim):
    return lax.dot_general(lhs, rhs, (((lhs_dim,), (rhs_dim,)), ((), ())), preferred_element_type=F32)


def down_skeletons(columns, y_dev, g0, g1, g2, r0, r1, r2, y2, y1, y0):
    for n in range(r2.shape[0]):
        y2[n] = (g2[n, :, columns] + mm(r2[n], y_dev[:, columns], 1, 0)).astype(BF16)
    for n in range(r1.shape[0]):
        y1[n] = (g1[n, :, columns] + mm(r1[n], y2[n // 2], 1, 0)).astype(BF16)
    for n in range(r0.shape[0]):
        y0[n] = (g0[n, :, columns] + mm(r0[n], y1[n // 2], 1, 0)).astype(BF16)


def up_kernel(devs, chunks, x_hbm, d_hbm, v_hbm, w0_hbm, b0_hbm, w1_hbm, b1_hbm, w2_hbm, b2_hbm, wu_hbm, bu_hbm, ru_hbm, wt_hbm, rt_hbm, bt_hbm, r0_hbm, r1_hbm, r2_hbm, u_hbm,
              y_dev, near, g0, g1, g2, r0, r1, r2, u,
              xb, d, v, w0, b0, w1, b1, w2, b2, wu, bu, ru, wt, rt, bt, xh0, xh1, xh2, xt, xsib, xchip, xall, x1, x1_sib, g_top, g_dev, y_out, y_all, y2, y1, y0, rt_t, bt_t,
              x_sem, d_sem, v_sem, w_sem, wsib_sem, swap_send, swap_recv, out_send, out_recv, top_send, top_recv, back_send, back_recv, pair_send, pair_recv):
    me = lax.axis_index('tree')
    chips = devs // 2
    half_chips = chips // 2
    depth = log_two(devs)
    core = lax.rem(me, 2)
    chip = me // 2
    other = 1 - core
    partner = chip * 2 + other
    leaves, leaf_size, cols = xb.shape
    width = cols // chunks
    side_width = width // 2
    part = side_width // chips
    my_half = chip // half_chips
    my_slot = lax.rem(chip, half_chips)

    barrier = pltpu.get_barrier_semaphore()
    for step in range(1, devs):
        pl.semaphore_signal(barrier, inc=1, device_id={'tree': lax.rem(me + step, devs)}, device_id_type=MESH)

    def remote(src, dst, send, recv, dest):
        return pltpu.make_async_remote_copy(src, dst, send, recv, device_id={'tree': dest}, device_id_type=MESH)

    def window(k):
        return pl.ds(k * width, width)

    def load_x(k, i):
        return pltpu.make_async_copy(x_hbm.at[pl.ds(i * leaf_size, leaf_size), window(k)], near.at[i, :, window(k)], x_sem.at[k, i])

    def load_d(i):
        return pltpu.make_async_copy(d_hbm.at[i], d.at[i], d_sem.at[i])

    def load_v(i):
        return pltpu.make_async_copy(v_hbm.at[i], v.at[i], v_sem.at[i])

    copies = {}
    for k, (name, hbm, vmem) in enumerate([('w0', w0_hbm, w0), ('w1', w1_hbm, w1), ('w2', w2_hbm, w2), ('wu', wu_hbm.at[0], wu.at[0]), ('bu', bu_hbm.at[0], bu), ('ru', ru_hbm.at[0], ru), ('b0', b0_hbm, b0), ('b1', b1_hbm, b1), ('b2', b2_hbm, b2), ('r0', r0_hbm, r0), ('r1', r1_hbm, r1), ('r2', r2_hbm, r2), ('u', u_hbm, u)]):
        copies[name] = pltpu.make_async_copy(hbm, vmem, w_sem.at[k])
    base = len(copies)

    def top_slices(hbm, vmem, first, sem):
        out = []
        at = 0
        for level in range(first, depth):
            count = 2 ** (level - 1)
            start = 2 ** level - 2 ** first + core * count
            out.append(pltpu.make_async_copy(hbm.at[pl.ds(start, count)], vmem.at[pl.ds(at, count)], w_sem.at[sem + level]))
            at += count
        return out

    wt_copies = top_slices(wt_hbm, wt, 2, base)
    rt_copies = top_slices(rt_hbm, rt, 2, base + depth)
    bt_copies = top_slices(bt_hbm, bt, 1, base + 2 * depth)
    wsib = remote(wu.at[0], wu.at[1], wsib_sem.at[0], wsib_sem.at[1], partner)

    group = leaves // 2

    def load_many(some, stage=iter(range(99))):
        with jax.named_scope(f'l{next(stage)}'):
            for copy in some:
                copy.start()

    first_half, second_half = range(group), range(group, leaves)
    load_many([load(i) for i in first_half for load in (load_v, lambda i: load_x(0, i))])
    load_many([copies['wu'], copies['w0']])
    load_many([load(i) for i in second_half for load in (load_v, lambda i: load_x(0, i))])
    load_many([copies['w1'], copies['w2']])
    load_many([load_x(1, i) for i in first_half])
    load_many([load_x(1, i) for i in second_half])
    load_many([load_d(i) for i in range(3)])
    load_many([load_d(i) for i in range(3, leaves)])
    load_many(rt_copies + bt_copies)
    load_many(wt_copies)
    load_many([copies[name] for name in ('b2', 'b1', 'bu', 'b0', 'ru', 'r2', 'r1', 'r0', 'u')])

    def pair_of(ref, n, k):
        both = ref[2 * n:2 * n + 2, :, window(k)]
        return both.reshape(both.shape[0] * both.shape[1], width)

    def stacked(ref, n):
        both = ref[2 * n:2 * n + 2]
        return both.reshape(both.shape[0] * both.shape[1], both.shape[2])

    def up_leaves(k, first, last):
        for i in range(first, last):
            if k == 0:
                load_v(i).wait()
            load_x(k, i).wait()
        for i in range(first, last):
            block = near[i, :, window(k)].astype(BF16)
            xb[i, :, window(k)] = block
            xh0[i, :, window(k)] = mm(v[i], block, 0, 0).astype(BF16)

    def up_merges(k):
        for n in range(leaves // 2):
            xh1[n, :, window(k)] = mm(stacked(w0, n), pair_of(xh0, n, k), 0, 0).astype(BF16)
        for n in range(leaves // 4):
            xh2[n, :, window(k)] = mm(stacked(w1, n), pair_of(xh1, n, k), 0, 0).astype(BF16)

    def swap_copy(k, side, order):
        return remote(xt.at[k, side], xsib.at[k, side], swap_send.at[k, order], swap_recv.at[k, order], partner)

    def swap_start(k, order):
        side = (other, core)[order]
        cut = pl.ds(pl.multiple_of(k * width + side * side_width, side_width), side_width)
        both = xh2[:, :, cut]
        xt[k, side] = mm(both.reshape(both.shape[0] * both.shape[1], side_width), w2[...].reshape(both.shape[0] * both.shape[1], w2.shape[2]), 0, 0).astype(BF16)
        swap_copy(k, side, order).start()

    def out_copy(k, step):
        dest = lax.rem(chip + step, chips)
        return remote(xchip.at[k, dest], xall.at[k, my_slot, core], out_send.at[k, step], out_recv.at[k, my_slot, core], dest * 2 + my_half)

    far_first = [half_chips]
    for step in range(half_chips - 1, 0, -1):
        far_first += [step, chips - step]

    def merge_send(k):
        swap_copy(k, core, 0).wait_recv()
        merged = (mm(xt[k, core], wu[0], 1, 0) + mm(xsib[k, core], wu[1], 1, 0)).astype(BF16)
        xchip[k] = merged.reshape(chips, part, merged.shape[1])
        for step in far_first:
            out_copy(k, step).start()

        @pl.when(core != my_half)
        def _():
            out_copy(k, 0).start()

        @pl.when(core == my_half)
        def _():
            xall[k, my_slot, core] = xchip[k, chip]

    def near_leaves(first, last):
        for i in range(first, last):
            load_d(i).wait()
        for i in range(first, last):
            near[i] = mm(d[i], xb[i], 1, 0)

    def is_mine(n, c):
        return jnp.logical_and(core * half_chips + n == chip, core == c)

    w_at = {level: 2 ** (level - 1) - 2 for level in range(2, depth)}
    b_at = {level: 2 ** (level - 1) - 1 for level in range(1, depth)}

    def top_solve(k):
        for n in range(half_chips):
            for c in range(2):
                @pl.when(jnp.logical_not(is_mine(n, c)))
                def _():
                    remote(xchip.at[k, 0], xall.at[k, n, c], out_send.at[k, 0], out_recv.at[k, n, c], partner).wait_recv()

        levels = [[xall[k, n].reshape(2 * part, xall.shape[-1]) for n in range(half_chips)]]
        for level in range(depth - 1, 1, -1):
            below = levels[-1]
            at = w_at[level]
            levels.append([(mm(below[2 * q], wt[at + 2 * q], 1, 0) + mm(below[2 * q + 1], wt[at + 2 * q + 1], 1, 0)).astype(BF16) for q in range(len(below) // 2)])
        x1[k] = levels[-1][0]
        swap = remote(x1.at[k], x1_sib.at[k], top_send.at[k], top_recv.at[k], partner)
        swap.start()
        for level in range(2, depth):
            nodes = levels[depth - 1 - level]
            for n in range(len(nodes)):
                g_top[w_at[level] + n] = mm(nodes[n ^ 1], bt[b_at[level] + n], 1, 1)
        swap.wait()
        y_top = [mm(x1_sib[k], bt_t[...], 1, 0).astype(BF16)]
        for level in range(2, depth):
            y_top = [(g_top[w_at[level] + n] + mm(y_top[n // 2], rt_t[w_at[level] + n], 1, 0)).astype(BF16) for n in range(2 ** (level - 1))]
        for n in range(half_chips):
            y_out[k, n] = y_top[n].reshape(2, part, y_out.shape[-1])
        for n in range(half_chips):
            for c in range(2):
                @pl.when(jnp.logical_not(is_mine(n, c)))
                def _():
                    back_copy(k, n, c).start()

                @pl.when(is_mine(n, c))
                def _():
                    y_all[k, c, chip] = y_out[k, n, c]

    def back_copy(k, n, c):
        return remote(y_out.at[k, n, c], y_all.at[k, c, chip], back_send.at[k, n, c], back_recv.at[k, chip], (core * half_chips + n) * 2 + c)

    def pair_copy(k, side):
        return remote(y_all.at[k, side], y_all.at[k, side], pair_send.at[k], pair_recv.at[k], partner)

    def back_wait(k):
        for j in range(chips):
            @pl.when(jnp.logical_or(j != chip, core != my_half))
            def _():
                remote(y_out.at[k, 0, 0], y_all.at[k, core, j], back_send.at[k, 0, 0], back_recv.at[k, j], partner).wait_recv()

        pair_copy(k, core).start()

    def finish(k):
        pair_copy(k, other).wait_recv()
        y_dev[:, window(k)] = (g_dev[:, window(k)] + mm(ru[...], y_all[k].reshape(width, y_all.shape[-1]), 1, 1)).astype(BF16)

    with jax.named_scope('p0'):
        up_leaves(0, 0, group)
        copies['wu'].wait()
        pl.semaphore_wait(barrier, devs - 1)
        wsib.start()
        copies['w0'].wait()
        copies['w1'].wait()
        copies['w2'].wait()
    with jax.named_scope('p1'):
        up_leaves(0, group, leaves)
        up_merges(0)
        swap_start(0, 0)
    with jax.named_scope('p2'):
        swap_start(0, 1)
    with jax.named_scope('p4'):
        up_leaves(1, 0, group)
        wsib.wait()
    with jax.named_scope('p5'):
        merge_send(0)
    with jax.named_scope('p6'):
        up_leaves(1, group, leaves)
        up_merges(1)
        swap_start(1, 0)
    with jax.named_scope('p7'):
        swap_start(1, 1)
    with jax.named_scope('p8'):
        near_leaves(0, 3)
    with jax.named_scope('p9'):
        merge_send(1)
        for copy in bt_copies + rt_copies:
            copy.wait()
    with jax.named_scope('p10'):
        near_leaves(3, leaves)
        for n in range(rt.shape[0]):
            rt_t[n] = rt[n].T
        bt_t[...] = bt[0].T
        for copy in wt_copies:
            copy.wait()
    with jax.named_scope('p11'):
        top_solve(0)
    with jax.named_scope('p12'):
        top_solve(1)
    with jax.named_scope('p13'):
        for name in ('b2', 'b1', 'b0', 'bu', 'ru', 'r2', 'r1', 'r0', 'u'):
            copies[name].wait()
        for k in range(chunks):
            swap_copy(k, other, 1).wait_recv()
        for k in range(chunks):
            g_dev[:, window(k)] = mm(bu[...], xsib[k].reshape(width, xsib.shape[-1]), 1, 1)
        for n in range(leaves // 4):
            g2[n] = mm(b2[n], xh2[n ^ 1], 1, 0)
        for n in range(leaves // 2):
            g1[n] = mm(b1[n], xh1[n ^ 1], 1, 0)
    with jax.named_scope('p14'):
        back_wait(0)
    with jax.named_scope('p15'):
        for n in range(leaves):
            g0[n] = mm(b0[n], xh0[n ^ 1], 1, 0)
    with jax.named_scope('p16'):
        finish(0)
        down_skeletons(window(0), y_dev, g0, g1, g2, r0, r1, r2, y2, y1, y0)
    with jax.named_scope('p17'):
        back_wait(1)
    with jax.named_scope('p18'):
        for i in range(leaves):
            near[i, :, window(0)] = near[i, :, window(0)] + mm(u[i], y0[i], 1, 0)
    with jax.named_scope('p19'):
        finish(1)

    for k in range(chunks):
        swap_copy(k, other, 0).wait_send()
        swap_copy(k, core, 1).wait_send()
        for step in far_first:
            out_copy(k, step).wait_send()

        @pl.when(core != my_half)
        def _():
            out_copy(k, 0).wait_send()

        for n in range(half_chips):
            for c in range(2):
                @pl.when(jnp.logical_not(is_mine(n, c)))
                def _():
                    back_copy(k, n, c).wait_send()

        pair_copy(k, core).wait_send()


def down_kernel(chunks, y_dev, near, g0, g1, g2, r0, r1, r2, u, out_hbm, y2, y1, y0, stage, out_sem):
    leaves, leaf_size, width = stage.shape
    last = pl.ds((chunks - 1) * width, width)
    done = pl.ds(0, (chunks - 1) * width)

    def store(i, src, columns, sem):
        return pltpu.make_async_copy(src, out_hbm.at[pl.ds(i * leaf_size, leaf_size), columns], sem)

    def early(i):
        return store(i, near.at[i, :, done], done, out_sem.at[0, i])

    def late(i):
        return store(i, stage.at[i], last, out_sem.at[1, i])

    def start_early(i, carry):
        early(i).start()
        return carry

    lax.fori_loop(0, leaves, start_early, 0)
    down_skeletons(last, y_dev, g0, g1, g2, r0, r1, r2, y2, y1, y0)
    for i in range(leaves):
        stage[i] = near[i, :, last] + mm(u[i], y0[i], 1, 0)
        late(i).start()
    for i in range(leaves):
        early(i).wait()
        late(i).wait()


def solution(mesh):
    devs = mesh.shape['tree']
    rows_spec = P(('batch', 'tree'), None)
    tree_spec = P('tree', None, None)
    full_spec = P(None, None, None)

    def body(x_loc, d_near, u_leaf, v_leaf, w_h0, r_h0, b_h0, w_h1, r_h1, b_h1, w_h2, r_h2, b_h2, w_upper, r_upper, b_upper, w_top, r_top, b_top):
        leaves, leaf_size, rank0 = u_leaf.shape
        cols = x_loc.shape[1]
        rank1 = w_h0.shape[2]
        rank2 = w_h1.shape[2]
        rank3 = w_h2.shape[2]
        chips = devs // 2
        chunks = 2
        width = cols // chunks
        part = cols // (chunks * devs)
        depth = log_two(devs)
        sds = jax.ShapeDtypeStruct
        dma = pltpu.SemaphoreType.DMA
        vmem = pltpu.VMEM
        outs = [vmem((rank3, cols), BF16), vmem((leaves, leaf_size, cols), F32), vmem((leaves, rank0, cols), F32), vmem((leaves // 2, rank1, cols), F32), vmem((leaves // 4, rank2, cols), F32)] + [vmem(a.shape, BF16) for a in (r_h0, r_h1, r_h2, u_leaf)]
        half_nodes = chips - 2
        scratch = [
            vmem((leaves, leaf_size, cols), BF16), vmem((leaves, leaf_size, leaf_size), BF16),
            vmem((leaves, leaf_size, rank0), BF16),
            vmem((leaves, rank0, rank1), BF16), vmem((leaves, rank0, rank0), BF16),
            vmem((leaves // 2, rank1, rank2), BF16), vmem((leaves // 2, rank1, rank1), BF16),
            vmem((leaves // 4, rank2, rank3), BF16), vmem((leaves // 4, rank2, rank2), BF16),
            vmem((2, rank3, rank3), BF16), vmem((rank3, rank3), BF16), vmem((rank3, rank3), BF16),
            vmem((half_nodes, rank3, rank3), BF16), vmem((half_nodes, rank3, rank3), BF16), vmem((half_nodes + 1, rank3, rank3), BF16),
            vmem((leaves, rank0, cols), BF16), vmem((leaves // 2, rank1, cols), BF16), vmem((leaves // 4, rank2, cols), BF16),
            vmem((chunks, 2, width // 2, rank3), BF16), vmem((chunks, 2, width // 2, rank3), BF16),
            vmem((chunks, chips, part, rank3), BF16), vmem((chunks, chips // 2, 2, part, rank3), BF16),
            vmem((chunks, 2 * part, rank3), BF16), vmem((chunks, 2 * part, rank3), BF16), vmem((half_nodes, 2 * part, rank3), F32), vmem((rank3, cols), F32),
            vmem((chunks, chips // 2, 2, part, rank3), BF16), vmem((chunks, 2, chips, part, rank3), BF16), vmem((leaves // 4, rank2, width), BF16), vmem((leaves // 2, rank1, width), BF16), vmem((leaves, rank0, width), BF16), vmem((half_nodes, rank3, rank3), BF16), vmem((rank3, rank3), BF16),
            dma((chunks, leaves)), dma((leaves,)), dma((leaves,)), dma((13 + 3 * depth,)), dma((2,)),
            dma((chunks, 2)), dma((chunks, 2)), dma((chunks, chips)), dma((chunks, chips // 2, 2)), dma((chunks,)), dma((chunks,)),
            dma((chunks, chips // 2, 2)), dma((chunks, chips)), dma((chunks,)), dma((chunks,)),
        ]
        held = pl.pallas_call(
            functools.partial(up_kernel, devs, chunks),
            out_shape=outs,
            in_specs=[HBM_ALL] * 19,
            out_specs=[VMEM_ALL] * 9,
            scratch_shapes=scratch,
            compiler_params=pltpu.CompilerParams(collective_id=0, has_side_effects=True, vmem_limit_bytes=40 * 2 ** 20),
            name='up_top',
        )(*[pltpu.with_memory_space_constraint(a, pltpu.HBM) for a in (x_loc, d_near, v_leaf, w_h0, b_h0, w_h1, b_h1, w_h2, b_h2, w_upper, b_upper, r_upper, w_top, r_top, b_top, r_h0, r_h1, r_h2, u_leaf)])
        return pl.pallas_call(
            functools.partial(down_kernel, chunks),
            out_shape=sds(x_loc.shape, F32),
            in_specs=[VMEM_ALL] * 9,
            out_specs=HBM_ALL,
            scratch_shapes=[vmem((leaves // 4, rank2, width), BF16), vmem((leaves // 2, rank1, width), BF16), vmem((leaves, rank0, width), BF16), vmem((leaves, leaf_size, width), F32), dma((2, leaves))],
            compiler_params=pltpu.CompilerParams(vmem_limit_bytes=14 * 2 ** 20),
            name='down_out',
        )(*[pltpu.with_memory_space_constraint(a, pltpu.VMEM) for a in held])

    return jax.shard_map(body, mesh=mesh, in_specs=(rows_spec,) + (tree_spec,) * 15 + (full_spec,) * 3, out_specs=rows_spec, check_vma=False)
```

```python
import functools
import math

import jax
import jax.numpy as jnp
from jax import lax
from jax.experimental import pallas as pl
from jax.experimental.pallas import tpu as pltpu
from jax.sharding import PartitionSpec as P

MESH = pl.DeviceIdType.MESH
F32 = jnp.float32
BF16 = jnp.bfloat16
VMEM_ALL = pl.BlockSpec(memory_space=pltpu.VMEM)
HBM_ALL = pl.BlockSpec(memory_space=pltpu.HBM)


def log_two(count):
    return int(math.log2(count) + 0.5)


def mm(lhs, rhs, lhs_dim, rhs_dim):
    return lax.dot_general(lhs, rhs, (((lhs_dim,), (rhs_dim,)), ((), ())), preferred_element_type=F32)


def down_skeletons(columns, y_dev, g0, g1, g2, r0, r1, r2, y2, y1, y0):
    for n in range(r2.shape[0]):
        y2[n] = (g2[n, :, columns] + mm(r2[n], y_dev[:, columns], 1, 0)).astype(BF16)
    for n in range(r1.shape[0]):
        y1[n] = (g1[n, :, columns] + mm(r1[n], y2[n // 2], 1, 0)).astype(BF16)
    for n in range(r0.shape[0]):
        y0[n] = (g0[n, :, columns] + mm(r0[n], y1[n // 2], 1, 0)).astype(BF16)


def up_kernel(devs, chunks, x_hbm, d_hbm, v_hbm, w0_hbm, b0_hbm, w1_hbm, b1_hbm, w2_hbm, b2_hbm, wu_hbm, bu_hbm, ru_hbm, wt_hbm, rt_hbm, bt_hbm, r0_hbm, r1_hbm, r2_hbm, u_hbm,
              y_dev, near, g0, g1, g2, r0, r1, r2, u,
              xb, d, v, w0, b0, w1, b1, w2, b2, wu, bu, ru, wt, rt, bt, xh0, xh1, xh2, xt, xsib, xchip, xall, x1, x1_sib, g_top, g_dev, y_out, y_all, y2, y1, y0, rt_t, bt_t,
              x_sem, d_sem, v_sem, w_sem, wsib_sem, swap_send, swap_recv, out_send, out_recv, top_send, top_recv, back_send, back_recv, pair_send, pair_recv):
    me = lax.axis_index('tree')
    chips = devs // 2
    half_chips = chips // 2
    depth = log_two(devs)
    core = lax.rem(me, 2)
    chip = me // 2
    other = 1 - core
    partner = chip * 2 + other
    leaves, leaf_size, cols = xb.shape
    width = cols // chunks
    side_width = width // 2
    part = side_width // chips
    my_half = chip // half_chips
    my_slot = lax.rem(chip, half_chips)
    upper_half = (my_slot * 2) // half_chips
    same_half = 1 - lax.rem(my_half + core, 2)
    falling = lax.rem(upper_half + same_half, 2)

    barrier = pltpu.get_barrier_semaphore()
    for step in range(1, devs):
        pl.semaphore_signal(barrier, inc=1, device_id={'tree': lax.rem(me + step, devs)}, device_id_type=MESH)

    def remote(src, dst, send, recv, dest):
        return pltpu.make_async_remote_copy(src, dst, send, recv, device_id={'tree': dest}, device_id_type=MESH)

    def window(k):
        return pl.ds(k * width, width)

    def load_x(k, i):
        return pltpu.make_async_copy(x_hbm.at[pl.ds(i * leaf_size, leaf_size), window(k)], near.at[i, :, window(k)], x_sem.at[k, i])

    def load_d(i):
        return pltpu.make_async_copy(d_hbm.at[i], d.at[i], d_sem.at[i])

    def load_v(i):
        return pltpu.make_async_copy(v_hbm.at[i], v.at[i], v_sem.at[i])

    copies = {}
    for k, (name, hbm, vmem) in enumerate([('w0', w0_hbm, w0), ('w1', w1_hbm, w1), ('w2', w2_hbm, w2), ('wu', wu_hbm.at[0], wu.at[0]), ('bu', bu_hbm.at[0], bu), ('ru', ru_hbm.at[0], ru), ('b0', b0_hbm, b0), ('b1', b1_hbm, b1), ('b2', b2_hbm, b2), ('r0', r0_hbm, r0), ('r1', r1_hbm, r1), ('r2', r2_hbm, r2), ('u', u_hbm, u)]):
        copies[name] = pltpu.make_async_copy(hbm, vmem, w_sem.at[k])
    base = len(copies)

    def top_slices(hbm, vmem, first, sem):
        out = []
        at = 0
        for level in range(first, depth):
            count = 2 ** (level - 1)
            start = 2 ** level - 2 ** first + core * count
            out.append(pltpu.make_async_copy(hbm.at[pl.ds(start, count)], vmem.at[pl.ds(at, count)], w_sem.at[sem + level]))
            at += count
        return out

    wt_copies = top_slices(wt_hbm, wt, 2, base)
    rt_copies = top_slices(rt_hbm, rt, 2, base + depth)
    bt_copies = top_slices(bt_hbm, bt, 1, base + 2 * depth)
    wsib = remote(wu.at[0], wu.at[1], wsib_sem.at[0], wsib_sem.at[1], partner)

    group = leaves // 2

    def load_many(some, stage=iter(range(99))):
        with jax.named_scope(f'l{next(stage)}'):
            for copy in some:
                copy.start()

    first_half, second_half = range(group), range(group, leaves)
    load_many([load(i) for i in first_half for load in (load_v, lambda i: load_x(0, i))])
    load_many([copies['wu'], copies['w0']])
    load_many([load(i) for i in second_half for load in (load_v, lambda i: load_x(0, i))])
    load_many([copies['w1'], copies['w2']])
    load_many([load_x(1, i) for i in first_half])
    load_many([load_x(1, i) for i in second_half])
    load_many([load_d(i) for i in range(3)])
    load_many([load_d(i) for i in range(3, leaves)])
    load_many(rt_copies + bt_copies)
    load_many(wt_copies)
    load_many([copies[name] for name in ('b2', 'b1', 'bu', 'b0', 'ru', 'r2', 'r1', 'r0', 'u')])

    def pair_of(ref, n, k):
        both = ref[2 * n:2 * n + 2, :, window(k)]
        return both.reshape(both.shape[0] * both.shape[1], width)

    def stacked(ref, n):
        both = ref[2 * n:2 * n + 2]
        return both.reshape(both.shape[0] * both.shape[1], both.shape[2])

    def up_leaves(k, first, last):
        for i in range(first, last):
            if k == 0:
                load_v(i).wait()
            load_x(k, i).wait()
        for i in range(first, last):
            block = near[i, :, window(k)].astype(BF16)
            xb[i, :, window(k)] = block
            xh0[i, :, window(k)] = mm(v[i], block, 0, 0).astype(BF16)

    def up_merges(k):
        for n in range(leaves // 2):
            xh1[n, :, window(k)] = mm(stacked(w0, n), pair_of(xh0, n, k), 0, 0).astype(BF16)
        for n in range(leaves // 4):
            xh2[n, :, window(k)] = mm(stacked(w1, n), pair_of(xh1, n, k), 0, 0).astype(BF16)

    def swap_copy(k, side, order):
        return remote(xt.at[k, side], xsib.at[k, side], swap_send.at[k, order], swap_recv.at[k, order], partner)

    def swap_start(k, order):
        side = (other, core)[order]
        cut = pl.ds(pl.multiple_of(k * width + side * side_width, side_width), side_width)
        both = xh2[:, :, cut]
        xt[k, side] = mm(both.reshape(both.shape[0] * both.shape[1], side_width), w2[...].reshape(both.shape[0] * both.shape[1], w2.shape[2]), 0, 0).astype(BF16)
        swap_copy(k, side, order).start()

    def out_copy(k, step):
        dest = lax.rem(chip + step, chips)
        return remote(xchip.at[k, dest], xall.at[k, my_slot, core], out_send.at[k, step], out_recv.at[k, my_slot, core], dest * 2 + my_half)

    far_first = [half_chips]
    for step in range(half_chips - 1, 0, -1):
        far_first += [step, chips - step]

    def merge_send(k):
        swap_copy(k, core, 0).wait_recv()
        merged = (mm(xt[k, core], wu[0], 1, 0) + mm(xsib[k, core], wu[1], 1, 0)).astype(BF16)
        xchip[k] = merged.reshape(chips, part, merged.shape[1])
        for step in far_first:
            out_copy(k, step).start()

        @pl.when(core != my_half)
        def _():
            out_copy(k, 0).start()

        @pl.when(core == my_half)
        def _():
            xall[k, my_slot, core] = xchip[k, chip]

    def near_leaves(first, last):
        for i in range(first, last):
            load_d(i).wait()
        for i in range(first, last):
            near[i] = mm(d[i], xb[i], 1, 0)

    def is_mine(n, c):
        return jnp.logical_and(core * half_chips + n == chip, core == c)

    w_at = {level: 2 ** (level - 1) - 2 for level in range(2, depth)}
    b_at = {level: 2 ** (level - 1) - 1 for level in range(1, depth)}

    def top_solve(k):
        for n in range(half_chips):
            for c in range(2):
                @pl.when(jnp.logical_not(is_mine(n, c)))
                def _():
                    remote(xchip.at[k, 0], xall.at[k, n, c], out_send.at[k, 0], out_recv.at[k, n, c], partner).wait_recv()

        levels = [[xall[k, n].reshape(2 * part, xall.shape[-1]) for n in range(half_chips)]]
        for level in range(depth - 1, 1, -1):
            below = levels[-1]
            at = w_at[level]
            levels.append([(mm(below[2 * q], wt[at + 2 * q], 1, 0) + mm(below[2 * q + 1], wt[at + 2 * q + 1], 1, 0)).astype(BF16) for q in range(len(below) // 2)])
        x1[k] = levels[-1][0]
        swap = remote(x1.at[k], x1_sib.at[k], top_send.at[k], top_recv.at[k], partner)
        swap.start()
        for level in range(2, depth):
            nodes = levels[depth - 1 - level]
            for n in range(len(nodes)):
                g_top[w_at[level] + n] = mm(nodes[n ^ 1], bt[b_at[level] + n], 1, 1)
        swap.wait()
        y_top = [mm(x1_sib[k], bt_t[...], 1, 0).astype(BF16)]
        for level in range(2, depth):
            y_top = [(g_top[w_at[level] + n] + mm(y_top[n // 2], rt_t[w_at[level] + n], 1, 0)).astype(BF16) for n in range(2 ** (level - 1))]
        for n in range(half_chips):
            y_out[k, n] = y_top[n].reshape(2, part, y_out.shape[-1])
        for i in range(half_chips):
            n = i + falling * (half_chips - 1 - 2 * i)
            for c in range(2):
                @pl.when(jnp.logical_not(is_mine(n, c)))
                def _():
                    back_copy(k, n, c).start()

                @pl.when(is_mine(n, c))
                def _():
                    y_all[k, c, chip] = y_out[k, n, c]

    def back_copy(k, n, c):
        return remote(y_out.at[k, n, c], y_all.at[k, c, chip], back_send.at[k, n, c], back_recv.at[k, chip], (core * half_chips + n) * 2 + c)

    def pair_copy(k, side):
        return remote(y_all.at[k, side], y_all.at[k, side], pair_send.at[k], pair_recv.at[k], partner)

    def back_wait(k):
        for j in range(chips):
            @pl.when(jnp.logical_or(j != chip, core != my_half))
            def _():
                remote(y_out.at[k, 0, 0], y_all.at[k, core, j], back_send.at[k, 0, 0], back_recv.at[k, j], partner).wait_recv()

        pair_copy(k, core).start()

    def finish(k):
        pair_copy(k, other).wait_recv()
        y_dev[:, window(k)] = (g_dev[:, window(k)] + mm(ru[...], y_all[k].reshape(width, y_all.shape[-1]), 1, 1)).astype(BF16)

    def add_far(first, last):
        for i in range(first, last):
            near[i, :, window(0)] = near[i, :, window(0)] + mm(u[i], y0[i], 1, 0)

    with jax.named_scope('p0'):
        up_leaves(0, 0, group)
        copies['wu'].wait()
        pl.semaphore_wait(barrier, devs - 1)
        wsib.start()
    with jax.named_scope('p1'):
        up_leaves(0, group, leaves)
        copies['w0'].wait()
        copies['w1'].wait()
        copies['w2'].wait()
    with jax.named_scope('q1'):
        up_merges(0)
        swap_start(0, 0)
    with jax.named_scope('p2'):
        swap_start(0, 1)
    with jax.named_scope('p4'):
        up_leaves(1, 0, group)
        wsib.wait()
    with jax.named_scope('p5'):
        merge_send(0)
    with jax.named_scope('p6'):
        up_leaves(1, group, leaves)
        up_merges(1)
        swap_start(1, 0)
    with jax.named_scope('p7'):
        swap_start(1, 1)
    with jax.named_scope('p8'):
        near_leaves(0, 2)
    with jax.named_scope('p9'):
        merge_send(1)
        for copy in bt_copies + rt_copies:
            copy.wait()
    with jax.named_scope('p10'):
        near_leaves(2, leaves)
        for n in range(rt.shape[0]):
            rt_t[n] = rt[n].T
        bt_t[...] = bt[0].T
        for copy in wt_copies:
            copy.wait()
    with jax.named_scope('p11'):
        top_solve(0)
    with jax.named_scope('p12'):
        top_solve(1)
    with jax.named_scope('p13'):
        for name in ('b2', 'b1', 'b0', 'bu', 'ru', 'r2', 'r1', 'r0', 'u'):
            copies[name].wait()
        for k in range(chunks):
            swap_copy(k, other, 1).wait_recv()
        for k in range(chunks):
            g_dev[:, window(k)] = mm(bu[...], xsib[k].reshape(width, xsib.shape[-1]), 1, 1)
        for n in range(leaves // 4):
            g2[n] = mm(b2[n], xh2[n ^ 1], 1, 0)
        for n in range(leaves // 2):
            g1[n] = mm(b1[n], xh1[n ^ 1], 1, 0)
    with jax.named_scope('p14'):
        back_wait(0)
    with jax.named_scope('p15'):
        for n in range(leaves):
            g0[n] = mm(b0[n], xh0[n ^ 1], 1, 0)
    with jax.named_scope('p16'):
        finish(0)
        down_skeletons(window(0), y_dev, g0, g1, g2, r0, r1, r2, y2, y1, y0)
    with jax.named_scope('p17'):
        add_far(0, 4)
    with jax.named_scope('q17'):
        back_wait(1)
    with jax.named_scope('p18'):
        add_far(4, leaves)
    with jax.named_scope('p19'):
        finish(1)

    for k in range(chunks):
        swap_copy(k, other, 0).wait_send()
        swap_copy(k, core, 1).wait_send()
        for step in far_first:
            out_copy(k, step).wait_send()

        @pl.when(core != my_half)
        def _():
            out_copy(k, 0).wait_send()

        for n in range(half_chips):
            for c in range(2):
                @pl.when(jnp.logical_not(is_mine(n, c)))
                def _():
                    back_copy(k, n, c).wait_send()

        pair_copy(k, core).wait_send()


def down_kernel(chunks, y_dev, near, g0, g1, g2, r0, r1, r2, u, out_hbm, y2, y1, y0, stage, out_sem):
    leaves, leaf_size, width = stage.shape
    last = pl.ds((chunks - 1) * width, width)
    done = pl.ds(0, (chunks - 1) * width)

    def store(i, src, columns, sem):
        return pltpu.make_async_copy(src, out_hbm.at[pl.ds(i * leaf_size, leaf_size), columns], sem)

    def early(i):
        return store(i, near.at[i, :, done], done, out_sem.at[0, i])

    def late(i):
        return store(i, stage.at[i], last, out_sem.at[1, i])

    def start_early(i, carry):
        early(i).start()
        return carry

    lax.fori_loop(0, leaves, start_early, 0)
    down_skeletons(last, y_dev, g0, g1, g2, r0, r1, r2, y2, y1, y0)
    for i in range(leaves):
        stage[i] = near[i, :, last] + mm(u[i], y0[i], 1, 0)
        late(i).start()
    for i in range(leaves):
        early(i).wait()
        late(i).wait()


def solution(mesh):
    devs = mesh.shape['tree']
    rows_spec = P(('batch', 'tree'), None)
    tree_spec = P('tree', None, None)
    full_spec = P(None, None, None)

    def body(x_loc, d_near, u_leaf, v_leaf, w_h0, r_h0, b_h0, w_h1, r_h1, b_h1, w_h2, r_h2, b_h2, w_upper, r_upper, b_upper, w_top, r_top, b_top):
        leaves, leaf_size, rank0 = u_leaf.shape
        cols = x_loc.shape[1]
        rank1 = w_h0.shape[2]
        rank2 = w_h1.shape[2]
        rank3 = w_h2.shape[2]
        chips = devs // 2
        chunks = 2
        width = cols // chunks
        part = cols // (chunks * devs)
        depth = log_two(devs)
        sds = jax.ShapeDtypeStruct
        dma = pltpu.SemaphoreType.DMA
        vmem = pltpu.VMEM
        outs = [vmem((rank3, cols), BF16), vmem((leaves, leaf_size, cols), F32), vmem((leaves, rank0, cols), F32), vmem((leaves // 2, rank1, cols), F32), vmem((leaves // 4, rank2, cols), F32)] + [vmem(a.shape, BF16) for a in (r_h0, r_h1, r_h2, u_leaf)]
        half_nodes = chips - 2
        scratch = [
            vmem((leaves, leaf_size, cols), BF16), vmem((leaves, leaf_size, leaf_size), BF16),
            vmem((leaves, leaf_size, rank0), BF16),
            vmem((leaves, rank0, rank1), BF16), vmem((leaves, rank0, rank0), BF16),
            vmem((leaves // 2, rank1, rank2), BF16), vmem((leaves // 2, rank1, rank1), BF16),
            vmem((leaves // 4, rank2, rank3), BF16), vmem((leaves // 4, rank2, rank2), BF16),
            vmem((2, rank3, rank3), BF16), vmem((rank3, rank3), BF16), vmem((rank3, rank3), BF16),
            vmem((half_nodes, rank3, rank3), BF16), vmem((half_nodes, rank3, rank3), BF16), vmem((half_nodes + 1, rank3, rank3), BF16),
            vmem((leaves, rank0, cols), BF16), vmem((leaves // 2, rank1, cols), BF16), vmem((leaves // 4, rank2, cols), BF16),
            vmem((chunks, 2, width // 2, rank3), BF16), vmem((chunks, 2, width // 2, rank3), BF16),
            vmem((chunks, chips, part, rank3), BF16), vmem((chunks, chips // 2, 2, part, rank3), BF16),
            vmem((chunks, 2 * part, rank3), BF16), vmem((chunks, 2 * part, rank3), BF16), vmem((half_nodes, 2 * part, rank3), F32), vmem((rank3, cols), F32),
            vmem((chunks, chips // 2, 2, part, rank3), BF16), vmem((chunks, 2, chips, part, rank3), BF16), vmem((leaves // 4, rank2, width), BF16), vmem((leaves // 2, rank1, width), BF16), vmem((leaves, rank0, width), BF16), vmem((half_nodes, rank3, rank3), BF16), vmem((rank3, rank3), BF16),
            dma((chunks, leaves)), dma((leaves,)), dma((leaves,)), dma((13 + 3 * depth,)), dma((2,)),
            dma((chunks, 2)), dma((chunks, 2)), dma((chunks, chips)), dma((chunks, chips // 2, 2)), dma((chunks,)), dma((chunks,)),
            dma((chunks, chips // 2, 2)), dma((chunks, chips)), dma((chunks,)), dma((chunks,)),
        ]
        held = pl.pallas_call(
            functools.partial(up_kernel, devs, chunks),
            out_shape=outs,
            in_specs=[HBM_ALL] * 19,
            out_specs=[VMEM_ALL] * 9,
            scratch_shapes=scratch,
            compiler_params=pltpu.CompilerParams(collective_id=0, has_side_effects=True, vmem_limit_bytes=40 * 2 ** 20),
            name='up_top',
        )(*[pltpu.with_memory_space_constraint(a, pltpu.HBM) for a in (x_loc, d_near, v_leaf, w_h0, b_h0, w_h1, b_h1, w_h2, b_h2, w_upper, b_upper, r_upper, w_top, r_top, b_top, r_h0, r_h1, r_h2, u_leaf)])
        return pl.pallas_call(
            functools.partial(down_kernel, chunks),
            out_shape=sds(x_loc.shape, F32),
            in_specs=[VMEM_ALL] * 9,
            out_specs=HBM_ALL,
            scratch_shapes=[vmem((leaves // 4, rank2, width), BF16), vmem((leaves // 2, rank1, width), BF16), vmem((leaves, rank0, width), BF16), vmem((leaves, leaf_size, width), F32), dma((2, leaves))],
            compiler_params=pltpu.CompilerParams(vmem_limit_bytes=14 * 2 ** 20),
            name='down_out',
        )(*[pltpu.with_memory_space_constraint(a, pltpu.VMEM) for a in held])

    return jax.shard_map(body, mesh=mesh, in_specs=(rows_spec,) + (tree_spec,) * 15 + (full_spec,) * 3, out_specs=rows_spec, check_vma=False)
```

```python
import functools
import math

import jax
import jax.numpy as jnp
from jax import lax
from jax.experimental import pallas as pl
from jax.experimental.pallas import tpu as pltpu
from jax.sharding import PartitionSpec as P

MESH = pl.DeviceIdType.MESH
F32 = jnp.float32
BF16 = jnp.bfloat16
VMEM_ALL = pl.BlockSpec(memory_space=pltpu.VMEM)
HBM_ALL = pl.BlockSpec(memory_space=pltpu.HBM)


def log_two(count):
    return int(math.log2(count) + 0.5)


def mm(lhs, rhs, lhs_dim, rhs_dim):
    return lax.dot_general(lhs, rhs, (((lhs_dim,), (rhs_dim,)), ((), ())), preferred_element_type=F32)


def down_skeletons(columns, y_dev, g0, g1, g2, r0, r1, r2, y2, y1, y0):
    for n in range(r2.shape[0]):
        y2[n] = (g2[n, :, columns] + mm(r2[n], y_dev[:, columns], 1, 0)).astype(BF16)
    for n in range(r1.shape[0]):
        y1[n] = (g1[n, :, columns] + mm(r1[n], y2[n // 2], 1, 0)).astype(BF16)
    for n in range(r0.shape[0]):
        y0[n] = (g0[n, :, columns] + mm(r0[n], y1[n // 2], 1, 0)).astype(BF16)


def up_kernel(devs, chunks, x_hbm, d_hbm, v_hbm, w0_hbm, b0_hbm, w1_hbm, b1_hbm, w2_hbm, b2_hbm, wu_hbm, bu_hbm, ru_hbm, wt_hbm, rt_hbm, bt_hbm, r0_hbm, r1_hbm, r2_hbm, u_hbm,
              y_dev, near, g0, g1, g2, r0, r1, r2, u,
              xb, d, v, w0, b0, w1, b1, w2, b2, wu, bu, ru, wt, rt, bt, xh0, xh1, xh2, xt, xsib, half_out, half_own, half_in, xchip, xall, x1, x1_sib, g_top, g_dev, y_out, y_all, y2, y1, y0, rt_t, bt_t,
              x_sem, d_sem, v_sem, w_sem, swap_send, swap_recv, out_send, out_recv, top_send, top_recv, back_send, back_recv, pair_send, pair_recv):
    me = lax.axis_index('tree')
    chips = devs // 2
    half_chips = chips // 2
    depth = log_two(devs)
    core = lax.rem(me, 2)
    chip = me // 2
    other = 1 - core
    partner = chip * 2 + other
    leaves, leaf_size, cols = xb.shape
    width = cols // chunks
    side_width = width // 2
    part = side_width // chips
    my_half = chip // half_chips
    my_slot = lax.rem(chip, half_chips)
    upper_half = (my_slot * 2) // half_chips
    same_half = 1 - lax.rem(my_half + core, 2)
    falling = lax.rem(upper_half + same_half, 2)

    barrier = pltpu.get_barrier_semaphore()
    for step in range(1, devs):
        pl.semaphore_signal(barrier, inc=1, device_id={'tree': lax.rem(me + step, devs)}, device_id_type=MESH)

    def remote(src, dst, send, recv, dest):
        return pltpu.make_async_remote_copy(src, dst, send, recv, device_id={'tree': dest}, device_id_type=MESH)

    def window(k):
        return pl.ds(k * width, width)

    def load_x(k, i):
        return pltpu.make_async_copy(x_hbm.at[pl.ds(i * leaf_size, leaf_size), window(k)], near.at[i, :, window(k)], x_sem.at[k, i])

    def load_d(i):
        return pltpu.make_async_copy(d_hbm.at[i], d.at[i], d_sem.at[i])

    def load_v(i):
        return pltpu.make_async_copy(v_hbm.at[i], v.at[i], v_sem.at[i])

    copies = {}
    for k, (name, hbm, vmem) in enumerate([('w0', w0_hbm, w0), ('w1', w1_hbm, w1), ('w2', w2_hbm, w2), ('wu', wu_hbm.at[0], wu), ('bu', bu_hbm.at[0], bu), ('ru', ru_hbm.at[0], ru), ('b0', b0_hbm, b0), ('b1', b1_hbm, b1), ('b2', b2_hbm, b2), ('r0', r0_hbm, r0), ('r1', r1_hbm, r1), ('r2', r2_hbm, r2), ('u', u_hbm, u)]):
        copies[name] = pltpu.make_async_copy(hbm, vmem, w_sem.at[k])
    base = len(copies)

    def top_slices(hbm, vmem, first, sem):
        out = []
        at = 0
        for level in range(first, depth):
            count = 2 ** (level - 1)
            start = 2 ** level - 2 ** first + core * count
            out.append(pltpu.make_async_copy(hbm.at[pl.ds(start, count)], vmem.at[pl.ds(at, count)], w_sem.at[sem + level]))
            at += count
        return out

    wt_copies = top_slices(wt_hbm, wt, 2, base)
    rt_copies = top_slices(rt_hbm, rt, 2, base + depth)
    bt_copies = top_slices(bt_hbm, bt, 1, base + 2 * depth)

    group = leaves // 2

    def load_many(some, stage=iter(range(99))):
        with jax.named_scope(f'l{next(stage)}'):
            for copy in some:
                copy.start()

    first_half, second_half = range(group), range(group, leaves)
    load_many([load(i) for i in first_half for load in (load_v, lambda i: load_x(0, i))])
    load_many([load(i) for i in second_half for load in (load_v, lambda i: load_x(0, i))])
    load_many([copies['w0'], copies['w1'], copies['w2'], copies['wu']])
    load_many([load_x(1, i) for i in first_half])
    load_many([load_x(1, i) for i in second_half])
    load_many([load_d(i) for i in range(3)])
    load_many([load_d(i) for i in range(3, leaves)])
    load_many(rt_copies + bt_copies)
    load_many(wt_copies)
    load_many([copies[name] for name in ('b2', 'b1', 'bu', 'b0', 'ru', 'r2', 'r1', 'r0', 'u')])

    def pair_of(ref, n, k):
        both = ref[2 * n:2 * n + 2, :, window(k)]
        return both.reshape(both.shape[0] * both.shape[1], width)

    def stacked(ref, n):
        both = ref[2 * n:2 * n + 2]
        return both.reshape(both.shape[0] * both.shape[1], both.shape[2])

    def up_leaves(k, first, last):
        for i in range(first, last):
            if k == 0:
                load_v(i).wait()
            load_x(k, i).wait()
        for i in range(first, last):
            block = near[i, :, window(k)].astype(BF16)
            xb[i, :, window(k)] = block
            xh0[i, :, window(k)] = mm(v[i], block, 0, 0).astype(BF16)

    def up_merges(k):
        for n in range(leaves // 2):
            xh1[n, :, window(k)] = mm(stacked(w0, n), pair_of(xh0, n, k), 0, 0).astype(BF16)
        for n in range(leaves // 4):
            xh2[n, :, window(k)] = mm(stacked(w1, n), pair_of(xh1, n, k), 0, 0).astype(BF16)

    def half_copy(k):
        return remote(half_out.at[k], half_in.at[k], swap_send.at[k, 0], swap_recv.at[k, 0], partner)

    def node_copy(k):
        return remote(xt.at[k], xsib.at[k], swap_send.at[k, 1], swap_recv.at[k, 1], partner)

    def node_skeleton(k):
        for side in (other, core):
            cut = pl.ds(pl.multiple_of(k * width + side * side_width, side_width), side_width)
            both = xh2[:, :, cut]
            xt[k, side] = mm(both.reshape(both.shape[0] * both.shape[1], side_width), w2[...].reshape(both.shape[0] * both.shape[1], w2.shape[2]), 0, 0).astype(BF16)

    def half_send(k):
        half_out[k] = mm(xt[k, other], wu[...], 1, 0)
        if k == 0:
            pl.semaphore_wait(barrier, devs - 1)
        half_copy(k).start()

    def half_keep(k):
        node_copy(k).start()
        half_own[k] = mm(xt[k, core], wu[...], 1, 0)

    def out_copy(k, step):
        dest = lax.rem(chip + step, chips)
        return remote(xchip.at[k, dest], xall.at[k, my_slot, core], out_send.at[k, step], out_recv.at[k, my_slot, core], dest * 2 + my_half)

    far_first = [half_chips]
    for step in range(half_chips - 1, 0, -1):
        far_first += [step, chips - step]

    def merge_send(k):
        half_copy(k).wait_recv()
        merged = (half_own[k] + half_in[k]).astype(BF16)
        xchip[k] = merged.reshape(chips, part, merged.shape[1])
        for step in far_first:
            out_copy(k, step).start()

        @pl.when(core != my_half)
        def _():
            out_copy(k, 0).start()

        @pl.when(core == my_half)
        def _():
            xall[k, my_slot, core] = xchip[k, chip]

    def near_leaves(first, last):
        for i in range(first, last):
            load_d(i).wait()
        for i in range(first, last):
            near[i] = mm(d[i], xb[i], 1, 0)

    def is_mine(n, c):
        return jnp.logical_and(core * half_chips + n == chip, core == c)

    w_at = {level: 2 ** (level - 1) - 2 for level in range(2, depth)}
    b_at = {level: 2 ** (level - 1) - 1 for level in range(1, depth)}

    def top_solve(k):
        for n in range(half_chips):
            for c in range(2):
                @pl.when(jnp.logical_not(is_mine(n, c)))
                def _():
                    remote(xchip.at[k, 0], xall.at[k, n, c], out_send.at[k, 0], out_recv.at[k, n, c], partner).wait_recv()

        levels = [[xall[k, n].reshape(2 * part, xall.shape[-1]) for n in range(half_chips)]]
        for level in range(depth - 1, 1, -1):
            below = levels[-1]
            at = w_at[level]
            levels.append([(mm(below[2 * q], wt[at + 2 * q], 1, 0) + mm(below[2 * q + 1], wt[at + 2 * q + 1], 1, 0)).astype(BF16) for q in range(len(below) // 2)])
        x1[k] = levels[-1][0]
        swap = remote(x1.at[k], x1_sib.at[k], top_send.at[k], top_recv.at[k], partner)
        swap.start()
        for level in range(2, depth):
            nodes = levels[depth - 1 - level]
            for n in range(len(nodes)):
                g_top[w_at[level] + n] = mm(nodes[n ^ 1], bt[b_at[level] + n], 1, 1)
        swap.wait()
        y_top = [mm(x1_sib[k], bt_t[...], 1, 0).astype(BF16)]
        for level in range(2, depth):
            y_top = [(g_top[w_at[level] + n] + mm(y_top[n // 2], rt_t[w_at[level] + n], 1, 0)).astype(BF16) for n in range(2 ** (level - 1))]
        for n in range(half_chips):
            y_out[k, n] = y_top[n].reshape(2, part, y_out.shape[-1])
        for i in range(half_chips):
            n = i + falling * (half_chips - 1 - 2 * i)
            for c in range(2):
                @pl.when(jnp.logical_not(is_mine(n, c)))
                def _():
                    back_copy(k, n, c).start()

                @pl.when(is_mine(n, c))
                def _():
                    y_all[k, c, chip] = y_out[k, n, c]

    def back_copy(k, n, c):
        return remote(y_out.at[k, n, c], y_all.at[k, c, chip], back_send.at[k, n, c], back_recv.at[k, chip], (core * half_chips + n) * 2 + c)

    def pair_copy(k, side):
        return remote(y_all.at[k, side], y_all.at[k, side], pair_send.at[k], pair_recv.at[k], partner)

    def back_wait(k):
        for j in range(chips):
            @pl.when(jnp.logical_or(j != chip, core != my_half))
            def _():
                remote(y_out.at[k, 0, 0], y_all.at[k, core, j], back_send.at[k, 0, 0], back_recv.at[k, j], partner).wait_recv()

        pair_copy(k, core).start()

    def finish(k):
        pair_copy(k, other).wait_recv()
        y_dev[:, window(k)] = (g_dev[:, window(k)] + mm(ru[...], y_all[k].reshape(width, y_all.shape[-1]), 1, 1)).astype(BF16)

    def add_far(first, last):
        for i in range(first, last):
            near[i, :, window(0)] = near[i, :, window(0)] + mm(u[i], y0[i], 1, 0)

    with jax.named_scope('p0'):
        up_leaves(0, 0, group)
    with jax.named_scope('p1'):
        up_leaves(0, group, leaves)
        for name in ('w0', 'w1', 'w2', 'wu'):
            copies[name].wait()
    with jax.named_scope('p2'):
        up_merges(0)
        node_skeleton(0)
    with jax.named_scope('p3'):
        half_send(0)
    with jax.named_scope('p4'):
        half_keep(0)
    with jax.named_scope('p5'):
        up_leaves(1, 0, group)
    with jax.named_scope('p6'):
        merge_send(0)
    with jax.named_scope('p7'):
        up_leaves(1, group, leaves)
        up_merges(1)
        node_skeleton(1)
    with jax.named_scope('q7'):
        half_send(1)
    with jax.named_scope('r7'):
        half_keep(1)
    with jax.named_scope('p8'):
        near_leaves(0, 2)
    with jax.named_scope('p9'):
        merge_send(1)
        for copy in bt_copies + rt_copies:
            copy.wait()
    with jax.named_scope('p10'):
        near_leaves(2, leaves)
        for n in range(rt.shape[0]):
            rt_t[n] = rt[n].T
        bt_t[...] = bt[0].T
        for copy in wt_copies:
            copy.wait()
    with jax.named_scope('p11'):
        top_solve(0)
    with jax.named_scope('p12'):
        top_solve(1)
    with jax.named_scope('p13'):
        for name in ('b2', 'b1', 'b0', 'bu', 'ru', 'r2', 'r1', 'r0', 'u'):
            copies[name].wait()
        for k in range(chunks):
            node_copy(k).wait_recv()
        for k in range(chunks):
            g_dev[:, window(k)] = mm(bu[...], xsib[k].reshape(width, xsib.shape[-1]), 1, 1)
        for n in range(leaves // 4):
            g2[n] = mm(b2[n], xh2[n ^ 1], 1, 0)
        for n in range(leaves // 2):
            g1[n] = mm(b1[n], xh1[n ^ 1], 1, 0)
    with jax.named_scope('p14'):
        back_wait(0)
    with jax.named_scope('p15'):
        for n in range(leaves):
            g0[n] = mm(b0[n], xh0[n ^ 1], 1, 0)
    with jax.named_scope('p16'):
        finish(0)
        down_skeletons(window(0), y_dev, g0, g1, g2, r0, r1, r2, y2, y1, y0)
    with jax.named_scope('p17'):
        add_far(0, 4)
    with jax.named_scope('q17'):
        back_wait(1)
    with jax.named_scope('p18'):
        add_far(4, leaves)
    with jax.named_scope('p19'):
        finish(1)

    for k in range(chunks):
        half_copy(k).wait_send()
        node_copy(k).wait_send()
        for step in far_first:
            out_copy(k, step).wait_send()

        @pl.when(core != my_half)
        def _():
            out_copy(k, 0).wait_send()

        for n in range(half_chips):
            for c in range(2):
                @pl.when(jnp.logical_not(is_mine(n, c)))
                def _():
                    back_copy(k, n, c).wait_send()

        pair_copy(k, core).wait_send()


def down_kernel(chunks, y_dev, near, g0, g1, g2, r0, r1, r2, u, out_hbm, y2, y1, y0, stage, out_sem):
    leaves, leaf_size, width = stage.shape
    last = pl.ds((chunks - 1) * width, width)
    done = pl.ds(0, (chunks - 1) * width)

    def store(i, src, columns, sem):
        return pltpu.make_async_copy(src, out_hbm.at[pl.ds(i * leaf_size, leaf_size), columns], sem)

    def early(i):
        return store(i, near.at[i, :, done], done, out_sem.at[0, i])

    def late(i):
        return store(i, stage.at[i], last, out_sem.at[1, i])

    def start_early(i, carry):
        early(i).start()
        return carry

    lax.fori_loop(0, leaves, start_early, 0)
    down_skeletons(last, y_dev, g0, g1, g2, r0, r1, r2, y2, y1, y0)
    for i in range(leaves):
        stage[i] = near[i, :, last] + mm(u[i], y0[i], 1, 0)
        late(i).start()
    for i in range(leaves):
        early(i).wait()
        late(i).wait()


def solution(mesh):
    devs = mesh.shape['tree']
    rows_spec = P(('batch', 'tree'), None)
    tree_spec = P('tree', None, None)
    full_spec = P(None, None, None)

    def body(x_loc, d_near, u_leaf, v_leaf, w_h0, r_h0, b_h0, w_h1, r_h1, b_h1, w_h2, r_h2, b_h2, w_upper, r_upper, b_upper, w_top, r_top, b_top):
        leaves, leaf_size, rank0 = u_leaf.shape
        cols = x_loc.shape[1]
        rank1 = w_h0.shape[2]
        rank2 = w_h1.shape[2]
        rank3 = w_h2.shape[2]
        chips = devs // 2
        chunks = 2
        width = cols // chunks
        part = cols // (chunks * devs)
        depth = log_two(devs)
        sds = jax.ShapeDtypeStruct
        dma = pltpu.SemaphoreType.DMA
        vmem = pltpu.VMEM
        outs = [vmem((rank3, cols), BF16), vmem((leaves, leaf_size, cols), F32), vmem((leaves, rank0, cols), F32), vmem((leaves // 2, rank1, cols), F32), vmem((leaves // 4, rank2, cols), F32)] + [vmem(a.shape, BF16) for a in (r_h0, r_h1, r_h2, u_leaf)]
        half_nodes = chips - 2
        scratch = [
            vmem((leaves, leaf_size, cols), BF16), vmem((leaves, leaf_size, leaf_size), BF16),
            vmem((leaves, leaf_size, rank0), BF16),
            vmem((leaves, rank0, rank1), BF16), vmem((leaves, rank0, rank0), BF16),
            vmem((leaves // 2, rank1, rank2), BF16), vmem((leaves // 2, rank1, rank1), BF16),
            vmem((leaves // 4, rank2, rank3), BF16), vmem((leaves // 4, rank2, rank2), BF16),
            vmem((rank3, rank3), BF16), vmem((rank3, rank3), BF16), vmem((rank3, rank3), BF16),
            vmem((half_nodes, rank3, rank3), BF16), vmem((half_nodes, rank3, rank3), BF16), vmem((half_nodes + 1, rank3, rank3), BF16),
            vmem((leaves, rank0, cols), BF16), vmem((leaves // 2, rank1, cols), BF16), vmem((leaves // 4, rank2, cols), BF16),
            vmem((chunks, 2, width // 2, rank3), BF16), vmem((chunks, 2, width // 2, rank3), BF16),
            vmem((chunks, width // 2, rank3), F32), vmem((chunks, width // 2, rank3), F32), vmem((chunks, width // 2, rank3), F32),
            vmem((chunks, chips, part, rank3), BF16), vmem((chunks, chips // 2, 2, part, rank3), BF16),
            vmem((chunks, 2 * part, rank3), BF16), vmem((chunks, 2 * part, rank3), BF16), vmem((half_nodes, 2 * part, rank3), F32), vmem((rank3, cols), F32),
            vmem((chunks, chips // 2, 2, part, rank3), BF16), vmem((chunks, 2, chips, part, rank3), BF16), vmem((leaves // 4, rank2, width), BF16), vmem((leaves // 2, rank1, width), BF16), vmem((leaves, rank0, width), BF16), vmem((half_nodes, rank3, rank3), BF16), vmem((rank3, rank3), BF16),
            dma((chunks, leaves)), dma((leaves,)), dma((leaves,)), dma((13 + 3 * depth,)),
            dma((chunks, 2)), dma((chunks, 2)), dma((chunks, chips)), dma((chunks, chips // 2, 2)), dma((chunks,)), dma((chunks,)),
            dma((chunks, chips // 2, 2)), dma((chunks, chips)), dma((chunks,)), dma((chunks,)),
        ]
        held = pl.pallas_call(
            functools.partial(up_kernel, devs, chunks),
            out_shape=outs,
            in_specs=[HBM_ALL] * 19,
            out_specs=[VMEM_ALL] * 9,
            scratch_shapes=scratch,
            compiler_params=pltpu.CompilerParams(collective_id=0, has_side_effects=True, vmem_limit_bytes=40 * 2 ** 20),
            name='up_top',
        )(*[pltpu.with_memory_space_constraint(a, pltpu.HBM) for a in (x_loc, d_near, v_leaf, w_h0, b_h0, w_h1, b_h1, w_h2, b_h2, w_upper, b_upper, r_upper, w_top, r_top, b_top, r_h0, r_h1, r_h2, u_leaf)])
        return pl.pallas_call(
            functools.partial(down_kernel, chunks),
            out_shape=sds(x_loc.shape, F32),
            in_specs=[VMEM_ALL] * 9,
            out_specs=HBM_ALL,
            scratch_shapes=[vmem((leaves // 4, rank2, width), BF16), vmem((leaves // 2, rank1, width), BF16), vmem((leaves, rank0, width), BF16), vmem((leaves, leaf_size, width), F32), dma((2, leaves))],
            compiler_params=pltpu.CompilerParams(vmem_limit_bytes=14 * 2 ** 20),
            name='down_out',
        )(*[pltpu.with_memory_space_constraint(a, pltpu.VMEM) for a in held])

    return jax.shard_map(body, mesh=mesh, in_specs=(rows_spec,) + (tree_spec,) * 15 + (full_spec,) * 3, out_specs=rows_spec, check_vma=False)
```

```python
import functools
import math

import jax
import jax.numpy as jnp
from jax import lax
from jax.experimental import pallas as pl
from jax.experimental.pallas import tpu as pltpu
from jax.sharding import PartitionSpec as P

MESH = pl.DeviceIdType.MESH
F32 = jnp.float32
BF16 = jnp.bfloat16
VMEM_ALL = pl.BlockSpec(memory_space=pltpu.VMEM)
HBM_ALL = pl.BlockSpec(memory_space=pltpu.HBM)


def log_two(count):
    return int(math.log2(count) + 0.5)


def mm(lhs, rhs, lhs_dim, rhs_dim):
    return lax.dot_general(lhs, rhs, (((lhs_dim,), (rhs_dim,)), ((), ())), preferred_element_type=F32)


def down_skeletons(columns, y_dev, g0, g1, g2, r0, r1, r2, y2, y1, y0):
    for n in range(r2.shape[0]):
        y2[n] = (g2[n, :, columns] + mm(r2[n], y_dev[:, columns], 1, 0)).astype(BF16)
    for n in range(r1.shape[0]):
        y1[n] = (g1[n, :, columns] + mm(r1[n], y2[n // 2], 1, 0)).astype(BF16)
    for n in range(r0.shape[0]):
        y0[n] = (g0[n, :, columns] + mm(r0[n], y1[n // 2], 1, 0)).astype(BF16)


def up_kernel(devs, chunks, x_hbm, d_hbm, v_hbm, w0_hbm, b0_hbm, w1_hbm, b1_hbm, w2_hbm, b2_hbm, wu_hbm, bu_hbm, ru_hbm, wt_hbm, rt_hbm, bt_hbm, r0_hbm, r1_hbm, r2_hbm, u_hbm,
              g_dev, y_last, ru, near, g0, g1, g2, r0, r1, r2, u,
              xb, d, v, w0, b0, w1, b1, w2, b2, wu, bu, wt, rt, bt, xh0, xh1, xh2, xt, xsib, half_out, half_own, half_in, xchip, xall, x1, x1_sib, g_top, y_dev, y_out, y_all, y2, y1, y0, rt_t, bt_t,
              x_sem, d_sem, v_sem, w_sem, swap_send, swap_recv, out_send, out_recv, top_send, top_recv, back_send, back_recv, pair_send, pair_recv):
    me = lax.axis_index('tree')
    chips = devs // 2
    half_chips = chips // 2
    depth = log_two(devs)
    core = lax.rem(me, 2)
    chip = me // 2
    other = 1 - core
    partner = chip * 2 + other
    leaves, leaf_size, cols = xb.shape
    width = cols // chunks
    side_width = width // 2
    part = side_width // chips
    my_half = chip // half_chips
    my_slot = lax.rem(chip, half_chips)
    upper_half = (my_slot * 2) // half_chips
    same_half = 1 - lax.rem(my_half + core, 2)
    falling = lax.rem(upper_half + same_half, 2)

    barrier = pltpu.get_barrier_semaphore()
    for step in range(1, devs):
        pl.semaphore_signal(barrier, inc=1, device_id={'tree': lax.rem(me + step, devs)}, device_id_type=MESH)

    def remote(src, dst, send, recv, dest):
        return pltpu.make_async_remote_copy(src, dst, send, recv, device_id={'tree': dest}, device_id_type=MESH)

    def window(k):
        return pl.ds(k * width, width)

    def load_x(k, i):
        return pltpu.make_async_copy(x_hbm.at[pl.ds(i * leaf_size, leaf_size), window(k)], near.at[i, :, window(k)], x_sem.at[k, i])

    def load_d(i):
        return pltpu.make_async_copy(d_hbm.at[i], d.at[i], d_sem.at[i])

    def load_v(i):
        return pltpu.make_async_copy(v_hbm.at[i], v.at[i], v_sem.at[i])

    copies = {}
    for k, (name, hbm, vmem) in enumerate([('w0', w0_hbm, w0), ('w1', w1_hbm, w1), ('w2', w2_hbm, w2), ('wu', wu_hbm.at[0], wu), ('bu', bu_hbm.at[0], bu), ('ru', ru_hbm.at[0], ru), ('b0', b0_hbm, b0), ('b1', b1_hbm, b1), ('b2', b2_hbm, b2), ('r0', r0_hbm, r0), ('r1', r1_hbm, r1), ('r2', r2_hbm, r2), ('u', u_hbm, u)]):
        copies[name] = pltpu.make_async_copy(hbm, vmem, w_sem.at[k])
    base = len(copies)

    def top_slices(hbm, vmem, first, sem):
        out = []
        at = 0
        for level in range(first, depth):
            count = 2 ** (level - 1)
            start = 2 ** level - 2 ** first + core * count
            out.append(pltpu.make_async_copy(hbm.at[pl.ds(start, count)], vmem.at[pl.ds(at, count)], w_sem.at[sem + level]))
            at += count
        return out

    wt_copies = top_slices(wt_hbm, wt, 2, base)
    rt_copies = top_slices(rt_hbm, rt, 2, base + depth)
    bt_copies = top_slices(bt_hbm, bt, 1, base + 2 * depth)

    group = leaves // 2

    def load_many(some, stage=iter(range(99))):
        with jax.named_scope(f'l{next(stage)}'):
            for copy in some:
                copy.start()

    first_half, second_half = range(group), range(group, leaves)
    load_many([load(i) for i in first_half for load in (load_v, lambda i: load_x(0, i))])
    load_many([load(i) for i in second_half for load in (load_v, lambda i: load_x(0, i))])
    load_many([copies['w0'], copies['w1'], copies['w2'], copies['wu']])
    load_many([load_x(1, i) for i in first_half])
    load_many([load_x(1, i) for i in second_half])
    load_many([load_d(i) for i in range(3)])
    load_many([load_d(i) for i in range(3, leaves)])
    load_many(rt_copies + bt_copies)
    load_many(wt_copies)
    load_many([copies[name] for name in ('b2', 'b1', 'bu', 'b0', 'ru', 'r2', 'r1', 'r0', 'u')])

    def pair_of(ref, n, k):
        both = ref[2 * n:2 * n + 2, :, window(k)]
        return both.reshape(both.shape[0] * both.shape[1], width)

    def stacked(ref, n):
        both = ref[2 * n:2 * n + 2]
        return both.reshape(both.shape[0] * both.shape[1], both.shape[2])

    def up_leaves(k, first, last):
        for i in range(first, last):
            if k == 0:
                load_v(i).wait()
            load_x(k, i).wait()
        for i in range(first, last):
            block = near[i, :, window(k)].astype(BF16)
            xb[i, :, window(k)] = block
            xh0[i, :, window(k)] = mm(v[i], block, 0, 0).astype(BF16)

    def up_merges(k):
        for n in range(leaves // 2):
            xh1[n, :, window(k)] = mm(stacked(w0, n), pair_of(xh0, n, k), 0, 0).astype(BF16)
        for n in range(leaves // 4):
            xh2[n, :, window(k)] = mm(stacked(w1, n), pair_of(xh1, n, k), 0, 0).astype(BF16)

    def half_copy(k):
        return remote(half_out.at[k], half_in.at[k], swap_send.at[k, 0], swap_recv.at[k, 0], partner)

    def node_copy(k):
        return remote(xt.at[k], xsib.at[k], swap_send.at[k, 1], swap_recv.at[k, 1], partner)

    def node_skeleton(k):
        for side in (other, core):
            cut = pl.ds(pl.multiple_of(k * width + side * side_width, side_width), side_width)
            both = xh2[:, :, cut]
            xt[k, side] = mm(both.reshape(both.shape[0] * both.shape[1], side_width), w2[...].reshape(both.shape[0] * both.shape[1], w2.shape[2]), 0, 0).astype(BF16)

    def half_send(k):
        half_out[k] = mm(xt[k, other], wu[...], 1, 0)
        if k == 0:
            pl.semaphore_wait(barrier, devs - 1)
        half_copy(k).start()

    def half_keep(k):
        node_copy(k).start()
        half_own[k] = mm(xt[k, core], wu[...], 1, 0)

    def out_copy(k, step):
        dest = lax.rem(chip + step, chips)
        return remote(xchip.at[k, dest], xall.at[k, my_slot, core], out_send.at[k, step], out_recv.at[k, my_slot, core], dest * 2 + my_half)

    far_first = [half_chips]
    for step in range(half_chips - 1, 0, -1):
        far_first += [step, chips - step]

    def merge_send(k):
        half_copy(k).wait_recv()
        merged = (half_own[k] + half_in[k]).astype(BF16)
        xchip[k] = merged.reshape(chips, part, merged.shape[1])
        for step in far_first:
            out_copy(k, step).start()

        @pl.when(core != my_half)
        def _():
            out_copy(k, 0).start()

        @pl.when(core == my_half)
        def _():
            xall[k, my_slot, core] = xchip[k, chip]

    def near_leaves(first, last):
        for i in range(first, last):
            load_d(i).wait()
        for i in range(first, last):
            near[i] = mm(d[i], xb[i], 1, 0)

    def is_mine(n, c):
        return jnp.logical_and(core * half_chips + n == chip, core == c)

    w_at = {level: 2 ** (level - 1) - 2 for level in range(2, depth)}
    b_at = {level: 2 ** (level - 1) - 1 for level in range(1, depth)}

    def top_solve(k):
        for n in range(half_chips):
            for c in range(2):
                @pl.when(jnp.logical_not(is_mine(n, c)))
                def _():
                    remote(xchip.at[k, 0], xall.at[k, n, c], out_send.at[k, 0], out_recv.at[k, n, c], partner).wait_recv()

        levels = [[xall[k, n].reshape(2 * part, xall.shape[-1]) for n in range(half_chips)]]
        for level in range(depth - 1, 1, -1):
            below = levels[-1]
            at = w_at[level]
            levels.append([(mm(below[2 * q], wt[at + 2 * q], 1, 0) + mm(below[2 * q + 1], wt[at + 2 * q + 1], 1, 0)).astype(BF16) for q in range(len(below) // 2)])
        x1[k] = levels[-1][0]
        swap = remote(x1.at[k], x1_sib.at[k], top_send.at[k], top_recv.at[k], partner)
        swap.start()
        for level in range(2, depth):
            nodes = levels[depth - 1 - level]
            for n in range(len(nodes)):
                g_top[w_at[level] + n] = mm(nodes[n ^ 1], bt[b_at[level] + n], 1, 1)
        swap.wait()
        y_top = [mm(x1_sib[k], bt_t[...], 1, 0).astype(BF16)]
        for level in range(2, depth):
            y_top = [(g_top[w_at[level] + n] + mm(y_top[n // 2], rt_t[w_at[level] + n], 1, 0)).astype(BF16) for n in range(2 ** (level - 1))]
        for n in range(half_chips):
            y_out[k, n] = y_top[n].reshape(2, part, y_out.shape[-1])
        for i in range(half_chips):
            n = i + falling * (half_chips - 1 - 2 * i)
            for c in range(2):
                @pl.when(jnp.logical_not(is_mine(n, c)))
                def _():
                    back_copy(k, n, c).start()

                @pl.when(is_mine(n, c))
                def _():
                    y_all[k, c, chip] = y_out[k, n, c]

    def back_copy(k, n, c):
        return remote(y_out.at[k, n, c], y_all.at[k, c, chip], back_send.at[k, n, c], back_recv.at[k, chip], (core * half_chips + n) * 2 + c)

    def pair_copy(k, side):
        return remote(y_all.at[k, side], y_all.at[k, side], pair_send.at[k], pair_recv.at[k], partner)

    def back_wait(k):
        for j in range(chips):
            @pl.when(jnp.logical_or(j != chip, core != my_half))
            def _():
                remote(y_out.at[k, 0, 0], y_all.at[k, core, j], back_send.at[k, 0, 0], back_recv.at[k, j], partner).wait_recv()

        pair_copy(k, core).start()

    def finish(k):
        pair_copy(k, other).wait_recv()
        y_dev[:, window(k)] = (g_dev[:, window(k)] + mm(ru[...], y_all[k].reshape(width, y_all.shape[-1]), 1, 1)).astype(BF16)

    def add_far(first, last):
        for i in range(first, last):
            near[i, :, window(0)] = near[i, :, window(0)] + mm(u[i], y0[i], 1, 0)

    with jax.named_scope('p0'):
        up_leaves(0, 0, group)
    with jax.named_scope('p1'):
        up_leaves(0, group, leaves)
        for name in ('w0', 'w1', 'w2', 'wu'):
            copies[name].wait()
    with jax.named_scope('p2'):
        up_merges(0)
        node_skeleton(0)
    with jax.named_scope('p3'):
        half_send(0)
    with jax.named_scope('p4'):
        half_keep(0)
    with jax.named_scope('p5'):
        up_leaves(1, 0, group)
    with jax.named_scope('p6'):
        merge_send(0)
    with jax.named_scope('p7'):
        up_leaves(1, group, leaves)
        up_merges(1)
        node_skeleton(1)
    with jax.named_scope('q7'):
        half_send(1)
    with jax.named_scope('r7'):
        half_keep(1)
    with jax.named_scope('p8'):
        near_leaves(0, 2)
    with jax.named_scope('p9'):
        merge_send(1)
        for copy in bt_copies + rt_copies:
            copy.wait()
    with jax.named_scope('p10'):
        near_leaves(2, leaves)
        for n in range(rt.shape[0]):
            rt_t[n] = rt[n].T
        bt_t[...] = bt[0].T
        for copy in wt_copies:
            copy.wait()
    with jax.named_scope('p11'):
        top_solve(0)
    with jax.named_scope('p12'):
        top_solve(1)
    with jax.named_scope('p13'):
        for name in ('b2', 'b1', 'b0', 'bu', 'ru', 'r2', 'r1', 'r0', 'u'):
            copies[name].wait()
        for k in range(chunks):
            node_copy(k).wait_recv()
        for k in range(chunks):
            g_dev[:, window(k)] = mm(bu[...], xsib[k].reshape(width, xsib.shape[-1]), 1, 1)
        for n in range(leaves // 4):
            g2[n] = mm(b2[n], xh2[n ^ 1], 1, 0)
        for n in range(leaves // 2):
            g1[n] = mm(b1[n], xh1[n ^ 1], 1, 0)
    with jax.named_scope('p14'):
        back_wait(0)
    with jax.named_scope('p15'):
        for n in range(leaves):
            g0[n] = mm(b0[n], xh0[n ^ 1], 1, 0)
    with jax.named_scope('p16'):
        finish(0)
        down_skeletons(window(0), y_dev, g0, g1, g2, r0, r1, r2, y2, y1, y0)
    with jax.named_scope('p17'):
        add_far(0, 2)
    with jax.named_scope('q17'):
        back_wait(1)
    with jax.named_scope('p18'):
        add_far(2, leaves)
    with jax.named_scope('p19'):
        pair_copy(1, other).wait_recv()
        y_last[...] = y_all[1].reshape(width, y_all.shape[-1])

    for k in range(chunks):
        half_copy(k).wait_send()
        node_copy(k).wait_send()
        for step in far_first:
            out_copy(k, step).wait_send()

        @pl.when(core != my_half)
        def _():
            out_copy(k, 0).wait_send()

        for n in range(half_chips):
            for c in range(2):
                @pl.when(jnp.logical_not(is_mine(n, c)))
                def _():
                    back_copy(k, n, c).wait_send()

        pair_copy(k, core).wait_send()


def down_kernel(chunks, g_dev, y_last, ru, near, g0, g1, g2, r0, r1, r2, u, out_hbm, y_dev, y2, y1, y0, stage, out_sem):
    leaves, leaf_size, width = stage.shape
    last = pl.ds((chunks - 1) * width, width)
    done = pl.ds(0, (chunks - 1) * width)

    def store(i, src, columns, sem):
        return pltpu.make_async_copy(src, out_hbm.at[pl.ds(i * leaf_size, leaf_size), columns], sem)

    def early(i):
        return store(i, near.at[i, :, done], done, out_sem.at[0, i])

    def late(i):
        return store(i, stage.at[i], last, out_sem.at[1, i])

    def start_early(i, carry):
        early(i).start()
        return carry

    lax.fori_loop(0, leaves, start_early, 0)
    y_dev[:, last] = (g_dev[:, last] + mm(ru[...], y_last[...], 1, 1)).astype(BF16)
    down_skeletons(last, y_dev, g0, g1, g2, r0, r1, r2, y2, y1, y0)
    for i in range(leaves):
        stage[i] = near[i, :, last] + mm(u[i], y0[i], 1, 0)
        late(i).start()
    for i in range(leaves):
        early(i).wait()
        late(i).wait()


def solution(mesh):
    devs = mesh.shape['tree']
    rows_spec = P(('batch', 'tree'), None)
    tree_spec = P('tree', None, None)
    full_spec = P(None, None, None)

    def body(x_loc, d_near, u_leaf, v_leaf, w_h0, r_h0, b_h0, w_h1, r_h1, b_h1, w_h2, r_h2, b_h2, w_upper, r_upper, b_upper, w_top, r_top, b_top):
        leaves, leaf_size, rank0 = u_leaf.shape
        cols = x_loc.shape[1]
        rank1 = w_h0.shape[2]
        rank2 = w_h1.shape[2]
        rank3 = w_h2.shape[2]
        chips = devs // 2
        chunks = 2
        width = cols // chunks
        part = cols // (chunks * devs)
        depth = log_two(devs)
        sds = jax.ShapeDtypeStruct
        dma = pltpu.SemaphoreType.DMA
        vmem = pltpu.VMEM
        outs = [vmem((rank3, cols), F32), vmem((width, rank3), BF16), vmem((rank3, rank3), BF16), vmem((leaves, leaf_size, cols), F32), vmem((leaves, rank0, cols), F32), vmem((leaves // 2, rank1, cols), F32), vmem((leaves // 4, rank2, cols), F32)] + [vmem(a.shape, BF16) for a in (r_h0, r_h1, r_h2, u_leaf)]
        half_nodes = chips - 2
        scratch = [
            vmem((leaves, leaf_size, cols), BF16), vmem((leaves, leaf_size, leaf_size), BF16),
            vmem((leaves, leaf_size, rank0), BF16),
            vmem((leaves, rank0, rank1), BF16), vmem((leaves, rank0, rank0), BF16),
            vmem((leaves // 2, rank1, rank2), BF16), vmem((leaves // 2, rank1, rank1), BF16),
            vmem((leaves // 4, rank2, rank3), BF16), vmem((leaves // 4, rank2, rank2), BF16),
            vmem((rank3, rank3), BF16), vmem((rank3, rank3), BF16),
            vmem((half_nodes, rank3, rank3), BF16), vmem((half_nodes, rank3, rank3), BF16), vmem((half_nodes + 1, rank3, rank3), BF16),
            vmem((leaves, rank0, cols), BF16), vmem((leaves // 2, rank1, cols), BF16), vmem((leaves // 4, rank2, cols), BF16),
            vmem((chunks, 2, width // 2, rank3), BF16), vmem((chunks, 2, width // 2, rank3), BF16),
            vmem((chunks, width // 2, rank3), F32), vmem((chunks, width // 2, rank3), F32), vmem((chunks, width // 2, rank3), F32),
            vmem((chunks, chips, part, rank3), BF16), vmem((chunks, chips // 2, 2, part, rank3), BF16),
            vmem((chunks, 2 * part, rank3), BF16), vmem((chunks, 2 * part, rank3), BF16), vmem((half_nodes, 2 * part, rank3), F32), vmem((rank3, cols), BF16),
            vmem((chunks, chips // 2, 2, part, rank3), BF16), vmem((chunks, 2, chips, part, rank3), BF16), vmem((leaves // 4, rank2, width), BF16), vmem((leaves // 2, rank1, width), BF16), vmem((leaves, rank0, width), BF16), vmem((half_nodes, rank3, rank3), BF16), vmem((rank3, rank3), BF16),
            dma((chunks, leaves)), dma((leaves,)), dma((leaves,)), dma((13 + 3 * depth,)),
            dma((chunks, 2)), dma((chunks, 2)), dma((chunks, chips)), dma((chunks, chips // 2, 2)), dma((chunks,)), dma((chunks,)),
            dma((chunks, chips // 2, 2)), dma((chunks, chips)), dma((chunks,)), dma((chunks,)),
        ]
        held = pl.pallas_call(
            functools.partial(up_kernel, devs, chunks),
            out_shape=outs,
            in_specs=[HBM_ALL] * 19,
            out_specs=[VMEM_ALL] * 11,
            scratch_shapes=scratch,
            compiler_params=pltpu.CompilerParams(collective_id=0, has_side_effects=True, vmem_limit_bytes=40 * 2 ** 20),
            name='up_top',
        )(*[pltpu.with_memory_space_constraint(a, pltpu.HBM) for a in (x_loc, d_near, v_leaf, w_h0, b_h0, w_h1, b_h1, w_h2, b_h2, w_upper, b_upper, r_upper, w_top, r_top, b_top, r_h0, r_h1, r_h2, u_leaf)])
        return pl.pallas_call(
            functools.partial(down_kernel, chunks),
            out_shape=sds(x_loc.shape, F32),
            in_specs=[VMEM_ALL] * 11,
            out_specs=HBM_ALL,
            scratch_shapes=[vmem((rank3, cols), BF16), vmem((leaves // 4, rank2, width), BF16), vmem((leaves // 2, rank1, width), BF16), vmem((leaves, rank0, width), BF16), vmem((leaves, leaf_size, width), F32), dma((2, leaves))],
            compiler_params=pltpu.CompilerParams(vmem_limit_bytes=14 * 2 ** 20),
            name='down_out',
        )(*[pltpu.with_memory_space_constraint(a, pltpu.VMEM) for a in held])

    return jax.shard_map(body, mesh=mesh, in_specs=(rows_spec,) + (tree_spec,) * 15 + (full_spec,) * 3, out_specs=rows_spec, check_vma=False)
```

```python
import functools
import math

import jax
import jax.numpy as jnp
from jax import lax
from jax.experimental import pallas as pl
from jax.experimental.pallas import tpu as pltpu
from jax.sharding import PartitionSpec as P

MESH = pl.DeviceIdType.MESH
F32 = jnp.float32
BF16 = jnp.bfloat16
VMEM_ALL = pl.BlockSpec(memory_space=pltpu.VMEM)
HBM_ALL = pl.BlockSpec(memory_space=pltpu.HBM)


def log_two(count):
    return int(math.log2(count) + 0.5)


def mm(lhs, rhs, lhs_dim, rhs_dim):
    return lax.dot_general(lhs, rhs, (((lhs_dim,), (rhs_dim,)), ((), ())), preferred_element_type=F32)


def down_skeletons(columns, y_dev, g0, g1, g2, r0, r1, r2, y2, y1, y0):
    for n in range(r2.shape[0]):
        y2[n] = (g2[n, :, columns] + mm(r2[n], y_dev[:, columns], 1, 0)).astype(BF16)
    for n in range(r1.shape[0]):
        y1[n] = (g1[n, :, columns] + mm(r1[n], y2[n // 2], 1, 0)).astype(BF16)
    for n in range(r0.shape[0]):
        y0[n] = (g0[n, :, columns] + mm(r0[n], y1[n // 2], 1, 0)).astype(BF16)


def up_kernel(devs, chunks, x_hbm, d_hbm, v_hbm, w0_hbm, b0_hbm, w1_hbm, b1_hbm, w2_hbm, b2_hbm, wu_hbm, bu_hbm, ru_hbm, wt_hbm, rt_hbm, bt_hbm, r0_hbm, r1_hbm, r2_hbm, u_hbm,
              g_dev, y_last, ru, near, g0, g1, g2, r0, r1, r2, u,
              xb, d, v, w0, b0, w1, b1, w2, b2, wu, bu, wt, rt, bt, xh0, xh1, xh2, xt, xsib, half_out, half_own, half_in, xchip, xall, x1, x1_sib, g_top, y_dev, y_out, y_all, y2, y1, y0, rt_t, bt_t,
              x_sem, d_sem, v_sem, w_sem, swap_send, swap_recv, out_send, out_recv, top_send, top_recv, back_send, back_recv, pair_send, pair_recv):
    me = lax.axis_index('tree')
    chips = devs // 2
    half_chips = chips // 2
    depth = log_two(devs)
    core = lax.rem(me, 2)
    chip = me // 2
    other = 1 - core
    partner = chip * 2 + other
    leaves, leaf_size, cols = xb.shape
    width = cols // chunks
    side_width = width // 2
    part = side_width // chips
    my_half = chip // half_chips
    my_slot = lax.rem(chip, half_chips)
    upper_half = (my_slot * 2) // half_chips
    same_half = 1 - lax.rem(my_half + core, 2)
    falling = lax.rem(upper_half + same_half, 2)

    barrier = pltpu.get_barrier_semaphore()
    for step in range(1, devs):
        pl.semaphore_signal(barrier, inc=1, device_id={'tree': lax.rem(me + step, devs)}, device_id_type=MESH)

    def remote(src, dst, send, recv, dest):
        return pltpu.make_async_remote_copy(src, dst, send, recv, device_id={'tree': dest}, device_id_type=MESH)

    def window(k):
        return pl.ds(k * width, width)

    def load_x(k, i):
        return pltpu.make_async_copy(x_hbm.at[pl.ds(i * leaf_size, leaf_size), window(k)], near.at[i, :, window(k)], x_sem.at[k, i])

    def load_d(i):
        return pltpu.make_async_copy(d_hbm.at[i], d.at[i], d_sem.at[i])

    def load_v(i):
        return pltpu.make_async_copy(v_hbm.at[i], v.at[i], v_sem.at[i])

    copies = {}
    for k, (name, hbm, vmem) in enumerate([('w0', w0_hbm, w0), ('w1', w1_hbm, w1), ('w2', w2_hbm, w2), ('wu', wu_hbm.at[0], wu), ('bu', bu_hbm.at[0], bu), ('ru', ru_hbm.at[0], ru), ('b0', b0_hbm, b0), ('b1', b1_hbm, b1), ('b2', b2_hbm, b2), ('r0', r0_hbm, r0), ('r1', r1_hbm, r1), ('r2', r2_hbm, r2), ('u', u_hbm, u)]):
        copies[name] = pltpu.make_async_copy(hbm, vmem, w_sem.at[k])
    base = len(copies)

    def top_slices(hbm, vmem, first, sem):
        out = []
        at = 0
        for level in range(first, depth):
            count = 2 ** (level - 1)
            start = 2 ** level - 2 ** first + core * count
            out.append(pltpu.make_async_copy(hbm.at[pl.ds(start, count)], vmem.at[pl.ds(at, count)], w_sem.at[sem + level]))
            at += count
        return out

    wt_copies = top_slices(wt_hbm, wt, 2, base)
    rt_copies = top_slices(rt_hbm, rt, 2, base + depth)
    bt_copies = top_slices(bt_hbm, bt, 1, base + 2 * depth)

    group = leaves // 2

    def load_many(some, stage=iter(range(99))):
        with jax.named_scope(f'l{next(stage)}'):
            for copy in some:
                copy.start()

    first_half, second_half = range(group), range(group, leaves)
    load_many([load(i) for i in first_half for load in (load_v, lambda i: load_x(0, i))])
    load_many([load(i) for i in second_half for load in (load_v, lambda i: load_x(0, i))])
    load_many([copies['w0'], copies['w1'], copies['w2'], copies['wu']])
    load_many([load_x(1, i) for i in first_half])
    load_many([load_x(1, i) for i in second_half])
    load_many([load_d(i) for i in range(3)])
    load_many([load_d(i) for i in range(3, leaves)])
    load_many(rt_copies + bt_copies)
    load_many(wt_copies)
    load_many([copies[name] for name in ('b2', 'b1', 'bu', 'b0', 'ru', 'r2', 'r1', 'r0', 'u')])

    def pair_of(ref, n, k):
        both = ref[2 * n:2 * n + 2, :, window(k)]
        return both.reshape(both.shape[0] * both.shape[1], width)

    def stacked(ref, n):
        both = ref[2 * n:2 * n + 2]
        return both.reshape(both.shape[0] * both.shape[1], both.shape[2])

    def up_leaves(k, first, last):
        for i in range(first, last):
            if k == 0:
                load_v(i).wait()
            load_x(k, i).wait()
        for i in range(first, last):
            block = near[i, :, window(k)].astype(BF16)
            xb[i, :, window(k)] = block
            xh0[i, :, window(k)] = mm(v[i], block, 0, 0).astype(BF16)

    def up_merges(k):
        for n in range(leaves // 2):
            xh1[n, :, window(k)] = mm(stacked(w0, n), pair_of(xh0, n, k), 0, 0).astype(BF16)
        for n in range(leaves // 4):
            xh2[n, :, window(k)] = mm(stacked(w1, n), pair_of(xh1, n, k), 0, 0).astype(BF16)

    def half_copy(k):
        return remote(half_out.at[k], half_in.at[k], swap_send.at[k, 0], swap_recv.at[k, 0], partner)

    def node_copy(k):
        return remote(xt.at[k], xsib.at[k], swap_send.at[k, 1], swap_recv.at[k, 1], partner)

    def node_skeleton(k):
        for side in (other, core):
            cut = pl.ds(pl.multiple_of(k * width + side * side_width, side_width), side_width)
            both = xh2[:, :, cut]
            xt[k, side] = mm(both.reshape(both.shape[0] * both.shape[1], side_width), w2[...].reshape(both.shape[0] * both.shape[1], w2.shape[2]), 0, 0).astype(BF16)

    def half_send(k):
        if k == 0:
            copies['wu'].wait()
        half_out[k] = mm(xt[k, other], wu[...], 1, 0)
        if k == 0:
            pl.semaphore_wait(barrier, devs - 1)
        half_copy(k).start()

    def half_keep(k):
        node_copy(k).start()
        half_own[k] = mm(xt[k, core], wu[...], 1, 0)

    def out_copy(k, step):
        dest = lax.rem(chip + step, chips)
        return remote(xchip.at[k, dest], xall.at[k, my_slot, core], out_send.at[k, step], out_recv.at[k, my_slot, core], dest * 2 + my_half)

    far_first = [half_chips]
    for step in range(half_chips - 1, 0, -1):
        far_first += [step, chips - step]

    def merge_send(k):
        half_copy(k).wait_recv()
        merged = (half_own[k] + half_in[k]).astype(BF16)
        xchip[k] = merged.reshape(chips, part, merged.shape[1])
        for step in far_first:
            out_copy(k, step).start()

        @pl.when(core != my_half)
        def _():
            out_copy(k, 0).start()

        @pl.when(core == my_half)
        def _():
            xall[k, my_slot, core] = xchip[k, chip]

    def near_leaves(first, last):
        for i in range(first, last):
            load_d(i).wait()
        for i in range(first, last):
            near[i] = mm(d[i], xb[i], 1, 0)

    def is_mine(n, c):
        return jnp.logical_and(core * half_chips + n == chip, core == c)

    w_at = {level: 2 ** (level - 1) - 2 for level in range(2, depth)}
    b_at = {level: 2 ** (level - 1) - 1 for level in range(1, depth)}

    def top_solve(k):
        for n in range(half_chips):
            for c in range(2):
                @pl.when(jnp.logical_not(is_mine(n, c)))
                def _():
                    remote(xchip.at[k, 0], xall.at[k, n, c], out_send.at[k, 0], out_recv.at[k, n, c], partner).wait_recv()

        levels = [[xall[k, n].reshape(2 * part, xall.shape[-1]) for n in range(half_chips)]]
        for level in range(depth - 1, 1, -1):
            below = levels[-1]
            at = w_at[level]
            levels.append([(mm(below[2 * q], wt[at + 2 * q], 1, 0) + mm(below[2 * q + 1], wt[at + 2 * q + 1], 1, 0)).astype(BF16) for q in range(len(below) // 2)])
        x1[k] = levels[-1][0]
        swap = remote(x1.at[k], x1_sib.at[k], top_send.at[k], top_recv.at[k], partner)
        swap.start()
        for level in range(2, depth):
            nodes = levels[depth - 1 - level]
            for n in range(len(nodes)):
                g_top[w_at[level] + n] = mm(nodes[n ^ 1], bt[b_at[level] + n], 1, 1)
        swap.wait()
        y_top = [mm(x1_sib[k], bt_t[...], 1, 0).astype(BF16)]
        for level in range(2, depth):
            y_top = [(g_top[w_at[level] + n] + mm(y_top[n // 2], rt_t[w_at[level] + n], 1, 0)).astype(BF16) for n in range(2 ** (level - 1))]
        for n in range(half_chips):
            y_out[k, n] = y_top[n].reshape(2, part, y_out.shape[-1])
        for i in range(half_chips):
            n = i + falling * (half_chips - 1 - 2 * i)
            for c in range(2):
                @pl.when(jnp.logical_not(is_mine(n, c)))
                def _():
                    back_copy(k, n, c).start()

                @pl.when(is_mine(n, c))
                def _():
                    y_all[k, c, chip] = y_out[k, n, c]

    def back_copy(k, n, c):
        return remote(y_out.at[k, n, c], y_all.at[k, c, chip], back_send.at[k, n, c], back_recv.at[k, chip], (core * half_chips + n) * 2 + c)

    def pair_copy(k, side):
        return remote(y_all.at[k, side], y_all.at[k, side], pair_send.at[k], pair_recv.at[k], partner)

    def back_wait(k):
        for j in range(chips):
            @pl.when(jnp.logical_or(j != chip, core != my_half))
            def _():
                remote(y_out.at[k, 0, 0], y_all.at[k, core, j], back_send.at[k, 0, 0], back_recv.at[k, j], partner).wait_recv()

        pair_copy(k, core).start()

    def finish(k):
        pair_copy(k, other).wait_recv()
        y_dev[:, window(k)] = (g_dev[:, window(k)] + mm(ru[...], y_all[k].reshape(width, y_all.shape[-1]), 1, 1)).astype(BF16)

    def add_far(first, last):
        for i in range(first, last):
            near[i, :, window(0)] = near[i, :, window(0)] + mm(u[i], y0[i], 1, 0)

    with jax.named_scope('p0'):
        up_leaves(0, 0, group)
    with jax.named_scope('p1'):
        up_leaves(0, group, leaves)
        for name in ('w0', 'w1', 'w2'):
            copies[name].wait()
    with jax.named_scope('p2'):
        up_merges(0)
        node_skeleton(0)
    with jax.named_scope('p3'):
        half_send(0)
    with jax.named_scope('p4'):
        half_keep(0)
    with jax.named_scope('p5'):
        up_leaves(1, 0, group + 2)
    with jax.named_scope('p6'):
        merge_send(0)
    with jax.named_scope('p7'):
        up_leaves(1, group + 2, leaves)
        up_merges(1)
        node_skeleton(1)
    with jax.named_scope('q7'):
        half_send(1)
    with jax.named_scope('r7'):
        half_keep(1)
    with jax.named_scope('p8'):
        near_leaves(0, 2)
    with jax.named_scope('p9'):
        merge_send(1)
        for copy in bt_copies + rt_copies:
            copy.wait()
    with jax.named_scope('p10'):
        near_leaves(2, leaves)
        for n in range(rt.shape[0]):
            rt_t[n] = rt[n].T
        bt_t[...] = bt[0].T
        for copy in wt_copies:
            copy.wait()
    with jax.named_scope('p11'):
        top_solve(0)
    with jax.named_scope('p12'):
        top_solve(1)
    with jax.named_scope('p13'):
        for name in ('b2', 'b1', 'b0', 'bu', 'ru', 'r2', 'r1', 'r0', 'u'):
            copies[name].wait()
        for k in range(chunks):
            node_copy(k).wait_recv()
        for k in range(chunks):
            g_dev[:, window(k)] = mm(bu[...], xsib[k].reshape(width, xsib.shape[-1]), 1, 1)
        for n in range(leaves // 4):
            g2[n] = mm(b2[n], xh2[n ^ 1], 1, 0)
        for n in range(leaves // 2):
            g1[n] = mm(b1[n], xh1[n ^ 1], 1, 0)
    with jax.named_scope('p14'):
        back_wait(0)
    with jax.named_scope('p15'):
        for n in range(leaves):
            g0[n] = mm(b0[n], xh0[n ^ 1], 1, 0)
    with jax.named_scope('p16'):
        finish(0)
        down_skeletons(window(0), y_dev, g0, g1, g2, r0, r1, r2, y2, y1, y0)
    with jax.named_scope('p17'):
        add_far(0, 2)
    with jax.named_scope('q17'):
        back_wait(1)
    with jax.named_scope('p18'):
        add_far(2, leaves)
    with jax.named_scope('p19'):
        pair_copy(1, other).wait_recv()
        y_last[...] = y_all[1].reshape(width, y_all.shape[-1])

    for k in range(chunks):
        half_copy(k).wait_send()
        node_copy(k).wait_send()
        for step in far_first:
            out_copy(k, step).wait_send()

        @pl.when(core != my_half)
        def _():
            out_copy(k, 0).wait_send()

        for n in range(half_chips):
            for c in range(2):
                @pl.when(jnp.logical_not(is_mine(n, c)))
                def _():
                    back_copy(k, n, c).wait_send()

        pair_copy(k, core).wait_send()


def down_kernel(chunks, g_dev, y_last, ru, near, g0, g1, g2, r0, r1, r2, u, out_hbm, y_dev, y2, y1, y0, stage, out_sem):
    leaves, leaf_size, width = stage.shape
    last = pl.ds((chunks - 1) * width, width)
    done = pl.ds(0, (chunks - 1) * width)

    def store(i, src, columns, sem):
        return pltpu.make_async_copy(src, out_hbm.at[pl.ds(i * leaf_size, leaf_size), columns], sem)

    def early(i):
        return store(i, near.at[i, :, done], done, out_sem.at[0, i])

    def late(i):
        return store(i, stage.at[i], last, out_sem.at[1, i])

    def start_early(i, carry):
        early(i).start()
        return carry

    lax.fori_loop(0, leaves, start_early, 0)
    y_dev[:, last] = (g_dev[:, last] + mm(ru[...], y_last[...], 1, 1)).astype(BF16)
    down_skeletons(last, y_dev, g0, g1, g2, r0, r1, r2, y2, y1, y0)
    for i in range(leaves):
        stage[i] = near[i, :, last] + mm(u[i], y0[i], 1, 0)
        late(i).start()
    for i in range(leaves):
        early(i).wait()
        late(i).wait()


def solution(mesh):
    devs = mesh.shape['tree']
    rows_spec = P(('batch', 'tree'), None)
    tree_spec = P('tree', None, None)
    full_spec = P(None, None, None)

    def body(x_loc, d_near, u_leaf, v_leaf, w_h0, r_h0, b_h0, w_h1, r_h1, b_h1, w_h2, r_h2, b_h2, w_upper, r_upper, b_upper, w_top, r_top, b_top):
        leaves, leaf_size, rank0 = u_leaf.shape
        cols = x_loc.shape[1]
        rank1 = w_h0.shape[2]
        rank2 = w_h1.shape[2]
        rank3 = w_h2.shape[2]
        chips = devs // 2
        chunks = 2
        width = cols // chunks
        part = cols // (chunks * devs)
        depth = log_two(devs)
        sds = jax.ShapeDtypeStruct
        dma = pltpu.SemaphoreType.DMA
        vmem = pltpu.VMEM
        outs = [vmem((rank3, cols), F32), vmem((width, rank3), BF16), vmem((rank3, rank3), BF16), vmem((leaves, leaf_size, cols), F32), vmem((leaves, rank0, cols), F32), vmem((leaves // 2, rank1, cols), F32), vmem((leaves // 4, rank2, cols), F32)] + [vmem(a.shape, BF16) for a in (r_h0, r_h1, r_h2, u_leaf)]
        half_nodes = chips - 2
        scratch = [
            vmem((leaves, leaf_size, cols), BF16), vmem((leaves, leaf_size, leaf_size), BF16),
            vmem((leaves, leaf_size, rank0), BF16),
            vmem((leaves, rank0, rank1), BF16), vmem((leaves, rank0, rank0), BF16),
            vmem((leaves // 2, rank1, rank2), BF16), vmem((leaves // 2, rank1, rank1), BF16),
            vmem((leaves // 4, rank2, rank3), BF16), vmem((leaves // 4, rank2, rank2), BF16),
            vmem((rank3, rank3), BF16), vmem((rank3, rank3), BF16),
            vmem((half_nodes, rank3, rank3), BF16), vmem((half_nodes, rank3, rank3), BF16), vmem((half_nodes + 1, rank3, rank3), BF16),
            vmem((leaves, rank0, cols), BF16), vmem((leaves // 2, rank1, cols), BF16), vmem((leaves // 4, rank2, cols), BF16),
            vmem((chunks, 2, width // 2, rank3), BF16), vmem((chunks, 2, width // 2, rank3), BF16),
            vmem((chunks, width // 2, rank3), F32), vmem((chunks, width // 2, rank3), F32), vmem((chunks, width // 2, rank3), F32),
            vmem((chunks, chips, part, rank3), BF16), vmem((chunks, chips // 2, 2, part, rank3), BF16),
            vmem((chunks, 2 * part, rank3), BF16), vmem((chunks, 2 * part, rank3), BF16), vmem((half_nodes, 2 * part, rank3), F32), vmem((rank3, cols), BF16),
            vmem((chunks, chips // 2, 2, part, rank3), BF16), vmem((chunks, 2, chips, part, rank3), BF16), vmem((leaves // 4, rank2, width), BF16), vmem((leaves // 2, rank1, width), BF16), vmem((leaves, rank0, width), BF16), vmem((half_nodes, rank3, rank3), BF16), vmem((rank3, rank3), BF16),
            dma((chunks, leaves)), dma((leaves,)), dma((leaves,)), dma((13 + 3 * depth,)),
            dma((chunks, 2)), dma((chunks, 2)), dma((chunks, chips)), dma((chunks, chips // 2, 2)), dma((chunks,)), dma((chunks,)),
            dma((chunks, chips // 2, 2)), dma((chunks, chips)), dma((chunks,)), dma((chunks,)),
        ]
        held = pl.pallas_call(
            functools.partial(up_kernel, devs, chunks),
            out_shape=outs,
            in_specs=[HBM_ALL] * 19,
            out_specs=[VMEM_ALL] * 11,
            scratch_shapes=scratch,
            compiler_params=pltpu.CompilerParams(collective_id=0, has_side_effects=True, vmem_limit_bytes=40 * 2 ** 20),
            name='up_top',
        )(*[pltpu.with_memory_space_constraint(a, pltpu.HBM) for a in (x_loc, d_near, v_leaf, w_h0, b_h0, w_h1, b_h1, w_h2, b_h2, w_upper, b_upper, r_upper, w_top, r_top, b_top, r_h0, r_h1, r_h2, u_leaf)])
        return pl.pallas_call(
            functools.partial(down_kernel, chunks),
            out_shape=sds(x_loc.shape, F32),
            in_specs=[VMEM_ALL] * 11,
            out_specs=HBM_ALL,
            scratch_shapes=[vmem((rank3, cols), BF16), vmem((leaves // 4, rank2, width), BF16), vmem((leaves // 2, rank1, width), BF16), vmem((leaves, rank0, width), BF16), vmem((leaves, leaf_size, width), F32), dma((2, leaves))],
            compiler_params=pltpu.CompilerParams(vmem_limit_bytes=14 * 2 ** 20),
            name='down_out',
        )(*[pltpu.with_memory_space_constraint(a, pltpu.VMEM) for a in held])

    return jax.shard_map(body, mesh=mesh, in_specs=(rows_spec,) + (tree_spec,) * 15 + (full_spec,) * 3, out_specs=rows_spec, check_vma=False)
```
